32 devices in a mesh: dp: 4 (over z), tensor: 8 (over y, x, core).
Axes of the slice: x: 2, y: 2, z: 4, core: 2. Of those that a mesh axis runs over, the one named last changes fastest.
Arguments:
- tokens: bfloat16 [1024, 4096], P(('dp', 'tensor')), may hold values from -4 to 4
- lengths: int32 [4], replicated, may hold values from 64 to 256, as said below
- norm_gains: float32 [2, 4096], replicated, may hold values from 0.25 to 1.75
- query_weight: bfloat16 [2, 4096, 4096], P(None, None, 'tensor'), may hold values from -0.09375 to 0.09375
- key_weight: bfloat16 [2, 4096, 1024], P(None, None, 'tensor'), may hold values from -0.09375 to 0.09375
- value_weight: bfloat16 [2, 4096, 1024], P(None, None, 'tensor'), may hold values from -0.09375 to 0.09375
- out_weight: bfloat16 [2, 4096, 4096], P(None, 'tensor'), may hold values from -0.09375 to 0.09375
- query_probe: bfloat16 [2, 4096, 4096], P(None, 'dp', 'tensor'), may hold values from -0.09375 to 0.09375
- key_probe: bfloat16 [2, 4096, 1024], P(None, 'dp', 'tensor'), may hold values from -0.09375 to 0.09375
- value_probe: bfloat16 [2, 4096, 1024], P(None, 'dp', 'tensor'), may hold values from -0.09375 to 0.09375
- out_probe: bfloat16 [2, 4096, 4096], P(None, 'tensor', 'dp'), may hold values from -0.09375 to 0.09375
Outputs:
- query_product: float32 [2, 4096, 4096], P(None, 'dp', 'tensor')
- key_product: float32 [2, 4096, 1024], P(None, 'dp', 'tensor')
- value_product: float32 [2, 4096, 1024], P(None, 'dp', 'tensor')
- out_product: float32 [2, 4096, 4096], P(None, 'tensor', 'dp')
The draws below stay inside these ranges and needn't reach their ends.
Inputs may be any that keep to these rules, and one draw needn't show every extreme that they name: lengths[i] counts the leading valid positions of sequence i; the last sequence is full.
All inputs are finite; a program needn't handle non-finite values.
Results may differ from the reference program's by a relative error of at most 0.035.
Values may be sent and summed in bfloat16 or wider, within the bound.
A program may use at most 128 MiB of HBM per device.

```python
import math
import jax
import jax.numpy as jnp
from jax import lax

D = 4096
HEADS = 32
KVH = 8
HD = 128
LAYERS = 2
LEN = 256
SEQUENCES = 4
TOKENS = 1024
N_DP = 4
N_TENSOR = 8


def draw_tokens(key, part):
    keys = jax.random.split(key, 3)
    row_scale = jnp.exp(jax.random.uniform(keys[1], (TOKENS, 1), jnp.float32, 0.0, math.log(10.0)))
    column_scale = jnp.exp(jax.random.uniform(keys[2], (1, D), jnp.float32, 0.0, math.log(10.0)))
    base = jax.random.truncated_normal(keys[0], -4.0, 4.0, (TOKENS, D), jnp.float32)
    return (0.01 * base * row_scale * column_scale).astype(jnp.bfloat16)


def draw_lengths(key, part):
    number = jnp.arange(SEQUENCES)
    lowest = LEN // 4 + LEN // 2 * number // max(SEQUENCES - 1, 1)
    extra = jax.random.randint(key, (SEQUENCES,), 0, LEN // 4 + 1)
    drawn = jnp.minimum(lowest + extra, LEN)
    return jnp.where(number == SEQUENCES - 1, LEN, drawn).astype(jnp.int32)


def block_scale(stream_key, extent, cuts, smallest, high):
    def one(axis_at, shards_of):
        draws = jax.random.uniform(jax.random.fold_in(jax.random.fold_in(stream_key, 6), axis_at), (shards_of,), jnp.float32, smallest / len(cuts), high / len(cuts))
        return jnp.repeat(jnp.exp(draws), extent[axis_at] // shards_of).reshape((-1,) + (1,) * (len(extent) - axis_at - 1))

    level = one(*cuts[0])
    for cut in cuts[1:]:
        level = level * one(*cut)
    return level


def scatter_about(rng, shape, deviation, reach, cuts=(), kind=jnp.bfloat16):
    gain = block_scale(rng, shape, cuts, -0.22, 0.18) if cuts else 1.0
    values = jax.random.normal(rng, shape, jnp.float32) * deviation * gain
    return jnp.minimum(jnp.maximum(values, -reach), reach).astype(kind)


def setup_inputs(seed: int = 0) -> dict:
    seeds = jax.random.split(jax.random.key(seed), 12)
    tokens = draw_tokens(jax.random.fold_in(seeds[11], 71), 0)
    lengths = draw_lengths(jax.random.fold_in(seeds[11], 71), 0)
    norm_gains = jnp.clip(1.0 + 0.15 * jax.random.normal(seeds[2], (LAYERS, D), jnp.float32), 0.25, 1.75)
    query_weight = scatter_about(seeds[3], (LAYERS, D, HEADS * HD), D ** -0.5, 0.09375, ((2, 8),))
    key_weight = scatter_about(seeds[4], (LAYERS, D, KVH * HD), D ** -0.5, 0.09375, ((2, 8),))
    value_weight = scatter_about(seeds[5], (LAYERS, D, KVH * HD), D ** -0.5, 0.09375, ((2, 8),))
    out_weight = scatter_about(seeds[6], (LAYERS, HEADS * HD, D), (HEADS * HD) ** -0.5, 0.09375, ((1, 8),))
    query_probe = scatter_about(seeds[7], (LAYERS, D, HEADS * HD), D ** -0.5, 0.09375, ((1, 4), (2, 8)))
    key_probe = scatter_about(seeds[8], (LAYERS, D, KVH * HD), D ** -0.5, 0.09375, ((1, 4), (2, 8)))
    value_probe = scatter_about(seeds[9], (LAYERS, D, KVH * HD), D ** -0.5, 0.09375, ((1, 4), (2, 8)))
    out_probe = scatter_about(seeds[10], (LAYERS, HEADS * HD, D), (HEADS * HD) ** -0.5, 0.09375, ((1, 8), (2, 4)))
    return dict(tokens=tokens, lengths=lengths, norm_gains=norm_gains, query_weight=query_weight, key_weight=key_weight, value_weight=value_weight, out_weight=out_weight, query_probe=query_probe, key_probe=key_probe, value_probe=value_probe, out_probe=out_probe)


EPS = 1e-05
THETA = 500000.0

def multiply(pattern, left_side, right_side):
    return jnp.einsum(pattern, left_side.astype(jnp.float32), right_side.astype(jnp.float32))

def matmul(left_side, right_side):
    return jnp.dot(left_side, right_side, preferred_element_type=jnp.float32)

def rope_tables(length, head_size):
    position = jnp.arange(length).astype(jnp.float32)
    column = jnp.arange(head_size // 2).astype(jnp.float32)
    frequency = jnp.exp(-math.log(THETA) * 2.0 * column / head_size)
    angles = position[:, None] * frequency[None, :]
    return (jnp.cos(angles), jnp.sin(angles))

def rotate(values, cosine_table, sine_table, direction):
    middle = values.shape[-1] // 2
    leading = values[..., :middle]
    trailing = values[..., middle:]
    cosine = cosine_table[None, :, None, :]
    sine_part = direction * sine_table[None, :, None, :]
    return jnp.concatenate([leading * cosine - trailing * sine_part, trailing * cosine + leading * sine_part], axis=-1)

def allowed_mask(size, length):
    row_index = jnp.arange(size)[:, None]
    column_index = jnp.arange(size)[None, :]
    return (column_index <= row_index) & (column_index < length)

def attend(queries, key_heads, value_heads, tangent_queries, tangent_keys, tangent_values, length):
    repeat = queries.shape[1] // key_heads.shape[1]
    key_heads = jnp.repeat(key_heads, repeat, axis=1)
    value_heads = jnp.repeat(value_heads, repeat, axis=1)
    tangent_keys = jnp.repeat(tangent_keys, repeat, axis=1)
    tangent_values = jnp.repeat(tangent_values, repeat, axis=1)
    scaling = 1.0 / math.sqrt(queries.shape[-1])
    allowed = allowed_mask(queries.shape[0], length)[None]
    scores = multiply('ihd,jhd->hij', queries, key_heads) * scaling
    powers = jnp.where(allowed, jnp.exp(scores), 0.0)
    weights = powers / lax.optimization_barrier(jnp.sum(powers, axis=-1, keepdims=True))
    weights_low = weights.astype(jnp.bfloat16)
    blended = multiply('hij,jhd->ihd', weights_low, value_heads).astype(jnp.bfloat16)
    tangent_scores = (multiply('ihd,jhd->hij', tangent_queries, key_heads) + multiply('ihd,jhd->hij', queries, tangent_keys)) * scaling
    tangent_weights = weights * (tangent_scores - lax.optimization_barrier(jnp.sum(weights * tangent_scores, axis=-1, keepdims=True)))
    tangent_blended = multiply('hij,jhd->ihd', tangent_weights.astype(jnp.bfloat16), value_heads) + multiply('hij,jhd->ihd', weights_low, tangent_values)
    return (blended, tangent_blended.astype(jnp.bfloat16))

def attend_back(queries, key_heads, value_heads, grad_mixed, length):
    repeat = queries.shape[1] // key_heads.shape[1]
    key_heads = jnp.repeat(key_heads, repeat, axis=1)
    value_heads = jnp.repeat(value_heads, repeat, axis=1)
    scaling = 1.0 / math.sqrt(queries.shape[-1])
    allowed = allowed_mask(queries.shape[0], length)[None]
    scores = multiply('ihd,jhd->hij', queries, key_heads) * scaling
    powers = jnp.where(allowed, jnp.exp(scores), 0.0)
    weights = powers / lax.optimization_barrier(jnp.sum(powers, axis=-1, keepdims=True))
    weights_low = weights.astype(jnp.bfloat16)
    grad_weights = multiply('ihd,jhd->hij', grad_mixed, value_heads)
    grad_values = multiply('hij,ihd->jhd', weights_low, grad_mixed)
    grad_scores = (weights * (grad_weights - lax.optimization_barrier(jnp.sum(weights * grad_weights, axis=-1, keepdims=True))) * scaling).astype(jnp.bfloat16)
    grad_queries = multiply('hij,jhd->ihd', grad_scores, key_heads)
    grad_keys = multiply('hij,ihd->jhd', grad_scores, queries)
    return (grad_queries, grad_keys, grad_values)

def normalize(stream, gain_row):
    wide_stream = stream.astype(jnp.float32)
    inverse = lax.rsqrt(lax.optimization_barrier(jnp.mean(wide_stream * wide_stream, axis=-1, keepdims=True)) + EPS)
    return (wide_stream, inverse, (wide_stream * inverse * gain_row).astype(jnp.bfloat16))

def norm_tangent(wide_stream, inverse, tangent, gain_row):
    shift = lax.optimization_barrier(jnp.mean(wide_stream * tangent, axis=-1, keepdims=True))
    return (gain_row * (tangent * inverse - wide_stream * inverse * inverse * inverse * shift)).astype(jnp.bfloat16)

def norm_back(wide_stream, inverse, grad_normed, gain_row):
    scaled = grad_normed * gain_row
    shift = lax.optimization_barrier(jnp.mean(wide_stream * scaled, axis=-1, keepdims=True))
    return inverse * (scaled - wide_stream * inverse * inverse * shift)

def device_sum(left_terms, right_terms):

    def accumulate(running, pieces):
        partial_value = jnp.zeros_like(running)
        for left_side, right_side in zip(pieces[0], pieces[1]):
            partial_value = partial_value + matmul(left_side, right_side)
        return (running + lax.optimization_barrier(partial_value.astype(jnp.bfloat16)).astype(jnp.float32), None)
    start = jnp.zeros((left_terms[0].shape[1], right_terms[0].shape[2]), jnp.float32)
    running, unused = lax.scan(accumulate, start, (left_terms, right_terms))
    return running

def group_sum(function, arrays, shape):
    batches = tuple((member.reshape((N_DP, member.shape[0] // N_DP) + member.shape[1:]) for member in arrays))

    def accumulate(running, pieces):
        partial_value = function(*pieces)
        return (running + lax.optimization_barrier(partial_value.astype(jnp.bfloat16)).astype(jnp.float32), None)
    running, unused = lax.scan(accumulate, jnp.zeros(shape, jnp.float32), batches)
    return running

def transpose_product(left_side, right_side):
    return matmul(left_side.T, right_side)

def head_pairs(normed_piece, key_piece):
    per_group = multiply('td,tnc->ndc', normed_piece, key_piece)
    group_size = N_TENSOR // KVH
    summed = per_group.reshape(KVH, group_size, per_group.shape[1], per_group.shape[2]).sum(axis=1)
    return summed.transpose(1, 0, 2).reshape(per_group.shape[1], -1)

def reference(tokens, lengths, norm_gains, query_weight, key_weight, value_weight, out_weight, query_probe, key_probe, value_probe, out_probe):
    group_size = N_TENSOR // KVH
    per_device = HEADS // N_TENSOR
    cosine_table, sine_table = rope_tables(LEN, HD)
    token_count = lengths.shape[0] * LEN
    position = jnp.arange(token_count) % LEN
    row_mask = (position < jnp.repeat(lengths, LEN)).astype(jnp.float32)

    def heads_of(values, count):
        return values.reshape(-1, LEN, count, HD)

    def flatten(values):
        return values.reshape(token_count, -1)

    def split_devices(values, columns):
        return values.reshape(token_count, N_TENSOR, columns).transpose(1, 0, 2)
    stream = tokens
    tangent = None
    stored = []
    for layer_index in range(LAYERS):
        gain_row = norm_gains[layer_index].astype(jnp.float32)
        wide_stream, inverse, normed = normalize(stream, gain_row)
        query_primal = matmul(normed, query_weight[layer_index])
        key_primal = matmul(normed, key_weight[layer_index])
        value_primal = matmul(normed, value_weight[layer_index])
        query_moved = matmul(normed, query_probe[layer_index])
        key_moved = matmul(normed, key_probe[layer_index])
        value_moved = matmul(normed, value_probe[layer_index])
        if tangent is not None:
            tangent_normed = norm_tangent(wide_stream, inverse, tangent, gain_row)
            query_moved = query_moved + matmul(tangent_normed, query_weight[layer_index])
            key_moved = key_moved + matmul(tangent_normed, key_weight[layer_index])
            value_moved = value_moved + matmul(tangent_normed, value_weight[layer_index])
        queries = rotate(heads_of(query_primal, HEADS), cosine_table, sine_table, 1.0).astype(jnp.bfloat16)
        key_heads = rotate(heads_of(key_primal, KVH), cosine_table, sine_table, 1.0).astype(jnp.bfloat16)
        value_heads = heads_of(value_primal, KVH).astype(jnp.bfloat16)
        tangent_queries = rotate(heads_of(query_moved, HEADS), cosine_table, sine_table, 1.0).astype(jnp.bfloat16)
        tangent_keys = rotate(heads_of(key_moved, KVH), cosine_table, sine_table, 1.0).astype(jnp.bfloat16)
        tangent_values = heads_of(value_moved, KVH).astype(jnp.bfloat16)
        blended, tangent_blended = lax.map(lambda pieces: attend(*pieces), (queries, key_heads, value_heads, tangent_queries, tangent_keys, tangent_values, lengths))
        blended = flatten(blended)
        tangent_blended = flatten(tangent_blended)
        out_split = out_weight[layer_index].reshape(N_TENSOR, per_device * HD, D)
        probe_split = out_probe[layer_index].reshape(N_TENSOR, per_device * HD, D)
        blended_split = split_devices(blended, per_device * HD)
        tangent_out = device_sum((split_devices(tangent_blended, per_device * HD), blended_split), (out_split, probe_split))
        stored.append((wide_stream, inverse, normed, queries, key_heads, value_heads, blended))
        if layer_index < LAYERS - 1:
            primal_out = device_sum((blended_split,), (out_split,))
            stream = (wide_stream + primal_out).astype(jnp.bfloat16)
        tangent = tangent_out if tangent is None else tangent + tangent_out
    cotangent = row_mask[:, None] * tangent
    query_products = [None] * LAYERS
    key_products = [None] * LAYERS
    value_products = [None] * LAYERS
    out_products = [None] * LAYERS
    for layer_index in reversed(range(LAYERS)):
        wide_stream, inverse, normed, queries, key_heads, value_heads, blended = stored[layer_index]
        cotangent_low = cotangent.astype(jnp.bfloat16)
        out_products[layer_index] = group_sum(transpose_product, (blended, cotangent_low), (HEADS * HD, D))
        grad_mixed = matmul(cotangent_low, out_weight[layer_index].T).astype(jnp.bfloat16)
        grad_queries, grad_keys, grad_values = lax.map(lambda pieces: attend_back(*pieces), (queries, key_heads, value_heads, heads_of(grad_mixed, HEADS), lengths))
        query_low = flatten(rotate(grad_queries, cosine_table, sine_table, -1.0).astype(jnp.bfloat16))
        key_grouped = grad_keys.reshape(-1, LEN, N_TENSOR, per_device, HD).sum(axis=3)
        key_low = rotate(key_grouped, cosine_table, sine_table, -1.0).astype(jnp.bfloat16).reshape(token_count, N_TENSOR, HD)
        value_low = grad_values.reshape(-1, LEN, N_TENSOR, per_device, HD).sum(axis=3).astype(jnp.bfloat16).reshape(token_count, N_TENSOR, HD)
        query_products[layer_index] = group_sum(transpose_product, (normed, query_low), (D, HEADS * HD))
        key_products[layer_index] = group_sum(head_pairs, (normed, key_low), (D, KVH * HD))
        value_products[layer_index] = group_sum(head_pairs, (normed, value_low), (D, KVH * HD))
        if layer_index > 0:
            key_split = jnp.repeat(key_weight[layer_index].reshape(D, KVH, HD).transpose(1, 2, 0), group_size, axis=0)
            value_split = jnp.repeat(value_weight[layer_index].reshape(D, KVH, HD).transpose(1, 2, 0), group_size, axis=0)
            query_split = query_weight[layer_index].T.reshape(N_TENSOR, per_device * HD, D)
            grad_normed = device_sum((split_devices(query_low, per_device * HD), key_low.transpose(1, 0, 2), value_low.transpose(1, 0, 2)), (query_split, key_split, value_split))
            cotangent = cotangent + norm_back(wide_stream, inverse, grad_normed, norm_gains[layer_index].astype(jnp.float32))
    return (jnp.stack(query_products), jnp.stack(key_products), jnp.stack(value_products), jnp.stack(out_products))
```

```python
import functools
import math

import jax
import jax.numpy as jnp
from jax import lax
from jax.experimental import pallas as pl
from jax.experimental.pallas import tpu as pltpu
from jax.sharding import PartitionSpec as P

HD = 128
LEN = 256
EPS = 1e-05
THETA = 500000.0
MESH = pl.DeviceIdType.MESH
SCALE = 1.0 / math.sqrt(HD)


def low(values):
    return values.astype(jnp.bfloat16)


def wide(values):
    return values.astype(jnp.float32)


def matmul(left_side, right_side):
    return jnp.dot(left_side, right_side, preferred_element_type=jnp.float32)


def contract_rows(left_side, right_side):
    return lax.dot_general(
        left_side, right_side, (((0,), (0,)), ((), ())), preferred_element_type=jnp.float32
    )


def contract_last(left_side, right_side):
    return lax.dot_general(
        left_side, right_side, (((1,), (1,)), ((), ())), preferred_element_type=jnp.float32
    )


def rope_tables(length, head_size):
    position = jnp.arange(length).astype(jnp.float32)
    column = jnp.arange(head_size // 2).astype(jnp.float32)
    frequency = jnp.exp(-math.log(THETA) * 2.0 * column / head_size)
    angles = position[:, None] * frequency[None, :]
    cosine, sine = jnp.cos(angles), jnp.sin(angles)
    return (
        jnp.concatenate([cosine, cosine], axis=-1),
        jnp.concatenate([-sine, sine], axis=-1),
    )


def flip(index, mask):
    result = index
    bit = 1
    while bit <= mask:
        if mask & bit:
            result = result + bit - 2 * bit * lax.rem(lax.div(index, bit), 2)
        bit *= 2
    return result


def semaphore_count(sizes):
    batches, width = sizes
    return 4 * width + 3 * batches


class Fabric:
    def __init__(self, sizes, send, recv):
        self.batches, self.width = sizes
        self.chips = self.width // 2
        self.row = lax.axis_index("dp")
        self.col = lax.axis_index("tensor")
        self.send, self.recv, self.used = send, recv, 0
        self.pending = []

    def copy(self, source, target, row, col):
        number = self.used
        self.used += 1
        assert number < semaphore_count((self.batches, self.width))
        made = pltpu.make_async_remote_copy(
            src_ref=source,
            dst_ref=target,
            send_sem=self.send.at[number],
            recv_sem=self.recv.at[number],
            device_id=(row, col),
            device_id_type=MESH,
        )
        made.start()
        self.pending.append(made)
        return made

    def drain(self):
        for made in self.pending:
            made.wait_send()

    def mate(self):
        return flip(self.col, 1)

    def peer(self, step):
        return flip(self.col, 2 * step)

    def batch(self, step):
        return flip(self.row, step)

    def greet(self, along_tensor=True):
        barrier = pltpu.get_barrier_semaphore()
        peers = [(self.batch(step), self.col) for step in range(1, self.batches)]
        if along_tensor:
            peers += [(self.row, self.peer(step)) for step in range(1, self.chips)]
            peers.append((self.row, self.mate()))
        for peer in peers:
            pl.semaphore_signal(barrier, inc=1, device_id=peer, device_id_type=MESH)
        return lambda: pl.semaphore_wait(barrier, len(peers))

    def gather(self, source, slot):
        there = slot(self.col)
        direct = [
            self.copy(source, there, self.row, self.peer(step)) for step in range(1, self.chips)
        ]
        beside = [self.copy(source, there, self.row, self.mate())]
        there[...] = source[...]

        def forward():
            for step in range(1, self.chips):
                direct[step - 1].wait_recv()
                piece = slot(self.peer(step))
                beside.append(self.copy(piece, piece, self.row, self.mate()))

        def finish():
            for made in beside:
                made.wait_recv()

        return forward, finish

    def pair_up(self, slot, beside):
        return [
            self.copy(slot(flip(self.mate(), 2 * step)), beside.at[step], self.row, self.mate())
            for step in range(self.chips)
        ]

    def spread(self, slot, copies, beside, summed, landed):
        sent = []
        order = list(range(self.chips - 1, 0, -1))
        for place, step in enumerate(order):
            copies[step].wait_recv()
            summed[step] = low(wide(slot(self.peer(step))[...]) + wide(beside[step]))
            if place:
                last = order[place - 1]
                sent.append(
                    self.copy(summed.at[last], landed.at[last], self.row, self.peer(last))
                )
        copies[0].wait_recv()
        total = wide(slot(self.col)[...]) + wide(beside[0])
        if order:
            last = order[-1]
            sent.append(self.copy(summed.at[last], landed.at[last], self.row, self.peer(last)))

        def finish():
            result = total
            for made, step in zip(sent, order):
                made.wait_recv()
                result = result + wide(landed[step])
            return result

        return finish

    def exchange(self, source, target):
        made = [
            self.copy(
                source.at[self.batch(step)], target.at[self.row], self.batch(step), self.col
            )
            for step in range(1, self.batches)
        ]
        target[self.row] = source[self.row]

        def finish():
            for copy in made:
                copy.wait_recv()

        return finish

    def scatter_batch(self, source, landed, steps):
        return [
            self.copy(
                source.at[self.batch(step)], landed.at[step], self.batch(step), self.col
            )
            for step in steps
        ]

    def gather_batch(self, source, target):
        made = [
            self.copy(source, target.at[self.row], self.batch(step), self.col)
            for step in range(1, self.batches)
        ]
        target[self.row] = source[...]
        return made


def inverse_of(stream):
    return lax.rsqrt(jnp.mean(stream * stream, axis=-1, keepdims=True) + EPS)


def set_shard(values, shard, pieces):
    rounded = low(values)
    shard[...] = rounded
    block = pieces.shape[-1]
    for number in range(pieces.shape[0]):
        pieces[number] = rounded[:, number * block : (number + 1) * block]


def gather_both(fabric, shard, pieces, exchanged, whole, blocks):
    arrived = fabric.exchange(pieces, exchanged)
    forward, finish = fabric.gather(shard, lambda col: whole.at[col])
    arrived()
    forward_blocks, finish_blocks = fabric.gather(exchanged, lambda col: blocks.at[:, col])
    forward()
    forward_blocks()
    finish()
    finish_blocks()


def add_landed(own, landed, copies, steps):
    total = wide(own)
    for made, step in zip(copies, steps):
        made.wait_recv()
        total = total + wide(landed[step])
    return total


def open_kernel(sizes, tokens, gain, whole, blocks, shard, pieces, exchanged, send, recv):
    fabric = Fabric(sizes, send, recv)
    ready = fabric.greet()
    stream = wide(tokens[...])
    set_shard(stream * inverse_of(stream) * gain[...], shard, pieces)
    ready()
    gather_both(fabric, shard, pieces, exchanged, whole, blocks)
    fabric.drain()


def second_kernel(
    sizes,
    terms,
    tokens,
    gain,
    partial,
    blended,
    stream_out,
    whole,
    blocks,
    moved,
    blended_all,
    beside,
    summed,
    landed,
    shard,
    pieces,
    exchanged,
    returned,
    send,
    recv,
):
    fabric = Fabric(sizes, send, recv)
    fabric.greet()()
    slot = lambda col: terms.at[col]
    paired = fabric.pair_up(slot, beside)
    steps = list(range(1, fabric.batches))
    back = fabric.scatter_batch(partial, returned, steps)
    total = fabric.spread(slot, paired, beside, summed, landed)()
    rounded = low(wide(tokens[...]) + total)
    stream_out[...] = rounded
    stream = wide(rounded)
    set_shard(stream * inverse_of(stream) * gain[...], shard, pieces)
    gather_both(fabric, shard, pieces, exchanged, whole, blocks)
    fetched = fabric.gather_batch(blended, blended_all)
    moved[...] = add_landed(partial[fabric.row], returned, back, steps)
    for made in fetched:
        made.wait_recv()
    fabric.drain()


def tangent_total(fabric, terms, probed, beside, summed, landed, probe_bufs, pieces, exchanged):
    beside_p, summed_p, landed_p = probe_bufs
    slot = lambda col: terms.at[col]
    slot_p = lambda col: probed.at[:, col]
    paired_p = fabric.pair_up(slot_p, beside_p)
    paired = fabric.pair_up(slot, beside)
    finish_p = fabric.spread(slot_p, paired_p, beside_p, summed_p, landed_p)
    finish = fabric.spread(slot, paired, beside, summed, landed)
    pieces[...] = low(finish_p())
    total = finish()
    fabric.exchange(pieces, exchanged)()
    block = pieces.shape[-1]
    return [
        total[:, number * block : (number + 1) * block] + wide(exchanged[number])
        for number in range(fabric.batches)
    ]


def third_kernel(
    sizes,
    terms,
    probed,
    stream_in,
    gain,
    partial,
    blended,
    tangent,
    whole,
    moved,
    blended_all,
    beside,
    summed,
    landed,
    beside_p,
    summed_p,
    landed_p,
    shard,
    pieces,
    exchanged,
    returned,
    send,
    recv,
):
    fabric = Fabric(sizes, send, recv)
    fabric.greet()()
    steps = list(range(1, fabric.batches))
    early = steps[: (len(steps) + 1) // 2]
    back = fabric.scatter_batch(partial, returned, early)
    parts = tangent_total(
        fabric, terms, probed, beside, summed, landed, (beside_p, summed_p, landed_p),
        pieces, exchanged,
    )
    back += fabric.scatter_batch(partial, returned, steps[len(early) :])
    change = jnp.concatenate(parts, axis=-1)
    tangent[...] = change
    stream = wide(stream_in[...])
    inverse = inverse_of(stream)
    shift = jnp.mean(stream * change, axis=-1, keepdims=True)
    shard[...] = low(
        gain[...] * (change * inverse - stream * inverse * inverse * inverse * shift)
    )
    fetched = fabric.gather_batch(blended, blended_all)
    forward, finish = fabric.gather(shard, lambda col: whole.at[col])
    forward()
    finish()
    moved[...] = add_landed(partial[fabric.row], returned, back, steps)
    for made in fetched:
        made.wait_recv()
    fabric.drain()


def fourth_kernel(
    sizes,
    terms,
    probed,
    tangent,
    mask,
    cotangent,
    whole,
    blocks,
    beside,
    summed,
    landed,
    beside_p,
    summed_p,
    landed_p,
    shard,
    pieces,
    exchanged,
    pieces_p,
    exchanged_p,
    send,
    recv,
):
    fabric = Fabric(sizes, send, recv)
    fabric.greet()()
    parts = tangent_total(
        fabric, terms, probed, beside, summed, landed, (beside_p, summed_p, landed_p),
        pieces_p, exchanged_p,
    )
    change = jnp.concatenate(parts, axis=-1)
    result = mask[...] * (tangent[...] + change)
    cotangent[...] = result
    set_shard(result, shard, pieces)
    gather_both(fabric, shard, pieces, exchanged, whole, blocks)
    fabric.drain()


def fifth_kernel(
    sizes,
    terms,
    stream_in,
    gain,
    cotangent,
    grads,
    cotangent_out,
    whole,
    blocks,
    grads_all,
    beside,
    summed,
    landed,
    shard,
    pieces,
    exchanged,
    send,
    recv,
):
    fabric = Fabric(sizes, send, recv)
    fabric.greet()()
    slot = lambda col: terms.at[col]
    paired = fabric.pair_up(slot, beside)
    total = fabric.spread(slot, paired, beside, summed, landed)()
    stream = wide(stream_in[...])
    inverse = inverse_of(stream)
    scaled = total * gain[...]
    shift = jnp.mean(stream * scaled, axis=-1, keepdims=True)
    result = cotangent[...] + inverse * (scaled - stream * inverse * inverse * shift)
    cotangent_out[...] = result
    set_shard(result, shard, pieces)
    gather_both(fabric, shard, pieces, exchanged, whole, blocks)
    fetched = fabric.gather_batch(grads, grads_all)
    for made in fetched:
        made.wait_recv()
    fabric.drain()


def last_kernel(sizes, grads, grads_all, send, recv):
    fabric = Fabric(sizes, send, recv)
    fabric.greet(along_tensor=False)()
    for made in fabric.gather_batch(grads, grads_all):
        made.wait_recv()
    fabric.drain()


def communicate(kernel, sizes, number, inputs, outputs, scratch):
    vmem = pl.BlockSpec(memory_space=pltpu.VMEM)
    return pl.pallas_call(
        functools.partial(kernel, sizes),
        out_shape=[jax.ShapeDtypeStruct(shape, kind) for shape, kind in outputs],
        in_specs=[vmem] * len(inputs),
        out_specs=[vmem] * len(outputs),
        scratch_shapes=[pltpu.VMEM(shape, jnp.bfloat16) for shape in scratch]
        + [pltpu.SemaphoreType.DMA((semaphore_count(sizes),))] * 2,
        compiler_params=pltpu.CompilerParams(collective_id=number, has_side_effects=True),
    )(*inputs)


def turn(values, cosine, sine, direction):
    other = pltpu.roll(values, HD // 2, 1)
    if direction > 0:
        return values * cosine + other * sine
    return values * cosine - other * sine


def head(index):
    return slice(index * HD, (index + 1) * HD)


def allowed_keys(length):
    row_index = lax.broadcasted_iota(jnp.int32, (LEN, LEN), 0)
    column_index = lax.broadcasted_iota(jnp.int32, (LEN, LEN), 1)
    return (column_index <= row_index) & (column_index < length)


def softmax_weights(queries, keys, allowed):
    powers = jnp.where(allowed, jnp.exp(contract_last(queries, keys) * SCALE), 0.0)
    return powers / jnp.sum(powers, axis=-1, keepdims=True)


def centred(weights, values):
    return weights * (values - jnp.sum(weights * values, axis=-1, keepdims=True))


def each_head(total_rows, query_width, key_width):
    repeat = query_width // key_width
    for seq in range(total_rows // LEN):
        rows = slice(seq * LEN, (seq + 1) * LEN)
        for number in range(key_width // HD):
            yield seq, rows, number, range(number * repeat, (number + 1) * repeat)


def primal_kernel(
    steps,
    with_out,
    lengths,
    normed,
    query_weight,
    key_weight,
    value_weight,
    blocks,
    query_probe,
    key_probe,
    value_probe,
    cosine,
    sine,
    *rest,
):
    if with_out:
        out_weight, queries, keys, values, blended, partial, out, acc_q, acc_k, acc_v = rest
    else:
        queries, keys, values, blended, partial, acc_q, acc_k, acc_v = rest
    step = pl.program_id(0)

    @pl.when(step == 0)
    def _():
        acc_q[...] = jnp.zeros_like(acc_q)
        acc_k[...] = jnp.zeros_like(acc_k)
        acc_v[...] = jnp.zeros_like(acc_v)

    @pl.when(step < steps)
    def _():
        part = normed[...]
        acc_q[...] += matmul(part, query_weight[0])
        acc_k[...] += matmul(part, key_weight[0])
        acc_v[...] += matmul(part, value_weight[0])
        rows = blocks[...]
        query_width = query_probe.shape[-1]
        partial[:, :query_width] = low(matmul(rows, query_probe[0]))
        partial[:, query_width:] = low(
            jnp.concatenate([matmul(rows, key_probe[0]), matmul(rows, value_probe[0])], axis=-1)
        )

    @pl.when(step == steps - 1)
    def _():
        values[...] = low(acc_v[...])
        total_rows, query_width = queries.shape
        for seq, rows, number, members in each_head(total_rows, query_width, keys.shape[1]):
            allowed = allowed_keys(lengths[seq])
            key_head = low(turn(acc_k[rows, head(number)], cosine[...], sine[...], 1))
            keys[rows, head(number)] = key_head
            value_head = low(acc_v[rows, head(number)])
            for member in members:
                query_head = low(turn(acc_q[rows, head(member)], cosine[...], sine[...], 1))
                queries[rows, head(member)] = query_head
                weights = low(softmax_weights(query_head, key_head, allowed))
                blended[rows, head(member)] = low(matmul(weights, value_head))

    if with_out:

        @pl.when(step >= steps)
        def _():
            out[...] = low(matmul(blended[...], out_weight[0]))


def tangent_kernel(
    steps,
    with_tangent,
    lengths,
    queries,
    keys,
    values,
    moved,
    cosine,
    sine,
    out_weight,
    blended_all,
    out_probe,
    *rest,
):
    if with_tangent:
        tangent, query_weight, key_weight, value_weight, terms, probed, acc, mixed = rest
    else:
        terms, probed, acc, mixed = rest
    step = pl.program_id(0)
    query_width, key_width = queries.shape[1], keys.shape[1]

    @pl.when(step == 0)
    def _():
        acc[...] = moved[...]

    if with_tangent:

        @pl.when(step < steps)
        def _():
            part = tangent[...]
            acc[:, :query_width] += matmul(part, query_weight[0])
            acc[:, query_width : query_width + key_width] += matmul(part, key_weight[0])
            acc[:, query_width + key_width :] += matmul(part, value_weight[0])

    @pl.when(step == steps - 1)
    def _():
        for seq, rows, number, members in each_head(queries.shape[0], query_width, key_width):
            allowed = allowed_keys(lengths[seq])
            key_head = keys[rows, head(number)]
            value_head = values[rows, head(number)]
            key_at = query_width // HD + number
            value_at = key_at + key_width // HD
            moved_key = low(turn(acc[rows, head(key_at)], cosine[...], sine[...], 1))
            moved_value = low(acc[rows, head(value_at)])
            for member in members:
                query_head = queries[rows, head(member)]
                moved_query = low(turn(acc[rows, head(member)], cosine[...], sine[...], 1))
                weights = softmax_weights(query_head, key_head, allowed)
                scores = SCALE * (
                    contract_last(moved_query, key_head) + contract_last(query_head, moved_key)
                )
                moved_weights = low(centred(weights, scores))
                mixed[rows, head(member)] = low(
                    matmul(moved_weights, value_head) + matmul(low(weights), moved_value)
                )

    @pl.when(step >= steps)
    def _():
        terms[...] = low(matmul(mixed[...], out_weight[0]))
        probed[...] = low(matmul(blended_all[...], out_probe[0]))


def backward_kernel(
    steps,
    with_grad,
    lengths,
    cotangent,
    out_weight,
    queries,
    keys,
    values,
    cosine,
    sine,
    *rest,
):
    if with_grad:
        query_weight, key_weight, value_weight, grads, terms, acc = rest
    else:
        grads, acc = rest
    step = pl.program_id(0)
    query_width, key_width = queries.shape[1], keys.shape[1]

    @pl.when(step == 0)
    def _():
        acc[...] = jnp.zeros_like(acc)

    @pl.when(step < steps)
    def _():
        acc[...] += contract_last(cotangent[...], out_weight[0])

    @pl.when(step == steps - 1)
    def _():
        for seq, rows, number, members in each_head(queries.shape[0], query_width, key_width):
            allowed = allowed_keys(lengths[seq])
            key_head = keys[rows, head(number)]
            value_head = values[rows, head(number)]
            key_at = query_width // HD + number
            value_at = key_at + key_width // HD
            key_total = jnp.zeros((LEN, HD), jnp.float32)
            value_total = jnp.zeros((LEN, HD), jnp.float32)
            for member in members:
                query_head = queries[rows, head(member)]
                mixed = low(acc[rows, head(member)])
                weights = softmax_weights(query_head, key_head, allowed)
                value_total = value_total + contract_rows(low(weights), mixed)
                scores = low(centred(weights, contract_last(mixed, value_head)) * SCALE)
                grads[rows, head(member)] = low(
                    turn(matmul(scores, key_head), cosine[...], sine[...], -1)
                )
                key_total = key_total + contract_rows(scores, query_head)
            grads[rows, head(key_at)] = low(turn(key_total, cosine[...], sine[...], -1))
            grads[rows, head(value_at)] = low(value_total)

    if with_grad:

        @pl.when(step >= steps)
        def _():
            terms[...] = low(
                contract_last(grads[:, :query_width], query_weight[0])
                + contract_last(grads[:, query_width : query_width + key_width], key_weight[0])
                + contract_last(grads[:, query_width + key_width :], value_weight[0])
            )


def product_kernel(layers, *refs):
    inputs, (query_out, key_out, value_out, out_out) = refs[:-4], refs[-4:]
    layer = pl.program_id(0)
    query_width, key_width = query_out.shape[-1], key_out.shape[-1]
    for number in range(layers):
        blocks, grads, blended, cotangent = inputs[4 * number : 4 * number + 4]

        @pl.when(layer == number)
        def _():
            product = contract_rows(blocks[...], grads[...])
            query_out[0] = product[:, :query_width]
            key_out[0] = product[:, query_width : query_width + key_width]
            value_out[0] = product[:, query_width + key_width :]
            out_out[0] = contract_rows(blended[...], cotangent[...])


CUTS = 4
FULL = None


def body(
    tokens,
    lengths,
    norm_gains,
    query_weight,
    key_weight,
    value_weight,
    out_weight,
    query_probe,
    key_probe,
    value_probe,
    out_probe,
):
    width = lax.axis_size("tensor")
    batches = lax.axis_size("dp")
    sizes = (batches, width)
    tensor_index = lax.axis_index("tensor")
    data_index = lax.axis_index("dp")
    share, model = tokens.shape
    group = share * width
    seq_count = group // LEN
    layers = query_weight.shape[0]
    assert layers == 2
    half_width = key_weight.shape[2]
    query_width = query_weight.shape[2]
    paired = half_width < HD
    key_width = 2 * half_width if paired else half_width
    sent_width = query_width + 2 * half_width
    block = query_probe.shape[1]
    chips = width // 2
    bf, f32 = jnp.bfloat16, jnp.float32
    cosine, sine = rope_tables(LEN, HD)
    group_lengths = lax.dynamic_slice_in_dim(lengths, data_index * seq_count, seq_count)
    position = tensor_index * share + jnp.arange(share)
    row_mask = wide(position % LEN < group_lengths[position // LEN])[:, None]
    lower_half = tensor_index % 2 == 0

    def swapped(value):
        pairs = [(source, source ^ 1) for source in range(width)]
        return lax.ppermute(value, "tensor", pairs)

    def join_halves(own_part):
        other_part = swapped(own_part)
        return jnp.where(
            lower_half,
            jnp.concatenate([own_part, other_part], axis=-1),
            jnp.concatenate([other_part, own_part], axis=-1),
        )

    def split_halves(values):
        first, second = values[:, :half_width], values[:, half_width:]
        own_part = jnp.where(lower_half, first, second)
        other_part = jnp.where(lower_half, second, first)
        return low(wide(own_part) + wide(swapped(other_part)))

    if paired:
        key_full, value_full = join_halves(key_weight), join_halves(value_weight)
    else:
        key_full, value_full = key_weight, value_weight

    def join_moved(moved):
        if not paired:
            return moved
        return jnp.concatenate(
            [
                moved[:, :query_width],
                join_halves(moved[:, query_width : query_width + half_width]),
                join_halves(moved[:, query_width + half_width :]),
            ],
            axis=-1,
        )

    def to_send(grads):
        if not paired:
            return grads
        return jnp.concatenate(
            [
                grads[:, :query_width],
                split_halves(grads[:, query_width : query_width + key_width]),
                split_halves(grads[:, query_width + key_width :]),
            ],
            axis=-1,
        )

    whole_shape = ((width, share, model), bf)
    blocks_shape = ((batches, width, share, block), bf)
    shard_shape = (share, model)
    pieces_shape = (batches, share, block)
    sum_shape = (chips, share, model)
    probe_shape = (chips, batches, share, block)
    back_shape = (batches, group, sent_width)
    rows_in_all = batches * group
    gains = [norm_gains[number][None] for number in range(layers)]
    cut = model // CUTS
    rows_cut = rows_in_all // CUTS

    def spec(shape, index):
        return pl.BlockSpec(shape, index)

    def fixed(shape):
        return pl.BlockSpec(shape, lambda i: (0,) * len(shape))

    def first_part(i):
        return jnp.minimum(i, CUTS - 1)

    def late_part(start):
        return lambda i: jnp.maximum(i - start, 0)

    smem = pl.BlockSpec(memory_space=pltpu.SMEM)
    table = fixed((LEN, HD))
    arbitrary = pltpu.CompilerParams(dimension_semantics=("arbitrary",))

    def cost(flops, moved_bytes):
        return pl.CostEstimate(flops=flops, bytes_accessed=moved_bytes, transcendentals=0)

    def weight_specs(layer, place):
        return [
            spec((1, cut, query_width), lambda i: (layer, place(i), 0)),
            spec((1, cut, key_width), lambda i: (layer, place(i), 0)),
            spec((1, cut, key_width), lambda i: (layer, place(i), 0)),
        ]

    def primal(layer, normed_all, blocks):
        with_out = layer < layers - 1
        late = late_part(CUTS)
        in_specs = [
            smem,
            spec((group, cut), lambda i: (0, first_part(i))),
            *weight_specs(layer, first_part),
            spec((rows_cut, block), lambda i: (first_part(i), 0)),
            spec((1, block, query_width), lambda i: (layer, 0, 0)),
            spec((1, block, half_width), lambda i: (layer, 0, 0)),
            spec((1, block, half_width), lambda i: (layer, 0, 0)),
            table,
            table,
        ]
        out_shape = [
            ((group, query_width), bf),
            ((group, key_width), bf),
            ((group, key_width), bf),
            ((group, query_width), bf),
            ((rows_in_all, sent_width), bf),
        ]
        out_specs = [
            fixed((group, query_width)),
            fixed((group, key_width)),
            fixed((group, key_width)),
            fixed((group, query_width)),
            spec((rows_cut, sent_width), lambda i: (first_part(i), 0)),
        ]
        args = [
            group_lengths,
            normed_all,
            query_weight,
            key_full,
            value_full,
            blocks,
            query_probe,
            key_probe,
            value_probe,
            cosine,
            sine,
        ]
        if with_out:
            in_specs.append(spec((1, query_width, cut), lambda i: (layer, 0, late(i))))
            args.append(out_weight)
            out_shape.append(((group, model), bf))
            out_specs.append(spec((group, cut), lambda i: (0, late(i))))
        return pl.pallas_call(
            functools.partial(primal_kernel, CUTS, with_out),
            grid=(CUTS * (2 if with_out else 1),),
            in_specs=in_specs,
            out_specs=out_specs,
            out_shape=[jax.ShapeDtypeStruct(shape, kind) for shape, kind in out_shape],
            scratch_shapes=[
                pltpu.VMEM((group, query_width), f32),
                pltpu.VMEM((group, key_width), f32),
                pltpu.VMEM((group, key_width), f32),
            ],
            compiler_params=arbitrary,
            cost_estimate=cost(2 * group * model * query_width * 3, 16 << 20),
        )(*args)

    def moved_on(layer, kept, moved, blended_all, tangent_all):
        with_tangent = tangent_all is not None
        steps = CUTS if with_tangent else 1
        late = late_part(steps)
        queries, keys, values = kept
        in_specs = [
            smem,
            fixed(queries.shape),
            fixed(keys.shape),
            fixed(values.shape),
            fixed(moved.shape),
            table,
            table,
            spec((1, query_width, cut), lambda i: (layer, 0, late(i))),
            spec((rows_cut, query_width), lambda i: (late(i), 0)),
            spec((1, query_width, block), lambda i: (layer, 0, 0)),
        ]
        args = [
            group_lengths,
            queries,
            keys,
            values,
            moved,
            cosine,
            sine,
            out_weight,
            blended_all.reshape(rows_in_all, query_width),
            out_probe,
        ]
        if with_tangent:
            in_specs += [
                spec((group, cut), lambda i: (0, first_part(i))),
                *weight_specs(layer, first_part),
            ]
            args += [tangent_all.reshape(group, model), query_weight, key_full, value_full]
        return pl.pallas_call(
            functools.partial(tangent_kernel, steps, with_tangent),
            grid=(steps + CUTS,),
            in_specs=in_specs,
            out_specs=[
                spec((group, cut), lambda i: (0, late(i))),
                spec((rows_cut, block), lambda i: (late(i), 0)),
            ],
            out_shape=[
                jax.ShapeDtypeStruct((group, model), bf),
                jax.ShapeDtypeStruct((rows_in_all, block), bf),
            ],
            scratch_shapes=[
                pltpu.VMEM(moved.shape, f32),
                pltpu.VMEM((group, query_width), bf),
            ],
            compiler_params=arbitrary,
            cost_estimate=cost(2 * group * model * query_width * 3, 16 << 20),
        )(*args)

    def backward(layer, cotangent_all, kept):
        with_grad = layer > 0
        late = late_part(CUTS)
        queries, keys, values = kept
        sent = query_width + 2 * key_width
        in_specs = [
            smem,
            spec((group, cut), lambda i: (0, first_part(i))),
            spec((1, query_width, cut), lambda i: (layer, 0, first_part(i))),
            fixed(queries.shape),
            fixed(keys.shape),
            fixed(values.shape),
            table,
            table,
        ]
        args = [
            group_lengths,
            cotangent_all.reshape(group, model),
            out_weight,
            queries,
            keys,
            values,
            cosine,
            sine,
        ]
        out_shape = [jax.ShapeDtypeStruct((group, sent), bf)]
        out_specs = [fixed((group, sent))]
        if with_grad:
            in_specs += weight_specs(layer, late)
            args += [query_weight, key_full, value_full]
            out_shape.append(jax.ShapeDtypeStruct((group, model), bf))
            out_specs.append(spec((group, cut), lambda i: (0, late(i))))
        return pl.pallas_call(
            functools.partial(backward_kernel, CUTS, with_grad),
            grid=(CUTS * (2 if with_grad else 1),),
            in_specs=in_specs,
            out_specs=out_specs,
            out_shape=out_shape,
            scratch_shapes=[pltpu.VMEM((group, query_width), f32)],
            compiler_params=arbitrary,
            cost_estimate=cost(2 * group * model * query_width * 3, 16 << 20),
        )(*args)

    def products(per_layer):
        out_block = out_probe.shape[2]
        by_rows = query_width % (CUTS * HD) == 0
        blended_cut = query_width // CUTS if by_rows else query_width
        out_cut = out_block if by_rows else out_block // CUTS
        in_specs, args = [], []
        for number, (blocks, grads, blended, cotangents) in enumerate(per_layer):

            def place(i, j, number=number):
                return (0, jnp.clip((i - number) * CUTS + j, 0, CUTS - 1))

            def still(i, j):
                return (0, 0)

            in_specs += [
                pl.BlockSpec((rows_in_all, block // CUTS), place),
                pl.BlockSpec((rows_in_all, sent_width), still),
                pl.BlockSpec((rows_in_all, blended_cut), place if by_rows else still),
                pl.BlockSpec((rows_in_all, out_cut), still if by_rows else place),
            ]
            args += [
                blocks.reshape(rows_in_all, block),
                grads.reshape(rows_in_all, sent_width),
                blended.reshape(rows_in_all, query_width),
                cotangents.reshape(rows_in_all, out_block),
            ]
        shapes = [
            (block, query_width),
            (block, half_width),
            (block, half_width),
            (query_width, out_block),
        ]
        return pl.pallas_call(
            functools.partial(product_kernel, layers),
            grid=(layers, CUTS),
            in_specs=in_specs,
            out_specs=[
                pl.BlockSpec((1, rows // CUTS, columns), lambda i, j: (i, j, 0))
                for rows, columns in shapes[:3]
            ]
            + [
                pl.BlockSpec(
                    (1, blended_cut, out_cut),
                    lambda i, j: (i, j, 0) if by_rows else (i, 0, j),
                )
            ],
            out_shape=[
                jax.ShapeDtypeStruct((layers, rows, columns), f32) for rows, columns in shapes
            ],
            compiler_params=pltpu.CompilerParams(
                dimension_semantics=("arbitrary", "arbitrary")
            ),
            cost_estimate=cost(2 * rows_in_all * block * query_width * 4, 32 << 20),
        )(*args)

    slots = (width, share, model)
    probe_slots = (batches, width, share, block)

    whole0, blocks0 = communicate(
        open_kernel,
        sizes,
        0,
        [tokens, gains[0]],
        [whole_shape, blocks_shape],
        [shard_shape, pieces_shape, pieces_shape],
    )
    queries, keys, values, blended0, partial, out = primal(
        0, whole0.reshape(group, model), blocks0.reshape(rows_in_all, block)
    )
    kept0 = (queries, keys, values)
    stream1, whole1, blocks1, moved, blended_all0 = communicate(
        second_kernel,
        sizes,
        1,
        [out.reshape(slots), tokens, gains[1], partial.reshape(back_shape), blended0],
        [
            (shard_shape, bf),
            whole_shape,
            blocks_shape,
            ((group, sent_width), f32),
            ((batches, group, query_width), bf),
        ],
        [sum_shape, sum_shape, sum_shape, shard_shape, pieces_shape, pieces_shape, back_shape],
    )
    terms, probed = moved_on(0, kept0, join_moved(moved), blended_all0, None)
    queries, keys, values, blended1, partial = primal(
        1, whole1.reshape(group, model), blocks1.reshape(rows_in_all, block)
    )
    kept1 = (queries, keys, values)
    sums = [sum_shape, sum_shape, sum_shape, probe_shape, probe_shape, probe_shape]
    tangent, tangent_all, moved, blended_all1 = communicate(
        third_kernel,
        sizes,
        2,
        [
            terms.reshape(slots),
            probed.reshape(probe_slots),
            stream1,
            gains[1],
            partial.reshape(back_shape),
            blended1,
        ],
        [
            (shard_shape, f32),
            whole_shape,
            ((group, sent_width), f32),
            ((batches, group, query_width), bf),
        ],
        sums + [shard_shape, pieces_shape, pieces_shape, back_shape],
    )
    terms, probed = moved_on(1, kept1, join_moved(moved), blended_all1, tangent_all)
    cotangent, cotangent_all, cotangents1 = communicate(
        fourth_kernel,
        sizes,
        3,
        [terms.reshape(slots), probed.reshape(probe_slots), tangent, row_mask],
        [(shard_shape, f32), whole_shape, blocks_shape],
        sums + [shard_shape, pieces_shape, pieces_shape, pieces_shape, pieces_shape],
    )
    grads1, terms = backward(1, cotangent_all, kept1)
    _, cotangent_all, cotangents0, grads_all1 = communicate(
        fifth_kernel,
        sizes,
        4,
        [terms.reshape(slots), stream1, gains[1], cotangent, to_send(grads1)],
        [
            (shard_shape, f32),
            whole_shape,
            blocks_shape,
            ((batches, group, sent_width), bf),
        ],
        [sum_shape, sum_shape, sum_shape, shard_shape, pieces_shape, pieces_shape],
    )
    (grads0,) = backward(0, cotangent_all, kept0)
    (grads_all0,) = communicate(
        last_kernel,
        sizes,
        5,
        [to_send(grads0)],
        [((batches, group, sent_width), bf)],
        [],
    )
    return tuple(
        products(
            [
                (blocks0, grads_all0, blended_all0, cotangents0),
                (blocks1, grads_all1, blended_all1, cotangents1),
            ]
        )
    )


def solution(mesh):
    placed = (
        P(("dp", "tensor"), None),
        P(),
        P(),
        P(None, None, "tensor"),
        P(None, None, "tensor"),
        P(None, None, "tensor"),
        P(None, "tensor", None),
        P(None, "dp", "tensor"),
        P(None, "dp", "tensor"),
        P(None, "dp", "tensor"),
        P(None, "tensor", "dp"),
    )
    return jax.shard_map(
        body,
        mesh=mesh,
        in_specs=placed,
        out_specs=(
            P(None, "dp", "tensor"),
            P(None, "dp", "tensor"),
            P(None, "dp", "tensor"),
            P(None, "tensor", "dp"),
        ),
        check_vma=False,
    )
```

```python
import functools
import math

import jax
import jax.numpy as jnp
from jax import lax
from jax.experimental import pallas as pl
from jax.experimental.pallas import tpu as pltpu
from jax.sharding import PartitionSpec as P

HD = 128
LEN = 256
EPS = 1e-05
THETA = 500000.0
MESH = pl.DeviceIdType.MESH
SCALE = 1.0 / math.sqrt(HD)


def low(values):
    return values.astype(jnp.bfloat16)


def wide(values):
    return values.astype(jnp.float32)


def matmul(left_side, right_side):
    return jnp.dot(left_side, right_side, preferred_element_type=jnp.float32)


def contract_rows(left_side, right_side):
    return lax.dot_general(
        left_side, right_side, (((0,), (0,)), ((), ())), preferred_element_type=jnp.float32
    )


def contract_last(left_side, right_side):
    return lax.dot_general(
        left_side, right_side, (((1,), (1,)), ((), ())), preferred_element_type=jnp.float32
    )


def rope_tables(length, head_size):
    position = jnp.arange(length).astype(jnp.float32)
    column = jnp.arange(head_size // 2).astype(jnp.float32)
    frequency = jnp.exp(-math.log(THETA) * 2.0 * column / head_size)
    angles = position[:, None] * frequency[None, :]
    cosine, sine = jnp.cos(angles), jnp.sin(angles)
    return (
        jnp.concatenate([cosine, cosine], axis=-1),
        jnp.concatenate([-sine, sine], axis=-1),
    )


def flip(index, mask):
    result = index
    bit = 1
    while bit <= mask:
        if mask & bit:
            result = result + bit - 2 * bit * lax.rem(lax.div(index, bit), 2)
        bit *= 2
    return result


def semaphore_count(sizes):
    batches, width = sizes
    return 4 * width + 6 * batches


class Fabric:
    def __init__(self, sizes, send, recv):
        self.batches, self.width = sizes
        self.chips = self.width // 2
        self.row = lax.axis_index("dp")
        self.col = lax.axis_index("tensor")
        self.send, self.recv, self.used = send, recv, 0
        self.pending = []
        self.guarded = []

    def copy(self, source, target, row, col):
        number = self.used
        self.used += 1
        assert number < semaphore_count((self.batches, self.width))
        made = pltpu.make_async_remote_copy(
            src_ref=source,
            dst_ref=target,
            send_sem=self.send.at[number],
            recv_sem=self.recv.at[number],
            device_id=(row, col),
            device_id_type=MESH,
        )
        made.start()
        self.pending.append(made)
        return made

    def drain(self):
        for made in self.pending:
            made.wait_send()
        for condition, made in self.guarded:
            pl.when(condition)(made.wait_send)

    def mate(self):
        return flip(self.col, 1)

    def peer(self, step):
        return flip(self.col, 2 * step)

    def batch(self, step):
        return flip(self.row, step)

    def greet(self, along_tensor=True):
        barrier = pltpu.get_barrier_semaphore()
        peers = [(self.batch(step), self.col) for step in range(1, self.batches)]
        if along_tensor:
            peers += [(self.row, self.peer(step)) for step in range(1, self.chips)]
            peers.append((self.row, self.mate()))
        for peer in peers:
            pl.semaphore_signal(barrier, inc=1, device_id=peer, device_id_type=MESH)
        return lambda: pl.semaphore_wait(barrier, len(peers))

    def gather(self, source, slot):
        there = slot(self.col)
        direct = [
            self.copy(source, there, self.row, self.peer(step)) for step in range(1, self.chips)
        ]
        beside = [self.copy(source, there, self.row, self.mate())]
        there[...] = source[...]

        def forward():
            for step in range(1, self.chips):
                direct[step - 1].wait_recv()
                piece = slot(self.peer(step))
                beside.append(self.copy(piece, piece, self.row, self.mate()))

        def finish():
            for made in beside:
                made.wait_recv()

        return forward, finish

    def pair_up(self, slot, beside):
        return [
            self.copy(slot(flip(self.mate(), 2 * step)), beside.at[step], self.row, self.mate())
            for step in range(self.chips)
        ]

    def spread(self, slot, copies, beside, summed, landed):
        sent = []
        order = list(range(self.chips - 1, 0, -1))
        for place, step in enumerate(order):
            copies[step].wait_recv()
            summed[step] = low(wide(slot(self.peer(step))[...]) + wide(beside[step]))
            if place:
                last = order[place - 1]
                sent.append(
                    self.copy(summed.at[last], landed.at[last], self.row, self.peer(last))
                )
        copies[0].wait_recv()
        total = wide(slot(self.col)[...]) + wide(beside[0])
        if order:
            last = order[-1]
            sent.append(self.copy(summed.at[last], landed.at[last], self.row, self.peer(last)))

        def finish():
            result = total
            for made, step in zip(sent, order):
                made.wait_recv()
                result = result + wide(landed[step])
            return result

        return finish

    def exchange(self, source, target):
        made = [
            self.copy(
                source.at[self.batch(step)], target.at[self.row], self.batch(step), self.col
            )
            for step in range(1, self.batches)
        ]
        target[self.row] = source[self.row]

        def finish():
            for copy in made:
                copy.wait_recv()

        return finish

    def reserve(self, count):
        first = self.used
        self.used += count
        assert self.used <= semaphore_count((self.batches, self.width))
        return first

    def hop(self, source, target, number, way):
        return pltpu.make_async_remote_copy(
            src_ref=source,
            dst_ref=target,
            send_sem=self.send.at[number],
            recv_sem=self.recv.at[number],
            device_id=(jnp.clip(self.row + way, 0, self.batches - 1), self.col),
            device_id_type=MESH,
        )

    def rank(self, way):
        return self.row if way > 0 else self.batches - 1 - self.row


class GatherChain:
    def __init__(self, fabric, source, target):
        self.fabric, self.source, self.target = fabric, source, target
        self.first = fabric.reserve(2 * (fabric.batches - 1))
        target[fabric.row] = source[...]

    def number(self, way, step):
        return self.first + (0 if way > 0 else self.fabric.batches - 1) + step - 1

    def arrive(self, step):
        fabric = self.fabric
        for way in (1, -1):
            piece = jnp.clip(fabric.row - way * step, 0, fabric.batches - 1)
            made = fabric.hop(
                self.target.at[piece], self.target.at[piece], self.number(way, step), way
            )
            pl.when(fabric.rank(way) >= step)(made.wait_recv)

    def step(self, step):
        fabric = self.fabric
        if step > 1:
            self.arrive(step - 1)
        for way in (1, -1):
            piece = jnp.clip(fabric.row - way * (step - 1), 0, fabric.batches - 1)
            source = self.source if step == 1 else self.target.at[piece]
            made = fabric.hop(source, self.target.at[piece], self.number(way, step), way)
            rank = fabric.rank(way)
            condition = (rank >= step - 1) & (rank < fabric.batches - 1)
            pl.when(condition)(made.start)
            fabric.guarded.append((condition, made))

    def finish(self):
        self.arrive(self.fabric.batches - 1)


class ScatterChain:
    def __init__(self, fabric, source, landed, leaving):
        self.fabric, self.source = fabric, source
        self.landed, self.leaving = landed, leaving
        self.first = fabric.reserve(2 * (fabric.batches - 1))

    def hop(self, source, way, step):
        side = 0 if way > 0 else 1
        number = self.first + side * (self.fabric.batches - 1) + step - 1
        return self.fabric.hop(source, self.landed.at[side, step - 1], number, way)

    def step(self, step):
        fabric = self.fabric
        last = fabric.batches - 1
        for way in (1, -1):
            side = 0 if way > 0 else 1
            rank = fabric.rank(way)
            goal = jnp.clip(fabric.batches + rank - step, 0, last)
            goal = goal if way > 0 else last - goal
            own = self.hop(self.source.at[goal], way, step)
            pl.when(rank == 0)(own.start)
            fabric.guarded.append((rank == 0, own))
            if step > 1:
                buffer = self.leaving.at[side, step - 1]
                summed = self.hop(buffer, way, step)
                before = self.hop(buffer, way, step - 1)
                condition = (rank > 0) & (rank < step)

                @pl.when(condition)
                def _():
                    before.wait_recv()
                    buffer[...] = low(
                        wide(self.source[goal]) + wide(self.landed[side, step - 2])
                    )
                    summed.start()

                fabric.guarded.append((condition, summed))

    def finish(self, total):
        fabric = self.fabric
        last = fabric.batches - 1
        total[...] = wide(self.source[fabric.row])
        for way in (1, -1):
            side = 0 if way > 0 else 1
            made = self.hop(self.source.at[fabric.row], way, last)

            @pl.when(fabric.rank(way) > 0)
            def _():
                made.wait_recv()
                total[...] += wide(self.landed[side, last - 1])


def inverse_of(stream):
    return lax.rsqrt(jnp.mean(stream * stream, axis=-1, keepdims=True) + EPS)


def set_shard(values, shard, pieces):
    rounded = low(values)
    shard[...] = rounded
    block = pieces.shape[-1]
    for number in range(pieces.shape[0]):
        pieces[number] = rounded[:, number * block : (number + 1) * block]


def open_kernel(sizes, tokens, gain, whole, blocks, shard, pieces, exchanged, send, recv):
    fabric = Fabric(sizes, send, recv)
    ready = fabric.greet()
    stream = wide(tokens[...])
    set_shard(stream * inverse_of(stream) * gain[...], shard, pieces)
    ready()
    arrived = fabric.exchange(pieces, exchanged)
    forward, finish = fabric.gather(shard, lambda col: whole.at[col])
    arrived()
    forward_blocks, finish_blocks = fabric.gather(exchanged, lambda col: blocks.at[:, col])
    forward()
    forward_blocks()
    finish()
    finish_blocks()
    fabric.drain()


def second_kernel(
    sizes,
    terms,
    tokens,
    gain,
    partial,
    blended,
    stream_out,
    whole,
    blocks,
    moved,
    blended_all,
    beside,
    summed,
    landed,
    shard,
    pieces,
    exchanged,
    returned,
    leaving,
    send,
    recv,
):
    fabric = Fabric(sizes, send, recv)
    back = ScatterChain(fabric, partial, returned, leaving)
    fetch = GatherChain(fabric, blended, blended_all)
    fabric.greet()()
    slot = lambda col: terms.at[col]
    paired = fabric.pair_up(slot, beside)
    back.step(1)
    fetch.step(1)
    total = fabric.spread(slot, paired, beside, summed, landed)()
    rounded = low(wide(tokens[...]) + total)
    stream_out[...] = rounded
    stream = wide(rounded)
    set_shard(stream * inverse_of(stream) * gain[...], shard, pieces)
    arrived = fabric.exchange(pieces, exchanged)
    forward, finish = fabric.gather(shard, lambda col: whole.at[col])
    steps = list(range(2, fabric.batches))
    for step in steps[:-1]:
        back.step(step)
        fetch.step(step)
    arrived()
    forward_blocks, finish_blocks = fabric.gather(exchanged, lambda col: blocks.at[:, col])
    forward()
    for step in steps[-1:]:
        back.step(step)
        fetch.step(step)
    forward_blocks()
    finish()
    finish_blocks()
    back.finish(moved)
    fetch.finish()
    fabric.drain()


def third_kernel(
    sizes,
    terms,
    probed,
    stream_in,
    gain,
    partial,
    blended,
    tangent,
    whole,
    moved,
    blended_all,
    beside,
    summed,
    landed,
    beside_p,
    summed_p,
    landed_p,
    shard,
    pieces,
    exchanged,
    returned,
    leaving,
    send,
    recv,
):
    fabric = Fabric(sizes, send, recv)
    back = ScatterChain(fabric, partial, returned, leaving)
    fetch = GatherChain(fabric, blended, blended_all)
    fabric.greet()()
    slot = lambda col: terms.at[col]
    slot_p = lambda col: probed.at[:, col]
    paired_p = fabric.pair_up(slot_p, beside_p)
    paired = fabric.pair_up(slot, beside)
    back.step(1)
    fetch.step(1)
    finish_p = fabric.spread(slot_p, paired_p, beside_p, summed_p, landed_p)
    finish = fabric.spread(slot, paired, beside, summed, landed)
    pieces[...] = low(finish_p())
    arrived = fabric.exchange(pieces, exchanged)
    steps = list(range(2, fabric.batches))
    for step in steps[:-1]:
        back.step(step)
        fetch.step(step)
    change = joined(finish(), arrived, exchanged)
    tangent[...] = change
    stream = wide(stream_in[...])
    inverse = inverse_of(stream)
    shift = jnp.mean(stream * change, axis=-1, keepdims=True)
    shard[...] = low(
        gain[...] * (change * inverse - stream * inverse * inverse * inverse * shift)
    )
    forward, finish = fabric.gather(shard, lambda col: whole.at[col])
    for step in steps[-1:]:
        back.step(step)
        fetch.step(step)
    forward()
    finish()
    back.finish(moved)
    fetch.finish()
    fabric.drain()


def joined(total, arrived, exchanged):
    arrived()
    block = exchanged.shape[-1]
    return jnp.concatenate(
        [
            total[:, number * block : (number + 1) * block] + wide(exchanged[number])
            for number in range(exchanged.shape[0])
        ],
        axis=-1,
    )


def fourth_kernel(
    sizes,
    terms,
    probed,
    tangent,
    mask,
    cotangent,
    whole,
    pieces_out,
    beside,
    summed,
    landed,
    beside_p,
    summed_p,
    landed_p,
    shard,
    pieces,
    exchanged,
    send,
    recv,
):
    fabric = Fabric(sizes, send, recv)
    fabric.greet()()
    slot = lambda col: terms.at[col]
    slot_p = lambda col: probed.at[:, col]
    paired_p = fabric.pair_up(slot_p, beside_p)
    paired = fabric.pair_up(slot, beside)
    finish_p = fabric.spread(slot_p, paired_p, beside_p, summed_p, landed_p)
    finish = fabric.spread(slot, paired, beside, summed, landed)
    pieces[...] = low(finish_p())
    arrived = fabric.exchange(pieces, exchanged)
    change = joined(finish(), arrived, exchanged)
    result = mask[...] * (tangent[...] + change)
    cotangent[...] = result
    set_shard(result, shard, pieces_out)
    forward, finish = fabric.gather(shard, lambda col: whole.at[col])
    forward()
    finish()
    fabric.drain()


def fifth_kernel(
    sizes,
    terms,
    stream_in,
    gain,
    cotangent,
    grads,
    pieces_in,
    whole,
    blocks,
    grads_all,
    pieces_out,
    beside,
    summed,
    landed,
    shard,
    exchanged,
    send,
    recv,
):
    fabric = Fabric(sizes, send, recv)
    fetch = GatherChain(fabric, grads, grads_all)
    fabric.greet()()
    slot = lambda col: terms.at[col]
    paired = fabric.pair_up(slot, beside)
    arrived = fabric.exchange(pieces_in, exchanged)
    fetch.step(1)
    total = fabric.spread(slot, paired, beside, summed, landed)()
    stream = wide(stream_in[...])
    inverse = inverse_of(stream)
    scaled = total * gain[...]
    shift = jnp.mean(stream * scaled, axis=-1, keepdims=True)
    result = cotangent[...] + inverse * (scaled - stream * inverse * inverse * shift)
    set_shard(result, shard, pieces_out)
    forward, finish = fabric.gather(shard, lambda col: whole.at[col])
    arrived()
    forward_blocks, finish_blocks = fabric.gather(exchanged, lambda col: blocks.at[:, col])
    steps = list(range(2, fabric.batches))
    for step in steps[:-1]:
        fetch.step(step)
    forward()
    for step in steps[-1:]:
        fetch.step(step)
    forward_blocks()
    finish()
    finish_blocks()
    fetch.finish()
    fabric.drain()


def last_kernel(sizes, grads, pieces_in, grads_all, blocks, exchanged, send, recv):
    fabric = Fabric(sizes, send, recv)
    fetch = GatherChain(fabric, grads, grads_all)
    fabric.greet()()
    arrived = fabric.exchange(pieces_in, exchanged)
    fetch.step(1)
    arrived()
    forward_blocks, finish_blocks = fabric.gather(exchanged, lambda col: blocks.at[:, col])
    steps = list(range(2, fabric.batches))
    for step in steps[:-1]:
        fetch.step(step)
    forward_blocks()
    for step in steps[-1:]:
        fetch.step(step)
    finish_blocks()
    fetch.finish()
    fabric.drain()


def communicate(kernel, sizes, number, inputs, outputs, scratch):
    vmem = pl.BlockSpec(memory_space=pltpu.VMEM)
    return pl.pallas_call(
        functools.partial(kernel, sizes),
        out_shape=[jax.ShapeDtypeStruct(shape, kind) for shape, kind in outputs],
        in_specs=[vmem] * len(inputs),
        out_specs=[vmem] * len(outputs),
        scratch_shapes=[pltpu.VMEM(shape, jnp.bfloat16) for shape in scratch]
        + [pltpu.SemaphoreType.DMA((semaphore_count(sizes),))] * 2,
        compiler_params=pltpu.CompilerParams(collective_id=number, has_side_effects=True),
    )(*inputs)


def turn(values, cosine, sine, direction):
    other = pltpu.roll(values, HD // 2, 1)
    if direction > 0:
        return values * cosine + other * sine
    return values * cosine - other * sine


def head(index):
    return slice(index * HD, (index + 1) * HD)


def allowed_keys(length):
    row_index = lax.broadcasted_iota(jnp.int32, (LEN, LEN), 0)
    column_index = lax.broadcasted_iota(jnp.int32, (LEN, LEN), 1)
    return (column_index <= row_index) & (column_index < length)


def softmax_weights(queries, keys, allowed):
    powers = jnp.where(allowed, jnp.exp(contract_last(queries, keys) * SCALE), 0.0)
    return powers / jnp.sum(powers, axis=-1, keepdims=True)


def centred(weights, values):
    return weights * (values - jnp.sum(weights * values, axis=-1, keepdims=True))


def each_head(total_rows, query_width, key_width):
    repeat = query_width // key_width
    for seq in range(total_rows // LEN):
        rows = slice(seq * LEN, (seq + 1) * LEN)
        for number in range(key_width // HD):
            yield seq, rows, number, range(number * repeat, (number + 1) * repeat)


def primal_kernel(
    steps,
    with_out,
    lengths,
    normed,
    query_weight,
    key_weight,
    value_weight,
    blocks,
    query_probe,
    key_probe,
    value_probe,
    cosine,
    sine,
    *rest,
):
    if with_out:
        out_weight, queries, keys, values, blended, partial, out, acc_q, acc_k, acc_v = rest
    else:
        queries, keys, values, blended, partial, acc_q, acc_k, acc_v = rest
    step = pl.program_id(0)

    @pl.when(step == 0)
    def _():
        acc_q[...] = jnp.zeros_like(acc_q)
        acc_k[...] = jnp.zeros_like(acc_k)
        acc_v[...] = jnp.zeros_like(acc_v)

    @pl.when(step < steps)
    def _():
        part = normed[...]
        acc_q[...] += matmul(part, query_weight[0])
        acc_k[...] += matmul(part, key_weight[0])
        acc_v[...] += matmul(part, value_weight[0])
        rows = blocks[...]
        query_width = query_probe.shape[-1]
        partial[:, :query_width] = low(matmul(rows, query_probe[0]))
        partial[:, query_width:] = low(
            jnp.concatenate([matmul(rows, key_probe[0]), matmul(rows, value_probe[0])], axis=-1)
        )

    @pl.when(step == steps - 1)
    def _():
        values[...] = low(acc_v[...])
        total_rows, query_width = queries.shape
        for seq, rows, number, members in each_head(total_rows, query_width, keys.shape[1]):
            allowed = allowed_keys(lengths[seq])
            key_head = low(turn(acc_k[rows, head(number)], cosine[...], sine[...], 1))
            keys[rows, head(number)] = key_head
            value_head = low(acc_v[rows, head(number)])
            for member in members:
                query_head = low(turn(acc_q[rows, head(member)], cosine[...], sine[...], 1))
                queries[rows, head(member)] = query_head
                weights = low(softmax_weights(query_head, key_head, allowed))
                blended[rows, head(member)] = low(matmul(weights, value_head))

    if with_out:

        @pl.when(step >= steps)
        def _():
            out[...] = low(matmul(blended[...], out_weight[0]))


def tangent_kernel(
    steps,
    with_tangent,
    lengths,
    queries,
    keys,
    values,
    moved,
    cosine,
    sine,
    out_weight,
    blended_all,
    out_probe,
    *rest,
):
    if with_tangent:
        tangent, query_weight, key_weight, value_weight, terms, probed, acc, mixed = rest
    else:
        terms, probed, acc, mixed = rest
    step = pl.program_id(0)
    query_width, key_width = queries.shape[1], keys.shape[1]

    @pl.when(step == 0)
    def _():
        acc[...] = moved[...]

    if with_tangent:

        @pl.when(step < steps)
        def _():
            part = tangent[...]
            acc[:, :query_width] += matmul(part, query_weight[0])
            acc[:, query_width : query_width + key_width] += matmul(part, key_weight[0])
            acc[:, query_width + key_width :] += matmul(part, value_weight[0])

    @pl.when(step == steps - 1)
    def _():
        for seq, rows, number, members in each_head(queries.shape[0], query_width, key_width):
            allowed = allowed_keys(lengths[seq])
            key_head = keys[rows, head(number)]
            value_head = values[rows, head(number)]
            key_at = query_width // HD + number
            value_at = key_at + key_width // HD
            moved_key = low(turn(acc[rows, head(key_at)], cosine[...], sine[...], 1))
            moved_value = low(acc[rows, head(value_at)])
            for member in members:
                query_head = queries[rows, head(member)]
                moved_query = low(turn(acc[rows, head(member)], cosine[...], sine[...], 1))
                weights = softmax_weights(query_head, key_head, allowed)
                scores = SCALE * (
                    contract_last(moved_query, key_head) + contract_last(query_head, moved_key)
                )
                moved_weights = low(centred(weights, scores))
                mixed[rows, head(member)] = low(
                    matmul(moved_weights, value_head) + matmul(low(weights), moved_value)
                )

    @pl.when(step >= steps)
    def _():
        terms[...] = low(matmul(mixed[...], out_weight[0]))
        probed[...] = low(matmul(blended_all[...], out_probe[0]))


def backward_kernel(
    steps,
    with_grad,
    lengths,
    cotangent,
    out_weight,
    queries,
    keys,
    values,
    cosine,
    sine,
    *rest,
):
    if with_grad:
        query_weight, key_weight, value_weight, grads, terms, acc = rest
    else:
        grads, acc = rest
    step = pl.program_id(0)
    query_width, key_width = queries.shape[1], keys.shape[1]

    @pl.when(step == 0)
    def _():
        acc[...] = jnp.zeros_like(acc)

    @pl.when(step < steps)
    def _():
        acc[...] += contract_last(cotangent[...], out_weight[0])

    @pl.when(step == steps - 1)
    def _():
        for seq, rows, number, members in each_head(queries.shape[0], query_width, key_width):
            allowed = allowed_keys(lengths[seq])
            key_head = keys[rows, head(number)]
            value_head = values[rows, head(number)]
            key_at = query_width // HD + number
            value_at = key_at + key_width // HD
            key_total = jnp.zeros((LEN, HD), jnp.float32)
            value_total = jnp.zeros((LEN, HD), jnp.float32)
            for member in members:
                query_head = queries[rows, head(member)]
                mixed = low(acc[rows, head(member)])
                weights = softmax_weights(query_head, key_head, allowed)
                value_total = value_total + contract_rows(low(weights), mixed)
                scores = low(centred(weights, contract_last(mixed, value_head)) * SCALE)
                grads[rows, head(member)] = low(
                    turn(matmul(scores, key_head), cosine[...], sine[...], -1)
                )
                key_total = key_total + contract_rows(scores, query_head)
            grads[rows, head(key_at)] = low(turn(key_total, cosine[...], sine[...], -1))
            grads[rows, head(value_at)] = low(value_total)

    if with_grad:

        @pl.when(step >= steps)
        def _():
            terms[...] = low(
                contract_last(grads[:, :query_width], query_weight[0])
                + contract_last(grads[:, query_width : query_width + key_width], key_weight[0])
                + contract_last(grads[:, query_width + key_width :], value_weight[0])
            )


def product_kernel(layers, *refs):
    inputs, (query_out, key_out, value_out, out_out) = refs[:-4], refs[-4:]
    layer = pl.program_id(0)
    query_width, key_width = query_out.shape[-1], key_out.shape[-1]
    for number in range(layers):
        blocks, grads, blended, cotangent = inputs[4 * number : 4 * number + 4]

        @pl.when(layer == number)
        def _():
            product = contract_rows(blocks[...], grads[...])
            query_out[0] = product[:, :query_width]
            key_out[0] = product[:, query_width : query_width + key_width]
            value_out[0] = product[:, query_width + key_width :]
            out_out[0] = contract_rows(blended[...], cotangent[...])


CUTS = 4
FULL = None


def body(
    tokens,
    lengths,
    norm_gains,
    query_weight,
    key_weight,
    value_weight,
    out_weight,
    query_probe,
    key_probe,
    value_probe,
    out_probe,
):
    width = lax.axis_size("tensor")
    batches = lax.axis_size("dp")
    sizes = (batches, width)
    tensor_index = lax.axis_index("tensor")
    data_index = lax.axis_index("dp")
    share, model = tokens.shape
    group = share * width
    seq_count = group // LEN
    layers = query_weight.shape[0]
    assert layers == 2
    half_width = key_weight.shape[2]
    query_width = query_weight.shape[2]
    paired = half_width < HD
    key_width = 2 * half_width if paired else half_width
    sent_width = query_width + 2 * half_width
    block = query_probe.shape[1]
    chips = width // 2
    bf, f32 = jnp.bfloat16, jnp.float32
    cosine, sine = rope_tables(LEN, HD)
    group_lengths = lax.dynamic_slice_in_dim(lengths, data_index * seq_count, seq_count)
    position = tensor_index * share + jnp.arange(share)
    row_mask = wide(position % LEN < group_lengths[position // LEN])[:, None]
    lower_half = tensor_index % 2 == 0

    def swapped(value):
        pairs = [(source, source ^ 1) for source in range(width)]
        return lax.ppermute(value, "tensor", pairs)

    def join_halves(own_part):
        other_part = swapped(own_part)
        return jnp.where(
            lower_half,
            jnp.concatenate([own_part, other_part], axis=-1),
            jnp.concatenate([other_part, own_part], axis=-1),
        )

    def split_halves(values):
        first, second = values[:, :half_width], values[:, half_width:]
        own_part = jnp.where(lower_half, first, second)
        other_part = jnp.where(lower_half, second, first)
        return low(wide(own_part) + wide(swapped(other_part)))

    if paired:
        key_full, value_full = join_halves(key_weight), join_halves(value_weight)
    else:
        key_full, value_full = key_weight, value_weight

    def join_moved(moved):
        if not paired:
            return moved
        return jnp.concatenate(
            [
                moved[:, :query_width],
                join_halves(moved[:, query_width : query_width + half_width]),
                join_halves(moved[:, query_width + half_width :]),
            ],
            axis=-1,
        )

    def to_send(grads):
        if not paired:
            return grads
        return jnp.concatenate(
            [
                grads[:, :query_width],
                split_halves(grads[:, query_width : query_width + key_width]),
                split_halves(grads[:, query_width + key_width :]),
            ],
            axis=-1,
        )

    whole_shape = ((width, share, model), bf)
    blocks_shape = ((batches, width, share, block), bf)
    shard_shape = (share, model)
    pieces_shape = (batches, share, block)
    sum_shape = (chips, share, model)
    probe_shape = (chips, batches, share, block)
    back_shape = (batches, group, sent_width)
    chain_shape = (2, batches - 1, group, sent_width)
    rows_in_all = batches * group
    gains = [norm_gains[number][None] for number in range(layers)]
    cut = model // CUTS
    rows_cut = rows_in_all // CUTS

    def spec(shape, index):
        return pl.BlockSpec(shape, index)

    def fixed(shape):
        return pl.BlockSpec(shape, lambda i: (0,) * len(shape))

    def first_part(i):
        return jnp.minimum(i, CUTS - 1)

    def late_part(start):
        return lambda i: jnp.maximum(i - start, 0)

    smem = pl.BlockSpec(memory_space=pltpu.SMEM)
    table = fixed((LEN, HD))
    arbitrary = pltpu.CompilerParams(dimension_semantics=("arbitrary",))

    def cost(flops, moved_bytes):
        return pl.CostEstimate(flops=flops, bytes_accessed=moved_bytes, transcendentals=0)

    def weight_specs(layer, place):
        return [
            spec((1, cut, query_width), lambda i: (layer, place(i), 0)),
            spec((1, cut, key_width), lambda i: (layer, place(i), 0)),
            spec((1, cut, key_width), lambda i: (layer, place(i), 0)),
        ]

    def primal(layer, normed_all, blocks):
        with_out = layer < layers - 1
        late = late_part(CUTS)
        in_specs = [
            smem,
            spec((group, cut), lambda i: (0, first_part(i))),
            *weight_specs(layer, first_part),
            spec((rows_cut, block), lambda i: (first_part(i), 0)),
            spec((1, block, query_width), lambda i: (layer, 0, 0)),
            spec((1, block, half_width), lambda i: (layer, 0, 0)),
            spec((1, block, half_width), lambda i: (layer, 0, 0)),
            table,
            table,
        ]
        out_shape = [
            ((group, query_width), bf),
            ((group, key_width), bf),
            ((group, key_width), bf),
            ((group, query_width), bf),
            ((rows_in_all, sent_width), bf),
        ]
        out_specs = [
            fixed((group, query_width)),
            fixed((group, key_width)),
            fixed((group, key_width)),
            fixed((group, query_width)),
            spec((rows_cut, sent_width), lambda i: (first_part(i), 0)),
        ]
        args = [
            group_lengths,
            normed_all,
            query_weight,
            key_full,
            value_full,
            blocks,
            query_probe,
            key_probe,
            value_probe,
            cosine,
            sine,
        ]
        if with_out:
            in_specs.append(spec((1, query_width, cut), lambda i: (layer, 0, late(i))))
            args.append(out_weight)
            out_shape.append(((group, model), bf))
            out_specs.append(spec((group, cut), lambda i: (0, late(i))))
        return pl.pallas_call(
            functools.partial(primal_kernel, CUTS, with_out),
            grid=(CUTS * (2 if with_out else 1),),
            in_specs=in_specs,
            out_specs=out_specs,
            out_shape=[jax.ShapeDtypeStruct(shape, kind) for shape, kind in out_shape],
            scratch_shapes=[
                pltpu.VMEM((group, query_width), f32),
                pltpu.VMEM((group, key_width), f32),
                pltpu.VMEM((group, key_width), f32),
            ],
            compiler_params=arbitrary,
            cost_estimate=cost(2 * group * model * query_width * 3, 16 << 20),
        )(*args)

    def moved_on(layer, kept, moved, blended_all, tangent_all):
        with_tangent = tangent_all is not None
        steps = CUTS if with_tangent else 1
        late = late_part(steps)
        queries, keys, values = kept
        in_specs = [
            smem,
            fixed(queries.shape),
            fixed(keys.shape),
            fixed(values.shape),
            fixed(moved.shape),
            table,
            table,
            spec((1, query_width, cut), lambda i: (layer, 0, late(i))),
            spec((rows_cut, query_width), lambda i: (late(i), 0)),
            spec((1, query_width, block), lambda i: (layer, 0, 0)),
        ]
        args = [
            group_lengths,
            queries,
            keys,
            values,
            moved,
            cosine,
            sine,
            out_weight,
            blended_all.reshape(rows_in_all, query_width),
            out_probe,
        ]
        if with_tangent:
            in_specs += [
                spec((group, cut), lambda i: (0, first_part(i))),
                *weight_specs(layer, first_part),
            ]
            args += [tangent_all.reshape(group, model), query_weight, key_full, value_full]
        return pl.pallas_call(
            functools.partial(tangent_kernel, steps, with_tangent),
            grid=(steps + CUTS,),
            in_specs=in_specs,
            out_specs=[
                spec((group, cut), lambda i: (0, late(i))),
                spec((rows_cut, block), lambda i: (late(i), 0)),
            ],
            out_shape=[
                jax.ShapeDtypeStruct((group, model), bf),
                jax.ShapeDtypeStruct((rows_in_all, block), bf),
            ],
            scratch_shapes=[
                pltpu.VMEM(moved.shape, f32),
                pltpu.VMEM((group, query_width), bf),
            ],
            compiler_params=arbitrary,
            cost_estimate=cost(2 * group * model * query_width * 3, 16 << 20),
        )(*args)

    def backward(layer, cotangent_all, kept):
        with_grad = layer > 0
        late = late_part(CUTS)
        queries, keys, values = kept
        sent = query_width + 2 * key_width
        in_specs = [
            smem,
            spec((group, cut), lambda i: (0, first_part(i))),
            spec((1, query_width, cut), lambda i: (layer, 0, first_part(i))),
            fixed(queries.shape),
            fixed(keys.shape),
            fixed(values.shape),
            table,
            table,
        ]
        args = [
            group_lengths,
            cotangent_all.reshape(group, model),
            out_weight,
            queries,
            keys,
            values,
            cosine,
            sine,
        ]
        out_shape = [jax.ShapeDtypeStruct((group, sent), bf)]
        out_specs = [fixed((group, sent))]
        if with_grad:
            in_specs += weight_specs(layer, late)
            args += [query_weight, key_full, value_full]
            out_shape.append(jax.ShapeDtypeStruct((group, model), bf))
            out_specs.append(spec((group, cut), lambda i: (0, late(i))))
        return pl.pallas_call(
            functools.partial(backward_kernel, CUTS, with_grad),
            grid=(CUTS * (2 if with_grad else 1),),
            in_specs=in_specs,
            out_specs=out_specs,
            out_shape=out_shape,
            scratch_shapes=[pltpu.VMEM((group, query_width), f32)],
            compiler_params=arbitrary,
            cost_estimate=cost(2 * group * model * query_width * 3, 16 << 20),
        )(*args)

    def products(per_layer):
        out_block = out_probe.shape[2]
        by_rows = query_width % (CUTS * HD) == 0
        blended_cut = query_width // CUTS if by_rows else query_width
        out_cut = out_block if by_rows else out_block // CUTS
        in_specs, args = [], []
        for number, (blocks, grads, blended, cotangents) in enumerate(per_layer):

            def place(i, j, number=number):
                return (0, jnp.clip((i - number) * CUTS + j, 0, CUTS - 1))

            def still(i, j):
                return (0, 0)

            in_specs += [
                pl.BlockSpec((rows_in_all, block // CUTS), place),
                pl.BlockSpec((rows_in_all, sent_width), still),
                pl.BlockSpec((rows_in_all, blended_cut), place if by_rows else still),
                pl.BlockSpec((rows_in_all, out_cut), still if by_rows else place),
            ]
            args += [
                blocks.reshape(rows_in_all, block),
                grads.reshape(rows_in_all, sent_width),
                blended.reshape(rows_in_all, query_width),
                cotangents.reshape(rows_in_all, out_block),
            ]
        shapes = [
            (block, query_width),
            (block, half_width),
            (block, half_width),
            (query_width, out_block),
        ]
        return pl.pallas_call(
            functools.partial(product_kernel, layers),
            grid=(layers, CUTS),
            in_specs=in_specs,
            out_specs=[
                pl.BlockSpec((1, rows // CUTS, columns), lambda i, j: (i, j, 0))
                for rows, columns in shapes[:3]
            ]
            + [
                pl.BlockSpec(
                    (1, blended_cut, out_cut),
                    lambda i, j: (i, j, 0) if by_rows else (i, 0, j),
                )
            ],
            out_shape=[
                jax.ShapeDtypeStruct((layers, rows, columns), f32) for rows, columns in shapes
            ],
            compiler_params=pltpu.CompilerParams(
                dimension_semantics=("arbitrary", "arbitrary")
            ),
            cost_estimate=cost(2 * rows_in_all * block * query_width * 4, 32 << 20),
        )(*args)

    slots = (width, share, model)
    probe_slots = (batches, width, share, block)

    whole0, blocks0 = communicate(
        open_kernel,
        sizes,
        0,
        [tokens, gains[0]],
        [whole_shape, blocks_shape],
        [shard_shape, pieces_shape, pieces_shape],
    )
    queries, keys, values, blended0, partial, out = primal(
        0, whole0.reshape(group, model), blocks0.reshape(rows_in_all, block)
    )
    kept0 = (queries, keys, values)
    stream1, whole1, blocks1, moved, blended_all0 = communicate(
        second_kernel,
        sizes,
        1,
        [out.reshape(slots), tokens, gains[1], partial.reshape(back_shape), blended0],
        [
            (shard_shape, bf),
            whole_shape,
            blocks_shape,
            ((group, sent_width), f32),
            ((batches, group, query_width), bf),
        ],
        [sum_shape, sum_shape, sum_shape, shard_shape, pieces_shape, pieces_shape, chain_shape, chain_shape],
    )
    terms, probed = moved_on(0, kept0, join_moved(moved), blended_all0, None)
    queries, keys, values, blended1, partial = primal(
        1, whole1.reshape(group, model), blocks1.reshape(rows_in_all, block)
    )
    kept1 = (queries, keys, values)
    sums = [sum_shape, sum_shape, sum_shape, probe_shape, probe_shape, probe_shape]
    tangent, tangent_all, moved, blended_all1 = communicate(
        third_kernel,
        sizes,
        2,
        [
            terms.reshape(slots),
            probed.reshape(probe_slots),
            stream1,
            gains[1],
            partial.reshape(back_shape),
            blended1,
        ],
        [
            (shard_shape, f32),
            whole_shape,
            ((group, sent_width), f32),
            ((batches, group, query_width), bf),
        ],
        sums + [shard_shape, pieces_shape, pieces_shape, chain_shape, chain_shape],
    )
    terms, probed = moved_on(1, kept1, join_moved(moved), blended_all1, tangent_all)
    cotangent, cotangent_all, cotangent_pieces = communicate(
        fourth_kernel,
        sizes,
        3,
        [terms.reshape(slots), probed.reshape(probe_slots), tangent, row_mask],
        [(shard_shape, f32), whole_shape, (pieces_shape, bf)],
        sums + [shard_shape, pieces_shape, pieces_shape],
    )
    grads1, terms = backward(1, cotangent_all, kept1)
    cotangent_all, cotangents1, grads_all1, cotangent_pieces = communicate(
        fifth_kernel,
        sizes,
        4,
        [
            terms.reshape(slots),
            stream1,
            gains[1],
            cotangent,
            to_send(grads1),
            cotangent_pieces,
        ],
        [
            whole_shape,
            blocks_shape,
            ((batches, group, sent_width), bf),
            (pieces_shape, bf),
        ],
        [sum_shape, sum_shape, sum_shape, shard_shape, pieces_shape],
    )
    (grads0,) = backward(0, cotangent_all, kept0)
    grads_all0, cotangents0 = communicate(
        last_kernel,
        sizes,
        5,
        [to_send(grads0), cotangent_pieces],
        [((batches, group, sent_width), bf), blocks_shape],
        [pieces_shape],
    )
    return tuple(
        products(
            [
                (blocks0, grads_all0, blended_all0, cotangents0),
                (blocks1, grads_all1, blended_all1, cotangents1),
            ]
        )
    )


def solution(mesh):
    placed = (
        P(("dp", "tensor"), None),
        P(),
        P(),
        P(None, None, "tensor"),
        P(None, None, "tensor"),
        P(None, None, "tensor"),
        P(None, "tensor", None),
        P(None, "dp", "tensor"),
        P(None, "dp", "tensor"),
        P(None, "dp", "tensor"),
        P(None, "tensor", "dp"),
    )
    return jax.shard_map(
        body,
        mesh=mesh,
        in_specs=placed,
        out_specs=(
            P(None, "dp", "tensor"),
            P(None, "dp", "tensor"),
            P(None, "dp", "tensor"),
            P(None, "tensor", "dp"),
        ),
        check_vma=False,
    )
```

```python
import functools
import math
import types

import jax
import jax.numpy as jnp
from jax import lax
from jax.experimental import pallas as pl
from jax.experimental.pallas import tpu as pltpu
from jax.sharding import PartitionSpec as P

HD = 128
LEN = 256
EPS = 1e-05
THETA = 500000.0
MESH = pl.DeviceIdType.MESH
SCALE = 1.0 / math.sqrt(HD)


def low(values):
    return values.astype(jnp.bfloat16)


def wide(values):
    return values.astype(jnp.float32)


def matmul(left_side, right_side):
    return jnp.dot(left_side, right_side, preferred_element_type=jnp.float32)


def contract_rows(left_side, right_side):
    return lax.dot_general(
        left_side, right_side, (((0,), (0,)), ((), ())), preferred_element_type=jnp.float32
    )


def contract_last(left_side, right_side):
    return lax.dot_general(
        left_side, right_side, (((1,), (1,)), ((), ())), preferred_element_type=jnp.float32
    )


def rope_tables(length, head_size):
    position = jnp.arange(length).astype(jnp.float32)
    column = jnp.arange(head_size // 2).astype(jnp.float32)
    frequency = jnp.exp(-math.log(THETA) * 2.0 * column / head_size)
    angles = position[:, None] * frequency[None, :]
    cosine, sine = jnp.cos(angles), jnp.sin(angles)
    return (
        jnp.concatenate([cosine, cosine], axis=-1),
        jnp.concatenate([-sine, sine], axis=-1),
    )


def flip(index, mask):
    result = index
    bit = 1
    while bit <= mask:
        if mask & bit:
            result = result + bit - 2 * bit * lax.rem(lax.div(index, bit), 2)
        bit *= 2
    return result


def semaphore_count(sizes):
    batches, width = sizes
    return 14 * width + 18 * batches


class Fabric:
    def __init__(self, sizes, send, recv):
        self.batches, self.width = sizes
        self.chips = self.width // 2
        self.row = lax.axis_index("dp")
        self.col = lax.axis_index("tensor")
        self.send, self.recv, self.used = send, recv, 0
        self.pending = []
        self.guarded = []

    def copy(self, source, target, row, col):
        number = self.used
        self.used += 1
        assert number < semaphore_count((self.batches, self.width))
        made = pltpu.make_async_remote_copy(
            src_ref=source,
            dst_ref=target,
            send_sem=self.send.at[number],
            recv_sem=self.recv.at[number],
            device_id=(row, col),
            device_id_type=MESH,
        )
        made.start()
        self.pending.append(made)
        return made

    def drain(self):
        for made in self.pending:
            made.wait_send()
        self.pending = []

    def drain_chains(self):
        for condition, made in self.guarded:
            pl.when(condition)(made.wait_send)
        self.guarded = []

    def mate(self):
        return flip(self.col, 1)

    def peer(self, step):
        return flip(self.col, 2 * step)

    def batch(self, step):
        return flip(self.row, step)

    def greet(self, along_tensor=True):
        barrier = pltpu.get_barrier_semaphore()
        peers = [(self.batch(step), self.col) for step in range(1, self.batches)]
        if along_tensor:
            peers += [(self.row, self.peer(step)) for step in range(1, self.chips)]
            peers.append((self.row, self.mate()))
        for peer in peers:
            pl.semaphore_signal(barrier, inc=1, device_id=peer, device_id_type=MESH)
        return lambda: pl.semaphore_wait(barrier, len(peers))

    def gather(self, source, slot):
        there = slot(self.col)
        direct = [
            self.copy(source, there, self.row, self.peer(step)) for step in range(1, self.chips)
        ]
        beside = [self.copy(source, there, self.row, self.mate())]
        there[...] = source[...]

        def forward():
            for step in range(1, self.chips):
                direct[step - 1].wait_recv()
                piece = slot(self.peer(step))
                beside.append(self.copy(piece, piece, self.row, self.mate()))

        def finish():
            for made in beside:
                made.wait_recv()

        return forward, finish

    def pair_up(self, slot, beside):
        return [
            self.copy(slot(flip(self.mate(), 2 * step)), beside.at[step], self.row, self.mate())
            for step in range(self.chips)
        ]

    def spread(self, slot, copies, beside, landed):
        def send(step):
            return self.copy(slot(self.peer(step)), landed.at[step], self.row, self.peer(step))

        sent = []
        order = list(range(self.chips - 1, 0, -1))
        for place, step in enumerate(order):
            copies[step].wait_recv()
            own = slot(self.peer(step))
            own[...] = low(wide(own[...]) + wide(beside[step]))
            if place:
                sent.append(send(order[place - 1]))
        copies[0].wait_recv()
        total = wide(slot(self.col)[...]) + wide(beside[0])
        if order:
            sent.append(send(order[-1]))

        def finish():
            result = total
            for made, step in zip(sent, order):
                made.wait_recv()
                result = result + wide(landed[step])
            return result

        return finish

    def exchange(self, source, target):
        made = [
            self.copy(
                source.at[self.batch(step)], target.at[self.row], self.batch(step), self.col
            )
            for step in range(1, self.batches)
        ]
        target[self.row] = source[self.row]

        def finish():
            for copy in made:
                copy.wait_recv()

        return finish

    def reserve(self, count):
        first = self.used
        self.used += count
        assert self.used <= semaphore_count((self.batches, self.width))
        return first

    def hop(self, source, target, number, way):
        return pltpu.make_async_remote_copy(
            src_ref=source,
            dst_ref=target,
            send_sem=self.send.at[number],
            recv_sem=self.recv.at[number],
            device_id=(jnp.clip(self.row + way, 0, self.batches - 1), self.col),
            device_id_type=MESH,
        )

    def rank(self, way):
        return self.row if way > 0 else self.batches - 1 - self.row


class GatherChain:
    def __init__(self, fabric, source, target):
        self.fabric, self.source, self.target = fabric, source, target
        self.first = fabric.reserve(2 * (fabric.batches - 1))

    def number(self, way, step):
        return self.first + (0 if way > 0 else self.fabric.batches - 1) + step - 1

    def arrive(self, step):
        fabric = self.fabric
        for way in (1, -1):
            piece = jnp.clip(fabric.row - way * step, 0, fabric.batches - 1)
            made = fabric.hop(
                self.target.at[piece], self.target.at[piece], self.number(way, step), way
            )
            pl.when(fabric.rank(way) >= step)(made.wait_recv)

    def step(self, step):
        fabric = self.fabric
        if step > 1:
            self.arrive(step - 1)
        for way in (1, -1):
            piece = jnp.clip(fabric.row - way * (step - 1), 0, fabric.batches - 1)
            source = self.source if step == 1 else self.target.at[piece]
            made = fabric.hop(source, self.target.at[piece], self.number(way, step), way)
            rank = fabric.rank(way)
            condition = (rank >= step - 1) & (rank < fabric.batches - 1)
            pl.when(condition)(made.start)
            fabric.guarded.append((condition, made))
        if step == 1:
            self.target[fabric.row] = self.source[...]

    def finish(self):
        self.arrive(self.fabric.batches - 1)


class ScatterChain:
    def __init__(self, fabric, source, landed):
        self.fabric, self.source, self.landed = fabric, source, landed
        self.first = fabric.reserve(2 * (fabric.batches - 1))

    def hop(self, source, way, step):
        side = 0 if way > 0 else 1
        number = self.first + side * (self.fabric.batches - 1) + step - 1
        return self.fabric.hop(source, self.landed.at[side, step - 1], number, way)

    def step(self, step):
        fabric = self.fabric
        last = fabric.batches - 1
        for way in (1, -1):
            side = 0 if way > 0 else 1
            rank = fabric.rank(way)
            goal = jnp.clip(fabric.batches + rank - step, 0, last)
            goal = goal if way > 0 else last - goal
            own = self.hop(self.source.at[goal], way, step)
            pl.when(rank == 0)(own.start)
            fabric.guarded.append((rank == 0, own))
            if step > 1:
                buffer = self.source.at[goal]
                summed = self.hop(buffer, way, step)
                before = self.hop(buffer, way, step - 1)
                condition = (rank > 0) & (rank < step)

                @pl.when(condition)
                def _():
                    before.wait_recv()
                    buffer[...] = low(wide(buffer[...]) + wide(self.landed[side, step - 2]))
                    summed.start()

                fabric.guarded.append((condition, summed))

    def finish(self, total):
        fabric = self.fabric
        last = fabric.batches - 1
        total[...] = wide(self.source[fabric.row])
        for way in (1, -1):
            side = 0 if way > 0 else 1
            made = self.hop(self.source.at[fabric.row], way, last)

            @pl.when(fabric.rank(way) > 0)
            def _():
                made.wait_recv()
                total[...] += wide(self.landed[side, last - 1])


def inverse_of(stream):
    return lax.rsqrt(jnp.mean(stream * stream, axis=-1, keepdims=True) + EPS)


def set_shard(values, shard, pieces):
    rounded = low(values)
    shard[...] = rounded
    block = pieces.shape[-1]
    for number in range(pieces.shape[0]):
        pieces[number] = rounded[:, number * block : (number + 1) * block]


def joined(total, exchanged):
    block = exchanged.shape[-1]
    return jnp.concatenate(
        [
            total[:, number * block : (number + 1) * block] + wide(exchanged[number])
            for number in range(exchanged.shape[0])
        ],
        axis=-1,
    )


def turn(values, cosine, sine, direction):
    other = pltpu.roll(values, HD // 2, 1)
    if direction > 0:
        return values * cosine + other * sine
    return values * cosine - other * sine


def head(index):
    return slice(index * HD, (index + 1) * HD)


def allowed_keys(length):
    row_index = lax.broadcasted_iota(jnp.int32, (LEN, LEN), 0)
    column_index = lax.broadcasted_iota(jnp.int32, (LEN, LEN), 1)
    return (column_index <= row_index) & (column_index < length)


def softmax_weights(queries, keys, allowed):
    powers = jnp.where(allowed, jnp.exp(contract_last(queries, keys) * SCALE), 0.0)
    return powers / jnp.sum(powers, axis=-1, keepdims=True)


def centred(weights, values):
    return weights * (values - jnp.sum(weights * values, axis=-1, keepdims=True))


def each_head(total_rows, query_width, key_width):
    repeat = query_width // key_width
    for seq in range(total_rows // LEN):
        rows = slice(seq * LEN, (seq + 1) * LEN)
        for number in range(key_width // HD):
            yield seq, rows, number, range(number * repeat, (number + 1) * repeat)


def repeated(count, function):
    def once(index, carry):
        function(index)
        return carry

    lax.fori_loop(0, count, once, 0)


def columns(index, size):
    return pl.ds(pl.multiple_of(index * size, size), size)


def rows_of(block):
    return block.reshape(-1, block.shape[-1])


def project(source, weights, layer, acc, cut):
    acc[...] = jnp.zeros_like(acc)
    widths = [weight.shape[-1] for weight in weights]

    def once(index):
        at = columns(index, cut)
        part = rows_of(source[:, :, at])
        start = 0
        for weight, width in zip(weights, widths):
            acc[:, start : start + width] += matmul(part, weight[layer, at, :])
            start += width

    repeated(source.shape[-1] // cut, once)


def probe_terms(blocks, probes, layer, partial):
    def once(index):
        rows = rows_of(blocks[index])
        start = 0
        for probe in probes:
            width = probe.shape[-1]
            partial[index, :, start : start + width] = low(matmul(rows, probe[layer]))
            start += width

    repeated(blocks.shape[0], once)


def out_terms(mixed, weight, layer, terms, cut):
    def once(index):
        at = columns(index, cut)
        terms[:, :, at] = low(matmul(mixed[...], weight[layer, :, at])).reshape(
            terms.shape[0], terms.shape[1], cut
        )

    repeated(terms.shape[-1] // cut, once)


def out_probe_terms(blended_all, probe, layer, probed):
    def once(index):
        probed[index] = low(matmul(blended_all[index], probe[layer])).reshape(probed.shape[1:])

    repeated(probed.shape[0], once)


def primal_attention(lengths, acc, cosine, sine, queries, keys, values, blended):
    total_rows, query_width = queries.shape
    key_width = keys.shape[1]
    values[...] = low(acc[:, query_width + key_width :])
    for seq, rows, number, members in each_head(total_rows, query_width, key_width):
        allowed = allowed_keys(lengths[seq])
        key_at = head(query_width // HD + number)
        key_head = low(turn(acc[rows, key_at], cosine[...], sine[...], 1))
        keys[rows, head(number)] = key_head
        value_head = values[rows, head(number)]
        for member in members:
            query_head = low(turn(acc[rows, head(member)], cosine[...], sine[...], 1))
            queries[rows, head(member)] = query_head
            weights = low(softmax_weights(query_head, key_head, allowed))
            blended[rows, head(member)] = low(matmul(weights, value_head))


def tangent_attention(lengths, acc, cosine, sine, queries, keys, values, mixed):
    query_width, key_width = queries.shape[1], keys.shape[1]
    for seq, rows, number, members in each_head(queries.shape[0], query_width, key_width):
        allowed = allowed_keys(lengths[seq])
        key_head = keys[rows, head(number)]
        value_head = values[rows, head(number)]
        key_at = query_width // HD + number
        value_at = key_at + key_width // HD
        moved_key = low(turn(acc[rows, head(key_at)], cosine[...], sine[...], 1))
        moved_value = low(acc[rows, head(value_at)])
        for member in members:
            query_head = queries[rows, head(member)]
            moved_query = low(turn(acc[rows, head(member)], cosine[...], sine[...], 1))
            weights = softmax_weights(query_head, key_head, allowed)
            scores = SCALE * (
                contract_last(moved_query, key_head) + contract_last(query_head, moved_key)
            )
            moved_weights = low(centred(weights, scores))
            mixed[rows, head(member)] = low(
                matmul(moved_weights, value_head) + matmul(low(weights), moved_value)
            )


def mixed_grads(cotangent, weight, layer, acc, cut):
    query_width = weight.shape[1]
    acc[:, :query_width] = jnp.zeros((acc.shape[0], query_width), jnp.float32)

    def once(index):
        at = columns(index, cut)
        acc[:, :query_width] += contract_last(rows_of(cotangent[:, :, at]), weight[layer, :, at])

    repeated(cotangent.shape[-1] // cut, once)


def backward_attention(lengths, acc, cosine, sine, queries, keys, values, grads):
    query_width, key_width = queries.shape[1], keys.shape[1]
    for seq, rows, number, members in each_head(queries.shape[0], query_width, key_width):
        allowed = allowed_keys(lengths[seq])
        key_head = keys[rows, head(number)]
        value_head = values[rows, head(number)]
        key_at = query_width // HD + number
        value_at = key_at + key_width // HD
        key_total = jnp.zeros((LEN, HD), jnp.float32)
        value_total = jnp.zeros((LEN, HD), jnp.float32)
        for member in members:
            query_head = queries[rows, head(member)]
            mixed = low(acc[rows, head(member)])
            weights = softmax_weights(query_head, key_head, allowed)
            value_total = value_total + contract_rows(low(weights), mixed)
            scores = low(centred(weights, contract_last(mixed, value_head)) * SCALE)
            grads[rows, head(member)] = low(
                turn(matmul(scores, key_head), cosine[...], sine[...], -1)
            )
            key_total = key_total + contract_rows(scores, query_head)
        grads[rows, head(key_at)] = low(turn(key_total, cosine[...], sine[...], -1))
        grads[rows, head(value_at)] = low(value_total)


def grad_terms(grads, weights, layer, terms, cut):
    def once(index):
        at = columns(index, cut)
        total = 0.0
        start = 0
        for weight in weights:
            width = weight.shape[-1]
            total = total + contract_last(grads[:, start : start + width], weight[layer, at, :])
            start += width
        terms[:, :, at] = low(total).reshape(terms.shape[0], terms.shape[1], cut)

    repeated(terms.shape[-1] // cut, once)


class Loads:
    def __init__(self, pairs, layers, semaphores):
        self.made = {}
        number = 0
        for layer in range(layers):
            for name, source, target in pairs:
                made = pltpu.make_async_copy(
                    source.at[layer], target.at[layer], semaphores.at[number]
                )
                made.start()
                self.made[name, layer] = made
                number += 1

    def need(self, layer, *names):
        for name in names:
            self.made.pop((name, layer)).wait()


PROJECTIONS = ("query_weight", "key_weight", "value_weight")
PROBES = ("query_probe", "key_probe", "value_probe")


def flow_kernel(sizes, cut, names, *refs):
    m = types.SimpleNamespace(**dict(zip(names, refs)))
    fabric = Fabric(sizes, m.send, m.recv)
    ready = fabric.greet()
    loaded = PROJECTIONS + ("out_weight",) + PROBES + ("out_probe",)
    loads = Loads(
        [(name, getattr(m, name), getattr(m, name + "_held")) for name in loaded],
        m.query_weight.shape[0],
        m.load_sem,
    )
    weights = [getattr(m, name + "_held") for name in PROJECTIONS]
    probes = [getattr(m, name + "_held") for name in PROBES]
    tables = (m.cosine, m.sine)
    kept = [(m.queries.at[layer], m.keys.at[layer], m.values.at[layer]) for layer in range(2)]
    blended = [m.blended.at[layer] for layer in range(2)]
    blended_all = [m.blended_all.at[layer] for layer in range(2)]
    partial = [m.partial.at[layer] for layer in range(2)]
    grads = [m.grads.at[layer] for layer in range(2)]
    grads_held = [m.grads_held.at[layer] for layer in range(2)]
    blocks = [m.blocks.at[layer] for layer in range(2)]
    backs = [ScatterChain(fabric, partial[layer], m.returned.at[layer]) for layer in range(2)]
    fetches = [GatherChain(fabric, blended[layer], blended_all[layer]) for layer in range(2)]
    grad_fetches = [GatherChain(fabric, grads[layer], grads_held[layer]) for layer in range(2)]
    middle = list(range(2, fabric.batches - 1))
    whole = lambda col: m.whole.at[col]
    slot = lambda col: m.terms.at[col]
    slot_p = lambda col: m.probed.at[:, col]
    stores = []

    def store(source, target, number):
        made = pltpu.make_async_copy(source, target, m.store_sem.at[number])
        made.start()
        return made

    def onto_blocks(layer):
        return lambda col: blocks[layer].at[:, col]

    stream = wide(m.tokens[...])
    set_shard(stream * inverse_of(stream) * m.gains[0:1, :], m.shard, m.pieces.at[0])
    ready()
    arrived = fabric.exchange(m.pieces.at[0], m.exchanged.at[0])
    forward, finish = fabric.gather(m.shard, whole)
    arrived()
    forward_blocks, finish_blocks = fabric.gather(m.exchanged.at[0], onto_blocks(0))
    forward()
    finish()
    loads.need(0, *PROJECTIONS)
    project(m.whole, weights, 0, m.acc, cut)
    primal_attention(m.lengths, m.acc, *tables, *kept[0], blended[0])
    fetches[0].step(1)
    forward_blocks()
    loads.need(0, "out_weight")
    out_terms(blended[0], m.out_weight_held, 0, m.terms, cut)
    paired = fabric.pair_up(slot, m.beside)
    finish_blocks()
    stores.append(store(blocks[0], m.blocks0, 0))
    loads.need(0, *PROBES)
    probe_terms(blocks[0], probes, 0, partial[0])
    backs[0].step(1)
    fabric.drain()
    total = fabric.spread(slot, paired, m.beside, m.landed)()

    rounded = low(wide(m.tokens[...]) + total)
    m.stream[...] = rounded
    stream = wide(rounded)
    fabric.drain()
    set_shard(stream * inverse_of(stream) * m.gains[1:2, :], m.shard, m.pieces.at[1])
    arrived = fabric.exchange(m.pieces.at[1], m.exchanged.at[1])
    forward, finish = fabric.gather(m.shard, whole)
    for step in middle:
        backs[0].step(step)
        fetches[0].step(step)
    arrived()
    forward_blocks, finish_blocks = fabric.gather(m.exchanged.at[1], onto_blocks(1))
    forward()
    finish()
    backs[0].step(fabric.batches - 1)
    fetches[0].step(fabric.batches - 1)
    loads.need(1, *PROJECTIONS)
    project(m.whole, weights, 1, m.acc, cut)
    primal_attention(m.lengths, m.acc, *tables, *kept[1], blended[1])
    forward_blocks()
    fetches[0].finish()
    backs[0].finish(m.acc)
    tangent_attention(m.lengths, m.acc, *tables, *kept[0], m.mixed)
    loads.need(0, "out_probe")
    out_probe_terms(blended_all[0], m.out_probe_held, 0, m.probed)
    paired_p = fabric.pair_up(slot_p, m.beside_p)
    out_terms(m.mixed, m.out_weight_held, 0, m.terms, cut)
    paired = fabric.pair_up(slot, m.beside)
    finish_blocks()
    stores.append(store(blocks[1], m.blocks1, 1))
    stores.append(store(blended_all[0], m.blended_all0, 2))
    loads.need(1, *PROBES)
    probe_terms(blocks[1], probes, 1, partial[1])
    backs[1].step(1)
    fetches[1].step(1)

    fabric.drain()
    finish_p = fabric.spread(slot_p, paired_p, m.beside_p, m.landed_p)
    finish = fabric.spread(slot, paired, m.beside, m.landed)
    m.pieces[0] = low(finish_p())
    arrived = fabric.exchange(m.pieces.at[0], m.exchanged.at[2])
    for step in middle:
        backs[1].step(step)
        fetches[1].step(step)
    total = finish()
    arrived()
    change = joined(total, m.exchanged.at[2])
    m.tangent[...] = change
    stream = wide(m.stream[...])
    inverse = inverse_of(stream)
    shift = jnp.mean(stream * change, axis=-1, keepdims=True)
    m.shard[...] = low(
        m.gains[1:2, :] * (change * inverse - stream * inverse * inverse * inverse * shift)
    )
    forward, finish = fabric.gather(m.shard, whole)
    backs[1].step(fabric.batches - 1)
    fetches[1].step(fabric.batches - 1)
    forward()
    finish()
    fabric.drain()
    project(m.whole, weights, 1, m.acc, cut)
    backs[1].finish(m.moved)
    m.acc[...] += m.moved[...]
    tangent_attention(m.lengths, m.acc, *tables, *kept[1], m.mixed)
    fetches[1].finish()
    stores.append(store(blended_all[1], m.blended_all1, 3))
    loads.need(1, "out_probe", "out_weight")
    out_probe_terms(blended_all[1], m.out_probe_held, 1, m.probed)
    paired_p = fabric.pair_up(slot_p, m.beside_p)
    out_terms(m.mixed, m.out_weight_held, 1, m.terms, cut)
    paired = fabric.pair_up(slot, m.beside)

    finish_p = fabric.spread(slot_p, paired_p, m.beside_p, m.landed_p)
    finish = fabric.spread(slot, paired, m.beside, m.landed)
    fabric.drain_chains()
    m.pieces[1] = low(finish_p())
    arrived = fabric.exchange(m.pieces.at[1], m.exchanged.at[3])
    total = finish()
    arrived()
    cotangent = m.mask[...] * (m.tangent[...] + joined(total, m.exchanged.at[3]))
    m.tangent[...] = cotangent
    set_shard(cotangent, m.shard, m.pieces.at[0])
    forward, finish = fabric.gather(m.shard, whole)
    arrived = fabric.exchange(m.pieces.at[0], m.exchanged.at[4])
    forward()
    finish()
    fabric.drain()
    for made in stores:
        made.wait()
    mixed_grads(m.whole, m.out_weight_held, 1, m.acc, cut)
    backward_attention(m.lengths, m.acc, *tables, *kept[1], grads[1])
    grad_fetches[1].step(1)
    grad_terms(grads[1], weights, 1, m.terms, cut)
    paired = fabric.pair_up(slot, m.beside)

    total = fabric.spread(slot, paired, m.beside, m.landed)()
    stream = wide(m.stream[...])
    inverse = inverse_of(stream)
    scaled = total * m.gains[1:2, :]
    shift = jnp.mean(stream * scaled, axis=-1, keepdims=True)
    cotangent = m.tangent[...] + inverse * (scaled - stream * inverse * inverse * shift)
    fabric.drain()
    set_shard(cotangent, m.shard, m.pieces.at[1])
    forward, finish = fabric.gather(m.shard, whole)
    last_arrived = fabric.exchange(m.pieces.at[1], m.exchanged.at[5])
    arrived()
    forward_blocks, finish_blocks = fabric.gather(m.exchanged.at[4], onto_blocks(0))
    for step in middle:
        grad_fetches[1].step(step)
    forward()
    finish()
    mixed_grads(m.whole, m.out_weight_held, 0, m.acc, cut)
    backward_attention(m.lengths, m.acc, *tables, *kept[0], grads[0])
    grad_fetches[1].step(fabric.batches - 1)
    grad_fetches[0].step(1)
    last_arrived()
    forward_last, finish_last = fabric.gather(m.exchanged.at[5], onto_blocks(1))
    forward_blocks()
    finish_blocks()
    last_stores = [store(blocks[0], m.cotangents1, 0)]
    for step in middle:
        grad_fetches[0].step(step)
    grad_fetches[1].finish()
    last_stores.append(store(grads_held[1], m.grads_all1, 1))
    forward_last()
    grad_fetches[0].step(fabric.batches - 1)
    finish_last()
    last_stores.append(store(blocks[1], m.cotangents0, 2))
    grad_fetches[0].finish()
    last_stores.append(store(grads_held[0], m.grads_all0, 3))
    for made in last_stores:
        made.wait()
    fabric.drain()
    fabric.drain_chains()


def product_kernel(layers, *refs):
    inputs, (query_out, key_out, value_out, out_out) = refs[:-4], refs[-4:]
    layer = pl.program_id(0)
    query_width, key_width = query_out.shape[-1], key_out.shape[-1]
    for number in range(layers):
        blocks, grads, blended, cotangent = inputs[4 * number : 4 * number + 4]

        @pl.when(layer == number)
        def _():
            product = contract_rows(blocks[...], grads[...])
            query_out[0] = product[:, :query_width]
            key_out[0] = product[:, query_width : query_width + key_width]
            value_out[0] = product[:, query_width + key_width :]
            out_out[0] = contract_rows(blended[...], cotangent[...])


CUTS = 4


def body(
    tokens,
    lengths,
    norm_gains,
    query_weight,
    key_weight,
    value_weight,
    out_weight,
    query_probe,
    key_probe,
    value_probe,
    out_probe,
):
    width = lax.axis_size("tensor")
    batches = lax.axis_size("dp")
    sizes = (batches, width)
    tensor_index = lax.axis_index("tensor")
    data_index = lax.axis_index("dp")
    share, model = tokens.shape
    group = share * width
    seq_count = group // LEN
    layers = query_weight.shape[0]
    assert layers == 2
    half_width = key_weight.shape[2]
    query_width = query_weight.shape[2]
    paired = half_width < HD
    key_width = 2 * half_width if paired else half_width
    sent_width = query_width + 2 * half_width
    block = query_probe.shape[1]
    cosine, sine = rope_tables(LEN, HD)
    group_lengths = lax.dynamic_slice_in_dim(lengths, data_index * seq_count, seq_count)
    position = tensor_index * share + jnp.arange(share)
    row_mask = wide(position % LEN < group_lengths[position // LEN])[:, None]
    lower_half = tensor_index % 2 == 0

    def swapped(value):
        pairs = [(source, source ^ 1) for source in range(width)]
        return lax.ppermute(value, "tensor", pairs)

    def join_halves(own_part):
        other_part = swapped(own_part)
        return jnp.where(
            lower_half,
            jnp.concatenate([own_part, other_part], axis=-1),
            jnp.concatenate([other_part, own_part], axis=-1),
        )

    def split_halves(values):
        first, second = values[:, :half_width], values[:, half_width:]
        own_part = jnp.where(lower_half, first, second)
        other_part = jnp.where(lower_half, second, first)
        return low(wide(own_part) + wide(swapped(other_part)))

    parts = [key_weight, value_weight, key_probe, value_probe]
    if paired:
        parts = [join_halves(part) for part in parts]
    key_full, value_full, key_probe_full, value_probe_full = parts

    def to_send(grads):
        if not paired:
            return grads
        return jnp.concatenate(
            [
                grads[:, :query_width],
                split_halves(grads[:, query_width : query_width + key_width]),
                split_halves(grads[:, query_width + key_width :]),
            ],
            axis=-1,
        )

    bf, f32 = jnp.bfloat16, jnp.float32
    chips = width // 2
    wide_width = query_width + 2 * key_width
    rows_in_all = batches * group

    def flow():
        inputs = dict(
            lengths=group_lengths,
            tokens=tokens,
            gains=norm_gains,
            mask=row_mask,
            cosine=cosine,
            sine=sine,
            query_weight=query_weight,
            key_weight=key_full,
            value_weight=value_full,
            out_weight=out_weight,
            query_probe=query_probe,
            key_probe=key_probe_full,
            value_probe=value_probe_full,
            out_probe=out_probe,
        )
        blocks_shape = (batches, width, share, block)
        outputs = dict(
            blocks0=blocks_shape,
            blocks1=blocks_shape,
            blended_all0=(batches, group, query_width),
            blended_all1=(batches, group, query_width),
            cotangents0=blocks_shape,
            cotangents1=blocks_shape,
            grads_all0=(batches, group, wide_width),
            grads_all1=(batches, group, wide_width),
        )
        held = {
            name + "_held": pltpu.VMEM(value.shape, bf)
            for name, value in list(inputs.items())[6:]
        }
        scratch = dict(
            whole=pltpu.VMEM((width, share, model), bf),
            blocks=pltpu.VMEM((layers,) + blocks_shape, bf),
            terms=pltpu.VMEM((width, share, model), bf),
            probed=pltpu.VMEM(blocks_shape, bf),
            beside=pltpu.VMEM((chips, share, model), bf),
            landed=pltpu.VMEM((chips, share, model), bf),
            beside_p=pltpu.VMEM((chips, batches, share, block), bf),
            landed_p=pltpu.VMEM((chips, batches, share, block), bf),
            partial=pltpu.VMEM((layers, batches, group, wide_width), bf),
            returned=pltpu.VMEM((layers, 2, batches - 1, group, wide_width), bf),
            queries=pltpu.VMEM((layers, group, query_width), bf),
            keys=pltpu.VMEM((layers, group, key_width), bf),
            values=pltpu.VMEM((layers, group, key_width), bf),
            blended=pltpu.VMEM((layers, group, query_width), bf),
            blended_all=pltpu.VMEM((layers, batches, group, query_width), bf),
            mixed=pltpu.VMEM((group, query_width), bf),
            grads=pltpu.VMEM((layers, group, wide_width), bf),
            grads_held=pltpu.VMEM((layers, batches, group, wide_width), bf),
            acc=pltpu.VMEM((group, wide_width), f32),
            moved=pltpu.VMEM((group, wide_width), f32),
            shard=pltpu.VMEM((share, model), bf),
            stream=pltpu.VMEM((share, model), bf),
            tangent=pltpu.VMEM((share, model), f32),
            pieces=pltpu.VMEM((2, batches, share, block), bf),
            exchanged=pltpu.VMEM((6, batches, share, block), bf),
            **held,
            send=pltpu.SemaphoreType.DMA((semaphore_count(sizes),)),
            recv=pltpu.SemaphoreType.DMA((semaphore_count(sizes),)),
            load_sem=pltpu.SemaphoreType.DMA((layers * len(held),)),
            store_sem=pltpu.SemaphoreType.DMA((4,)),
        )
        vmem = pl.BlockSpec(memory_space=pltpu.VMEM)
        anywhere = pl.BlockSpec(memory_space=pl.ANY)
        return pl.pallas_call(
            functools.partial(
                flow_kernel, sizes, model // CUTS, [*inputs, *outputs, *scratch]
            ),
            out_shape=[jax.ShapeDtypeStruct(shape, bf) for shape in outputs.values()],
            in_specs=[pl.BlockSpec(memory_space=pltpu.SMEM)]
            + [vmem] * 5
            + [anywhere] * len(held),
            out_specs=[anywhere] * len(outputs),
            scratch_shapes=list(scratch.values()),
            compiler_params=pltpu.CompilerParams(
                collective_id=0, has_side_effects=True, vmem_limit_bytes=67043328
            ),
        )(*inputs.values())

    def cost(flops, moved_bytes):
        return pl.CostEstimate(flops=flops, bytes_accessed=moved_bytes, transcendentals=0)

    def products(per_layer):
        out_block = out_probe.shape[2]
        by_rows = query_width % (CUTS * HD) == 0
        blended_cut = query_width // CUTS if by_rows else query_width
        out_cut = out_block if by_rows else out_block // CUTS
        in_specs, args = [], []
        for number, (blocks, grads, blended, cotangents) in enumerate(per_layer):

            def place(i, j, number=number):
                return (0, jnp.clip((i - number) * CUTS + j, 0, CUTS - 1))

            def still(i, j):
                return (0, 0)

            in_specs += [
                pl.BlockSpec((rows_in_all, block // CUTS), place),
                pl.BlockSpec((rows_in_all, sent_width), still),
                pl.BlockSpec((rows_in_all, blended_cut), place if by_rows else still),
                pl.BlockSpec((rows_in_all, out_cut), still if by_rows else place),
            ]
            args += [
                blocks.reshape(rows_in_all, block),
                grads.reshape(rows_in_all, sent_width),
                blended.reshape(rows_in_all, query_width),
                cotangents.reshape(rows_in_all, out_block),
            ]
        shapes = [
            (block, query_width),
            (block, half_width),
            (block, half_width),
            (query_width, out_block),
        ]
        return pl.pallas_call(
            functools.partial(product_kernel, layers),
            grid=(layers, CUTS),
            in_specs=in_specs,
            out_specs=[
                pl.BlockSpec((1, rows // CUTS, columns), lambda i, j: (i, j, 0))
                for rows, columns in shapes[:3]
            ]
            + [
                pl.BlockSpec(
                    (1, blended_cut, out_cut),
                    lambda i, j: (i, j, 0) if by_rows else (i, 0, j),
                )
            ],
            out_shape=[
                jax.ShapeDtypeStruct((layers, rows, columns), f32) for rows, columns in shapes
            ],
            compiler_params=pltpu.CompilerParams(
                dimension_semantics=("arbitrary", "arbitrary")
            ),
            cost_estimate=cost(2 * rows_in_all * block * query_width * 4, 32 << 20),
        )(*args)

    results = flow()
    blocks0, blocks1, blended0, blended1, cotangents0, cotangents1, grads0, grads1 = results
    sent = [to_send(grads.reshape(rows_in_all, wide_width)) for grads in (grads0, grads1)]
    return tuple(
        products(
            [
                (blocks0, sent[0], blended0, cotangents0),
                (blocks1, sent[1], blended1, cotangents1),
            ]
        )
    )


def solution(mesh):
    placed = (
        P(("dp", "tensor"), None),
        P(),
        P(),
        P(None, None, "tensor"),
        P(None, None, "tensor"),
        P(None, None, "tensor"),
        P(None, "tensor", None),
        P(None, "dp", "tensor"),
        P(None, "dp", "tensor"),
        P(None, "dp", "tensor"),
        P(None, "tensor", "dp"),
    )
    return jax.shard_map(
        body,
        mesh=mesh,
        in_specs=placed,
        out_specs=(
            P(None, "dp", "tensor"),
            P(None, "dp", "tensor"),
            P(None, "dp", "tensor"),
            P(None, "tensor", "dp"),
        ),
        check_vma=False,
    )
```

```python
import functools
import math
import types

import jax
import jax.numpy as jnp
import numpy as np
from jax import lax
from jax.experimental import pallas as pl
from jax.experimental.pallas import tpu as pltpu
from jax.sharding import PartitionSpec as P

HD = 128
LEN = 256
EPS = 1e-05
THETA = 500000.0
MESH = pl.DeviceIdType.MESH
SCALE = 1.0 / math.sqrt(HD)


def low(values):
    return values.astype(jnp.bfloat16)


def wide(values):
    return values.astype(jnp.float32)


def matmul(left_side, right_side):
    return jnp.dot(left_side, right_side, preferred_element_type=jnp.float32)


def contract_rows(left_side, right_side):
    return lax.dot_general(
        left_side, right_side, (((0,), (0,)), ((), ())), preferred_element_type=jnp.float32
    )


def contract_last(left_side, right_side):
    return lax.dot_general(
        left_side, right_side, (((1,), (1,)), ((), ())), preferred_element_type=jnp.float32
    )


def rope_tables(length, head_size):
    frequency = np.exp(-math.log(THETA) * 2.0 * np.arange(head_size // 2) / head_size)
    angles = np.arange(length)[:, None] * frequency.astype(np.float32)[None, :]
    cosine, sine = np.cos(angles), np.sin(angles)
    return (
        np.concatenate([cosine, cosine], axis=-1).astype(np.float32),
        np.concatenate([-sine, sine], axis=-1).astype(np.float32),
    )


def flip(index, mask):
    result = index
    bit = 1
    while bit <= mask:
        if mask & bit:
            result = result + bit - 2 * bit * lax.rem(lax.div(index, bit), 2)
        bit *= 2
    return result


def semaphore_count(sizes):
    batches, width = sizes
    return 24 * width + 18 * batches


class Fabric:
    def __init__(self, sizes, send, recv):
        self.batches, self.width = sizes
        self.chips = self.width // 2
        self.row = lax.axis_index("dp")
        self.col = lax.axis_index("tensor")
        self.send, self.recv, self.used = send, recv, 0
        self.pending = []
        self.guarded = []

    def copy(self, source, target, row, col):
        number = self.used
        self.used += 1
        assert number < semaphore_count((self.batches, self.width))
        made = pltpu.make_async_remote_copy(
            src_ref=source,
            dst_ref=target,
            send_sem=self.send.at[number],
            recv_sem=self.recv.at[number],
            device_id=(row, col),
            device_id_type=MESH,
        )
        made.start()
        self.pending.append(made)
        return made

    def drain(self, only=None):
        for made in self.pending if only is None else only:
            made.wait_send()
        gone = set() if only is None else {id(made) for made in only}
        self.pending = [made for made in self.pending if gone and id(made) not in gone]

    def drain_chains(self):
        for condition, made in self.guarded:
            pl.when(condition)(made.wait_send)
        self.guarded = []

    def mate(self):
        return flip(self.col, 1)

    def peer(self, step):
        return flip(self.col, 2 * step)

    def batch(self, step):
        return flip(self.row, step)

    def greet(self, along_tensor=True):
        barrier = pltpu.get_barrier_semaphore()
        peers = [(self.batch(step), self.col) for step in range(1, self.batches)]
        if along_tensor:
            peers += [(self.row, self.peer(step)) for step in range(1, self.chips)]
            peers.append((self.row, self.mate()))
        for peer in peers:
            pl.semaphore_signal(barrier, inc=1, device_id=peer, device_id_type=MESH)
        return lambda: pl.semaphore_wait(barrier, len(peers))

    def exchange(self, source, target):
        made = [
            self.copy(
                source.at[self.batch(step)], target.at[self.row], self.batch(step), self.col
            )
            for step in range(1, self.batches)
        ]
        target[self.row] = source[self.row]

        def finish():
            for copy in made:
                copy.wait_recv()

        return finish

    def reserve(self, count):
        first = self.used
        self.used += count
        assert self.used <= semaphore_count((self.batches, self.width))
        return first

    def hop(self, source, target, number, way):
        return pltpu.make_async_remote_copy(
            src_ref=source,
            dst_ref=target,
            send_sem=self.send.at[number],
            recv_sem=self.recv.at[number],
            device_id=(jnp.clip(self.row + way, 0, self.batches - 1), self.col),
            device_id_type=MESH,
        )

    def rank(self, way):
        return self.row if way > 0 else self.batches - 1 - self.row


class Gather:
    def __init__(self, fabric, source, slot, half):
        self.fabric, self.slot, self.half = fabric, slot, half
        self.made, self.beside = [], []
        there = slot(fabric.col)
        if fabric.chips == 4:
            self.first = [
                self.copy(half(source, 0), half(there, 0), fabric.peer(1)),
                self.copy(half(source, 1), half(there, 1), fabric.peer(2)),
            ]
            self.second = [
                self.copy(half(source, 1), half(there, 1), fabric.peer(1)),
                self.copy(half(source, 0), half(there, 0), fabric.peer(2)),
            ]
        else:
            self.direct = [
                self.copy(source, there, fabric.peer(step)) for step in range(1, fabric.chips)
            ]
        self.beside.append(self.copy(source, there, fabric.mate()))
        there[...] = source[...]

    def copy(self, source, target, col):
        made = self.fabric.copy(source, target, self.fabric.row, col)
        self.made.append(made)
        return made

    def beside_too(self, piece):
        self.beside.append(self.copy(piece, piece, self.fabric.mate()))

    def relay(self):
        fabric = self.fabric
        self.relayed = []
        if fabric.chips == 4:
            for number in range(2):
                self.first[number].wait_recv()
                piece = self.half(self.slot(fabric.peer(1 + number)), number)
                self.relayed.append(self.copy(piece, piece, fabric.peer(2 - number)))
                self.beside_too(piece)

    def forward(self):
        fabric = self.fabric
        if fabric.chips == 4:
            for number in range(2):
                self.second[number].wait_recv()
                self.beside_too(self.half(self.slot(fabric.peer(1 + number)), 1 - number))
            for number in range(2):
                self.relayed[number].wait_recv()
                self.beside_too(self.half(self.slot(fabric.peer(3)), number))
        else:
            for step in range(1, fabric.chips):
                self.direct[step - 1].wait_recv()
                self.beside_too(self.slot(fabric.peer(step)))

    def finish(self):
        for made in self.beside:
            made.wait_recv()

    def drain(self):
        self.fabric.drain(self.made)


class Reduce:
    def __init__(self, fabric, slot, beside, landed, relayed, half):
        self.fabric, self.slot, self.half = fabric, slot, half
        self.beside, self.landed, self.relayed = beside, landed, relayed
        self.paired = [
            fabric.copy(
                slot(flip(fabric.mate(), 2 * step)), beside.at[step], fabric.row, fabric.mate()
            )
            for step in range(fabric.chips)
        ]

    def add(self, step):
        self.paired[step].wait_recv()
        own = self.slot(self.fabric.peer(step))
        own[...] = low(wide(own[...]) + wide(self.beside[step]))

    def part(self, step, number):
        return self.half(self.slot(self.fabric.peer(step)), number)

    def send(self, step, number=None):
        fabric = self.fabric
        if number is None:
            source, target = self.slot(fabric.peer(step)), self.landed.at[step]
        else:
            source, target = self.part(step, number), self.half(self.landed.at[step], number)
        self.sent.append((step, number, fabric.copy(source, target, fabric.row, fabric.peer(step))))

    def spread(self):
        fabric = self.fabric
        self.sent = []
        if fabric.chips == 4:
            self.add(3)
            self.add(1)
            self.passed = [
                fabric.copy(
                    self.part(3, number),
                    self.relayed.at[number],
                    fabric.row,
                    fabric.peer(1 + number),
                )
                for number in range(2)
            ]
            self.add(2)
            self.send(1, 0)
        else:
            order = list(range(fabric.chips - 1, 0, -1))
            for place, step in enumerate(order):
                self.add(step)
                if place:
                    self.send(order[place - 1])
        self.paired[0].wait_recv()
        self.total = wide(self.slot(fabric.col)[...]) + wide(self.beside[0])
        if fabric.chips == 4:
            self.send(2, 1)
        elif order:
            self.send(order[-1])

    def relay(self):
        if self.fabric.chips == 4:
            for number in range(2):
                self.passed[number].wait_recv()
                part = self.part(2 - number, number)
                part[...] = low(wide(part[...]) + wide(self.relayed[number]))
                self.send(2 - number, number)

    def finish(self):
        result = self.total
        for step, number, made in self.sent:
            made.wait_recv()
        for step in range(1, self.fabric.chips):
            if self.fabric.chips != 4 or step < 3:
                result = result + wide(self.landed[step])
        return result


class GatherChain:
    def __init__(self, fabric, source, target):
        self.fabric, self.source, self.target = fabric, source, target
        self.first = fabric.reserve(2 * (fabric.batches - 1))

    def number(self, way, step):
        return self.first + (0 if way > 0 else self.fabric.batches - 1) + step - 1

    def arrive(self, step):
        fabric = self.fabric
        for way in (1, -1):
            piece = jnp.clip(fabric.row - way * step, 0, fabric.batches - 1)
            made = fabric.hop(
                self.target.at[piece], self.target.at[piece], self.number(way, step), way
            )
            pl.when(fabric.rank(way) >= step)(made.wait_recv)

    def step(self, step):
        fabric = self.fabric
        if step > 1:
            self.arrive(step - 1)
        for way in (1, -1):
            piece = jnp.clip(fabric.row - way * (step - 1), 0, fabric.batches - 1)
            source = self.source if step == 1 else self.target.at[piece]
            made = fabric.hop(source, self.target.at[piece], self.number(way, step), way)
            rank = fabric.rank(way)
            condition = (rank >= step - 1) & (rank < fabric.batches - 1)
            pl.when(condition)(made.start)
            fabric.guarded.append((condition, made))
        if step == 1:
            self.target[fabric.row] = self.source[...]

    def finish(self):
        self.arrive(self.fabric.batches - 1)


class ScatterChain:
    def __init__(self, fabric, source, landed):
        self.fabric, self.source, self.landed = fabric, source, landed
        self.first = fabric.reserve(2 * (fabric.batches - 1))

    def hop(self, source, way, step):
        side = 0 if way > 0 else 1
        number = self.first + side * (self.fabric.batches - 1) + step - 1
        return self.fabric.hop(source, self.landed.at[side, step - 1], number, way)

    def step(self, step):
        fabric = self.fabric
        last = fabric.batches - 1
        for way in (1, -1):
            side = 0 if way > 0 else 1
            rank = fabric.rank(way)
            goal = jnp.clip(fabric.batches + rank - step, 0, last)
            goal = goal if way > 0 else last - goal
            own = self.hop(self.source.at[goal], way, step)
            pl.when(rank == 0)(own.start)
            fabric.guarded.append((rank == 0, own))
            if step > 1:
                buffer = self.source.at[goal]
                summed = self.hop(buffer, way, step)
                before = self.hop(buffer, way, step - 1)
                condition = (rank > 0) & (rank < step)

                @pl.when(condition)
                def _():
                    before.wait_recv()
                    buffer[...] = low(wide(buffer[...]) + wide(self.landed[side, step - 2]))
                    summed.start()

                fabric.guarded.append((condition, summed))

    def finish(self, total):
        fabric = self.fabric
        last = fabric.batches - 1
        total[...] = wide(self.source[fabric.row])
        for way in (1, -1):
            side = 0 if way > 0 else 1
            made = self.hop(self.source.at[fabric.row], way, last)

            @pl.when(fabric.rank(way) > 0)
            def _():
                made.wait_recv()
                total[...] += wide(self.landed[side, last - 1])


def inverse_of(stream):
    return lax.rsqrt(jnp.mean(stream * stream, axis=-1, keepdims=True) + EPS)


def set_shard(values, shard, pieces):
    rounded = low(values)
    shard[...] = rounded
    block = pieces.shape[-1]
    for number in range(pieces.shape[0]):
        pieces[number] = rounded[:, number * block : (number + 1) * block]


def joined(total, exchanged):
    block = exchanged.shape[-1]
    return jnp.concatenate(
        [
            total[:, number * block : (number + 1) * block] + wide(exchanged[number])
            for number in range(exchanged.shape[0])
        ],
        axis=-1,
    )


def turn(values, cosine, sine, direction):
    other = pltpu.roll(values, HD // 2, 1)
    if direction > 0:
        return values * cosine + other * sine
    return values * cosine - other * sine


def head(index):
    return slice(index * HD, (index + 1) * HD)


def allowed_keys(length):
    row_index = lax.broadcasted_iota(jnp.int32, (LEN, LEN), 0)
    column_index = lax.broadcasted_iota(jnp.int32, (LEN, LEN), 1)
    return (column_index <= row_index) & (column_index < length)


def softmax_weights(queries, keys, allowed):
    powers = jnp.where(allowed, jnp.exp(contract_last(queries, keys) * SCALE), 0.0)
    return powers / jnp.sum(powers, axis=-1, keepdims=True)


def centred(weights, values):
    return weights * (values - jnp.sum(weights * values, axis=-1, keepdims=True))


def each_head(total_rows, query_width, key_width):
    repeat = query_width // key_width
    for seq in range(total_rows // LEN):
        rows = slice(seq * LEN, (seq + 1) * LEN)
        for number in range(key_width // HD):
            yield seq, rows, number, range(number * repeat, (number + 1) * repeat)


def repeated(count, function):
    def once(index, carry):
        function(index)
        return carry

    lax.fori_loop(0, count, once, 0)


def columns(index, size):
    return pl.ds(pl.multiple_of(index * size, size), size)


def rows_of(block):
    return block.reshape(-1, block.shape[-1])


def project(source, weights, layer, acc, cut):
    acc[...] = jnp.zeros_like(acc)
    widths = [weight.shape[-1] for weight in weights]

    def once(index):
        at = columns(index, cut)
        part = rows_of(source[:, :, at])
        start = 0
        for weight, width in zip(weights, widths):
            acc[:, start : start + width] += matmul(part, weight[layer, at, :])
            start += width

    repeated(source.shape[-1] // cut, once)


def probe_terms(blocks, probes, layer, partial):
    def once(index):
        rows = rows_of(blocks[index])
        start = 0
        for probe in probes:
            width = probe.shape[-1]
            partial[index, :, start : start + width] = low(matmul(rows, probe[layer]))
            start += width

    repeated(blocks.shape[0], once)


def out_terms(mixed, weight, layer, terms, cut):
    def once(index):
        at = columns(index, cut)
        terms[:, :, at] = low(matmul(mixed[...], weight[layer, :, at])).reshape(
            terms.shape[0], terms.shape[1], cut
        )

    repeated(terms.shape[-1] // cut, once)


def out_probe_terms(blended_all, probe, layer, probed):
    def once(index):
        probed[index] = low(matmul(blended_all[index], probe[layer])).reshape(probed.shape[1:])

    repeated(probed.shape[0], once)


def primal_attention(lengths, acc, cosine, sine, queries, keys, values, blended):
    total_rows, query_width = queries.shape
    key_width = keys.shape[1]
    values[...] = low(acc[:, query_width + key_width :])
    for seq, rows, number, members in each_head(total_rows, query_width, key_width):
        allowed = allowed_keys(lengths[seq])
        key_at = head(query_width // HD + number)
        key_head = low(turn(acc[rows, key_at], cosine[...], sine[...], 1))
        keys[rows, head(number)] = key_head
        value_head = values[rows, head(number)]
        for member in members:
            query_head = low(turn(acc[rows, head(member)], cosine[...], sine[...], 1))
            queries[rows, head(member)] = query_head
            weights = low(softmax_weights(query_head, key_head, allowed))
            blended[rows, head(member)] = low(matmul(weights, value_head))


def tangent_attention(lengths, acc, cosine, sine, queries, keys, values, mixed):
    query_width, key_width = queries.shape[1], keys.shape[1]
    for seq, rows, number, members in each_head(queries.shape[0], query_width, key_width):
        allowed = allowed_keys(lengths[seq])
        key_head = keys[rows, head(number)]
        value_head = values[rows, head(number)]
        key_at = query_width // HD + number
        value_at = key_at + key_width // HD
        moved_key = low(turn(acc[rows, head(key_at)], cosine[...], sine[...], 1))
        moved_value = low(acc[rows, head(value_at)])
        for member in members:
            query_head = queries[rows, head(member)]
            moved_query = low(turn(acc[rows, head(member)], cosine[...], sine[...], 1))
            weights = softmax_weights(query_head, key_head, allowed)
            scores = SCALE * (
                contract_last(moved_query, key_head) + contract_last(query_head, moved_key)
            )
            moved_weights = low(centred(weights, scores))
            mixed[rows, head(member)] = low(
                matmul(moved_weights, value_head) + matmul(low(weights), moved_value)
            )


def mixed_grads(cotangent, weight, layer, acc, cut):
    query_width = weight.shape[1]
    acc[:, :query_width] = jnp.zeros((acc.shape[0], query_width), jnp.float32)

    def once(index):
        at = columns(index, cut)
        acc[:, :query_width] += contract_last(rows_of(cotangent[:, :, at]), weight[layer, :, at])

    repeated(cotangent.shape[-1] // cut, once)


def backward_attention(lengths, acc, cosine, sine, queries, keys, values, grads):
    query_width, key_width = queries.shape[1], keys.shape[1]
    for seq, rows, number, members in each_head(queries.shape[0], query_width, key_width):
        allowed = allowed_keys(lengths[seq])
        key_head = keys[rows, head(number)]
        value_head = values[rows, head(number)]
        key_at = query_width // HD + number
        value_at = key_at + key_width // HD
        key_total = jnp.zeros((LEN, HD), jnp.float32)
        value_total = jnp.zeros((LEN, HD), jnp.float32)
        for member in members:
            query_head = queries[rows, head(member)]
            mixed = low(acc[rows, head(member)])
            weights = softmax_weights(query_head, key_head, allowed)
            value_total = value_total + contract_rows(low(weights), mixed)
            scores = low(centred(weights, contract_last(mixed, value_head)) * SCALE)
            grads[rows, head(member)] = low(
                turn(matmul(scores, key_head), cosine[...], sine[...], -1)
            )
            key_total = key_total + contract_rows(scores, query_head)
        grads[rows, head(key_at)] = low(turn(key_total, cosine[...], sine[...], -1))
        grads[rows, head(value_at)] = low(value_total)


def grad_terms(grads, weights, layer, terms, cut):
    def once(index):
        at = columns(index, cut)
        total = 0.0
        start = 0
        for weight in weights:
            width = weight.shape[-1]
            total = total + contract_last(grads[:, start : start + width], weight[layer, at, :])
            start += width
        terms[:, :, at] = low(total).reshape(terms.shape[0], terms.shape[1], cut)

    repeated(terms.shape[-1] // cut, once)


class Loads:
    def __init__(self, pairs, layers, semaphores):
        self.made = {}
        number = 0
        for layer in range(layers):
            for name, source, target in pairs:
                made = pltpu.make_async_copy(
                    source.at[layer], target.at[layer], semaphores.at[number]
                )
                made.start()
                self.made[name, layer] = made
                number += 1

    def need(self, layer, *names):
        for name in names:
            self.made.pop((name, layer)).wait()


PROJECTIONS = ("query_weight", "key_weight", "value_weight")
PROBES = ("query_probe", "key_probe", "value_probe")


def flow_kernel(sizes, cut, names, *refs):
    m = types.SimpleNamespace(**dict(zip(names, refs)))
    fabric = Fabric(sizes, m.send, m.recv)
    ready = fabric.greet()
    loaded = PROJECTIONS + ("out_weight",) + PROBES + ("out_probe",)
    loads = Loads(
        [(name, getattr(m, name), getattr(m, name + "_held")) for name in loaded],
        m.query_weight.shape[0],
        m.load_sem,
    )
    weights = [getattr(m, name + "_held") for name in PROJECTIONS]
    probes = [getattr(m, name + "_held") for name in PROBES]
    tables = (m.cosine, m.sine)
    kept = [(m.queries.at[layer], m.keys.at[layer], m.values.at[layer]) for layer in range(2)]
    blended = [m.blended.at[layer] for layer in range(2)]
    blended_all = [m.blended_all.at[layer] for layer in range(2)]
    partial = [m.partial.at[layer] for layer in range(2)]
    grads = [m.grads.at[layer] for layer in range(2)]
    grads_held = [m.grads_held.at[layer] for layer in range(2)]
    blocks = [m.blocks.at[layer] for layer in range(2)]
    backs = [ScatterChain(fabric, partial[layer], m.returned.at[layer]) for layer in range(2)]
    fetches = [GatherChain(fabric, blended[layer], blended_all[layer]) for layer in range(2)]
    grad_fetches = [GatherChain(fabric, grads[layer], grads_held[layer]) for layer in range(2)]
    share, model = m.tokens.shape
    sequences = m.whole.shape[0] * share // LEN
    lengths = [m.lengths[fabric.row * sequences + number] for number in range(sequences)]
    middle = list(range(2, fabric.batches - 1))
    final = fabric.batches - 1
    stores = []

    def whole(col):
        return m.whole.at[col]

    def slot(col):
        return m.terms.at[col]

    def slot_p(col):
        return m.probed.at[:, col]

    def onto_blocks(layer):
        return lambda col: blocks[layer].at[:, col]

    def half(ref, number):
        return ref.at[:, number * (model // 2) : (number + 1) * (model // 2)]

    def half_p(ref, number):
        count = fabric.batches // 2
        return ref.at[number * count : (number + 1) * count]

    def store(source, target, number):
        made = pltpu.make_async_copy(source, target, m.store_sem.at[number])
        made.start()
        return made

    def gather_shard():
        return Gather(fabric, m.shard, whole, half)

    def gather_blocks(number, layer):
        return Gather(fabric, m.exchanged.at[number], onto_blocks(layer), half_p)

    def exchange(number, place):
        return fabric.exchange(m.pieces.at[place], m.exchanged.at[number])

    def reduce_terms():
        return Reduce(fabric, slot, m.beside, m.landed, m.relayed, half)

    def reduce_probed():
        return Reduce(fabric, slot_p, m.beside_p, m.landed_p, m.relayed_p, half_p)

    def steps(chain, numbers):
        for number in numbers:
            chain.step(number)

    stream = wide(m.tokens[...])
    set_shard(stream * inverse_of(stream) * m.gains[0:1, :], m.shard, m.pieces.at[0])
    ready()
    arrived = exchange(0, 0)
    gathered = gather_shard()
    gathered.relay()
    arrived()
    gathered_blocks = gather_blocks(0, 0)
    gathered.forward()
    gathered.finish()
    loads.need(0, *PROJECTIONS)
    project(m.whole, weights, 0, m.acc, cut)
    gathered_blocks.relay()
    primal_attention(lengths, m.acc, *tables, *kept[0], blended[0])
    fetches[0].step(1)
    loads.need(0, "out_weight")
    out_terms(blended[0], m.out_weight_held, 0, m.terms, cut)
    gathered.drain()
    summing = reduce_terms()
    gathered_blocks.forward()
    summing.spread()
    gathered_blocks.finish()
    stores.append(store(blocks[0], m.blocks0, 0))
    loads.need(0, *PROBES)
    probe_terms(blocks[0], probes, 0, partial[0])
    backs[0].step(1)
    summing.relay()
    total = summing.finish()

    rounded = low(wide(m.tokens[...]) + total)
    m.stream[...] = rounded
    stream = wide(rounded)
    set_shard(stream * inverse_of(stream) * m.gains[1:2, :], m.shard, m.pieces.at[1])
    arrived = exchange(1, 1)
    gathered = gather_shard()
    gathered.relay()
    steps(backs[0], middle)
    steps(fetches[0], middle)
    arrived()
    gathered_blocks = gather_blocks(1, 1)
    gathered.forward()
    gathered.finish()
    loads.need(1, *PROJECTIONS)
    project(m.whole, weights, 1, m.acc, cut)
    gathered_blocks.relay()
    backs[0].step(final)
    primal_attention(lengths, m.acc, *tables, *kept[1], blended[1])
    fetches[0].step(final)
    gathered_blocks.forward()
    gathered_blocks.finish()
    stores.append(store(blocks[1], m.blocks1, 1))
    loads.need(1, *PROBES)
    probe_terms(blocks[1], probes, 1, partial[1])
    backs[0].finish(m.acc)
    backs[1].step(1)
    fetches[1].step(1)
    tangent_attention(lengths, m.acc, *tables, *kept[0], m.mixed)
    fetches[0].finish()
    stores.append(store(blended_all[0], m.blended_all0, 2))
    fabric.drain()
    loads.need(0, "out_probe")
    out_probe_terms(blended_all[0], m.out_probe_held, 0, m.probed)
    summing_p = reduce_probed()
    out_terms(m.mixed, m.out_weight_held, 0, m.terms, cut)
    summing = reduce_terms()

    summing_p.spread()
    summing_p.relay()
    summing.spread()
    steps(backs[1], middle)
    summing.relay()
    m.pieces[0] = low(summing_p.finish())
    arrived = exchange(2, 0)
    steps(fetches[1], middle)
    backs[1].step(final)
    total = summing.finish()
    arrived()
    change = joined(total, m.exchanged.at[2])
    m.tangent[...] = change
    stream = wide(m.stream[...])
    inverse = inverse_of(stream)
    shift = jnp.mean(stream * change, axis=-1, keepdims=True)
    m.shard[...] = low(
        m.gains[1:2, :] * (change * inverse - stream * inverse * inverse * inverse * shift)
    )
    gathered = gather_shard()
    gathered.relay()
    fetches[1].step(final)
    gathered.forward()
    gathered.finish()
    fabric.drain()
    project(m.whole, weights, 1, m.acc, cut)
    backs[1].finish(m.moved)
    m.acc[...] += m.moved[...]
    tangent_attention(lengths, m.acc, *tables, *kept[1], m.mixed)
    fetches[1].finish()
    stores.append(store(blended_all[1], m.blended_all1, 3))
    loads.need(1, "out_probe", "out_weight")
    out_probe_terms(blended_all[1], m.out_probe_held, 1, m.probed)
    summing_p = reduce_probed()
    out_terms(m.mixed, m.out_weight_held, 1, m.terms, cut)
    summing = reduce_terms()

    summing_p.spread()
    summing_p.relay()
    summing.spread()
    summing.relay()
    fabric.drain_chains()
    m.pieces[1] = low(summing_p.finish())
    arrived = exchange(3, 1)
    total = summing.finish()
    arrived()
    first_row = fabric.col * share
    sequence = lax.div(first_row, LEN)
    position = first_row - sequence * LEN + lax.broadcasted_iota(jnp.int32, (share, 1), 0)
    valid = position < m.lengths[fabric.row * sequences + sequence]
    cotangent = jnp.where(valid, 1.0, 0.0) * (
        m.tangent[...] + joined(total, m.exchanged.at[3])
    )
    m.tangent[...] = cotangent
    set_shard(cotangent, m.shard, m.pieces.at[0])
    gathered = gather_shard()
    arrived = exchange(4, 0)
    gathered.relay()
    gathered.forward()
    gathered.finish()
    fabric.drain()
    for made in stores:
        made.wait()
    mixed_grads(m.whole, m.out_weight_held, 1, m.acc, cut)
    backward_attention(lengths, m.acc, *tables, *kept[1], grads[1])
    grad_fetches[1].step(1)
    grad_terms(grads[1], weights, 1, m.terms, cut)
    summing = reduce_terms()

    summing.spread()
    summing.relay()
    steps(grad_fetches[1], middle)
    total = summing.finish()
    stream = wide(m.stream[...])
    inverse = inverse_of(stream)
    scaled = total * m.gains[1:2, :]
    shift = jnp.mean(stream * scaled, axis=-1, keepdims=True)
    cotangent = m.tangent[...] + inverse * (scaled - stream * inverse * inverse * shift)
    set_shard(cotangent, m.shard, m.pieces.at[1])
    gathered = gather_shard()
    last_arrived = exchange(5, 1)
    gathered.relay()
    arrived()
    gathered_blocks = gather_blocks(4, 0)
    grad_fetches[1].step(final)
    gathered.forward()
    gathered.finish()
    mixed_grads(m.whole, m.out_weight_held, 0, m.acc, cut)
    gathered_blocks.relay()
    backward_attention(lengths, m.acc, *tables, *kept[0], grads[0])
    grad_fetches[0].step(1)
    last_arrived()
    gathered_last = gather_blocks(5, 1)
    gathered_blocks.forward()
    gathered_blocks.finish()
    last_stores = [store(blocks[0], m.cotangents1, 0)]
    gathered_last.relay()
    grad_fetches[1].finish()
    last_stores.append(store(grads_held[1], m.grads_all1, 1))
    steps(grad_fetches[0], middle)
    gathered_last.forward()
    gathered_last.finish()
    last_stores.append(store(blocks[1], m.cotangents0, 2))
    grad_fetches[0].step(final)
    grad_fetches[0].finish()
    last_stores.append(store(grads_held[0], m.grads_all0, 3))
    for made in last_stores:
        made.wait()
    fabric.drain()
    fabric.drain_chains()


def product_kernel(layers, *refs):
    inputs, (query_out, key_out, value_out, out_out) = refs[:-4], refs[-4:]
    layer = pl.program_id(0)
    query_width, key_width = query_out.shape[-1], key_out.shape[-1]
    for number in range(layers):
        blocks, grads, blended, cotangent = inputs[4 * number : 4 * number + 4]

        @pl.when(layer == number)
        def _():
            product = contract_rows(blocks[...], grads[...])
            query_out[0] = product[:, :query_width]
            key_out[0] = product[:, query_width : query_width + key_width]
            value_out[0] = product[:, query_width + key_width :]
            out_out[0] = contract_rows(blended[...], cotangent[...])


CUTS = 4


def body(
    tokens,
    lengths,
    norm_gains,
    query_weight,
    key_weight,
    value_weight,
    out_weight,
    query_probe,
    key_probe,
    value_probe,
    out_probe,
):
    width = lax.axis_size("tensor")
    batches = lax.axis_size("dp")
    sizes = (batches, width)
    tensor_index = lax.axis_index("tensor")
    share, model = tokens.shape
    group = share * width
    assert LEN % share == 0
    layers = query_weight.shape[0]
    assert layers == 2
    half_width = key_weight.shape[2]
    query_width = query_weight.shape[2]
    paired = half_width < HD
    key_width = 2 * half_width if paired else half_width
    sent_width = query_width + 2 * half_width
    block = query_probe.shape[1]
    cosine, sine = rope_tables(LEN, HD)
    lower_half = tensor_index % 2 == 0

    def swapped(value):
        pairs = [(source, source ^ 1) for source in range(width)]
        return lax.ppermute(value, "tensor", pairs)

    def join_halves(own_part):
        other_part = swapped(own_part)
        return jnp.where(
            lower_half,
            jnp.concatenate([own_part, other_part], axis=-1),
            jnp.concatenate([other_part, own_part], axis=-1),
        )

    def split_halves(values):
        first, second = values[:, :half_width], values[:, half_width:]
        own_part = jnp.where(lower_half, first, second)
        other_part = jnp.where(lower_half, second, first)
        return low(wide(own_part) + wide(swapped(other_part)))

    parts = [key_weight, value_weight, key_probe, value_probe]
    if paired:
        parts = [join_halves(part) for part in parts]
    key_full, value_full, key_probe_full, value_probe_full = parts

    def to_send(grads):
        if not paired:
            return grads
        return jnp.concatenate(
            [
                grads[:, :query_width],
                split_halves(grads[:, query_width : query_width + key_width]),
                split_halves(grads[:, query_width + key_width :]),
            ],
            axis=-1,
        )

    bf, f32 = jnp.bfloat16, jnp.float32
    chips = width // 2
    wide_width = query_width + 2 * key_width
    rows_in_all = batches * group

    def flow():
        inputs = dict(
            lengths=lengths,
            tokens=tokens,
            gains=norm_gains,
            cosine=cosine,
            sine=sine,
            query_weight=query_weight,
            key_weight=key_full,
            value_weight=value_full,
            out_weight=out_weight,
            query_probe=query_probe,
            key_probe=key_probe_full,
            value_probe=value_probe_full,
            out_probe=out_probe,
        )
        blocks_shape = (batches, width, share, block)
        outputs = dict(
            blocks0=blocks_shape,
            blocks1=blocks_shape,
            blended_all0=(batches, group, query_width),
            blended_all1=(batches, group, query_width),
            cotangents0=blocks_shape,
            cotangents1=blocks_shape,
            grads_all0=(batches, group, wide_width),
            grads_all1=(batches, group, wide_width),
        )
        held = {
            name + "_held": pltpu.VMEM(value.shape, bf)
            for name, value in list(inputs.items())[5:]
        }
        scratch = dict(
            whole=pltpu.VMEM((width, share, model), bf),
            blocks=pltpu.VMEM((layers,) + blocks_shape, bf),
            terms=pltpu.VMEM((width, share, model), bf),
            probed=pltpu.VMEM(blocks_shape, bf),
            beside=pltpu.VMEM((chips, share, model), bf),
            landed=pltpu.VMEM((chips, share, model), bf),
            beside_p=pltpu.VMEM((chips, batches, share, block), bf),
            landed_p=pltpu.VMEM((chips, batches, share, block), bf),
            relayed=pltpu.VMEM((2, share, model // 2), bf),
            relayed_p=pltpu.VMEM((2, batches // 2, share, block), bf),
            partial=pltpu.VMEM((layers, batches, group, wide_width), bf),
            returned=pltpu.VMEM((layers, 2, batches - 1, group, wide_width), bf),
            queries=pltpu.VMEM((layers, group, query_width), bf),
            keys=pltpu.VMEM((layers, group, key_width), bf),
            values=pltpu.VMEM((layers, group, key_width), bf),
            blended=pltpu.VMEM((layers, group, query_width), bf),
            blended_all=pltpu.VMEM((layers, batches, group, query_width), bf),
            mixed=pltpu.VMEM((group, query_width), bf),
            grads=pltpu.VMEM((layers, group, wide_width), bf),
            grads_held=pltpu.VMEM((layers, batches, group, wide_width), bf),
            acc=pltpu.VMEM((group, wide_width), f32),
            moved=pltpu.VMEM((group, wide_width), f32),
            shard=pltpu.VMEM((share, model), bf),
            stream=pltpu.VMEM((share, model), bf),
            tangent=pltpu.VMEM((share, model), f32),
            pieces=pltpu.VMEM((2, batches, share, block), bf),
            exchanged=pltpu.VMEM((6, batches, share, block), bf),
            **held,
            send=pltpu.SemaphoreType.DMA((semaphore_count(sizes),)),
            recv=pltpu.SemaphoreType.DMA((semaphore_count(sizes),)),
            load_sem=pltpu.SemaphoreType.DMA((layers * len(held),)),
            store_sem=pltpu.SemaphoreType.DMA((4,)),
        )
        vmem = pl.BlockSpec(memory_space=pltpu.VMEM)
        anywhere = pl.BlockSpec(memory_space=pl.ANY)
        return pl.pallas_call(
            functools.partial(
                flow_kernel, sizes, model // CUTS, [*inputs, *outputs, *scratch]
            ),
            out_shape=[jax.ShapeDtypeStruct(shape, bf) for shape in outputs.values()],
            in_specs=[pl.BlockSpec(memory_space=pltpu.SMEM)]
            + [vmem] * 4
            + [anywhere] * len(held),
            out_specs=[anywhere] * len(outputs),
            scratch_shapes=list(scratch.values()),
            compiler_params=pltpu.CompilerParams(
                collective_id=0, has_side_effects=True, vmem_limit_bytes=67043328
            ),
        )(*inputs.values())

    def cost(flops, moved_bytes):
        return pl.CostEstimate(flops=flops, bytes_accessed=moved_bytes, transcendentals=0)

    def products(per_layer):
        out_block = out_probe.shape[2]
        by_rows = query_width % (CUTS * HD) == 0
        blended_cut = query_width // CUTS if by_rows else query_width
        out_cut = out_block if by_rows else out_block // CUTS
        in_specs, args = [], []
        for number, (blocks, grads, blended, cotangents) in enumerate(per_layer):

            def place(i, j, number=number):
                return (0, jnp.clip((i - number) * CUTS + j, 0, CUTS - 1))

            def still(i, j):
                return (0, 0)

            in_specs += [
                pl.BlockSpec((rows_in_all, block // CUTS), place),
                pl.BlockSpec((rows_in_all, sent_width), still),
                pl.BlockSpec((rows_in_all, blended_cut), place if by_rows else still),
                pl.BlockSpec((rows_in_all, out_cut), still if by_rows else place),
            ]
            args += [
                blocks.reshape(rows_in_all, block),
                grads.reshape(rows_in_all, sent_width),
                blended.reshape(rows_in_all, query_width),
                cotangents.reshape(rows_in_all, out_block),
            ]
        shapes = [
            (block, query_width),
            (block, half_width),
            (block, half_width),
            (query_width, out_block),
        ]
        return pl.pallas_call(
            functools.partial(product_kernel, layers),
            grid=(layers, CUTS),
            in_specs=in_specs,
            out_specs=[
                pl.BlockSpec((1, rows // CUTS, columns), lambda i, j: (i, j, 0))
                for rows, columns in shapes[:3]
            ]
            + [
                pl.BlockSpec(
                    (1, blended_cut, out_cut),
                    lambda i, j: (i, j, 0) if by_rows else (i, 0, j),
                )
            ],
            out_shape=[
                jax.ShapeDtypeStruct((layers, rows, columns), f32) for rows, columns in shapes
            ],
            compiler_params=pltpu.CompilerParams(
                dimension_semantics=("arbitrary", "arbitrary")
            ),
            cost_estimate=cost(2 * rows_in_all * block * query_width * 4, 32 << 20),
        )(*args)

    results = flow()
    blocks0, blocks1, blended0, blended1, cotangents0, cotangents1, grads0, grads1 = results
    sent = [to_send(grads.reshape(rows_in_all, wide_width)) for grads in (grads0, grads1)]
    return tuple(
        products(
            [
                (blocks0, sent[0], blended0, cotangents0),
                (blocks1, sent[1], blended1, cotangents1),
            ]
        )
    )


def solution(mesh):
    placed = (
        P(("dp", "tensor"), None),
        P(),
        P(),
        P(None, None, "tensor"),
        P(None, None, "tensor"),
        P(None, None, "tensor"),
        P(None, "tensor", None),
        P(None, "dp", "tensor"),
        P(None, "dp", "tensor"),
        P(None, "dp", "tensor"),
        P(None, "tensor", "dp"),
    )
    return jax.shard_map(
        body,
        mesh=mesh,
        in_specs=placed,
        out_specs=(
            P(None, "dp", "tensor"),
            P(None, "dp", "tensor"),
            P(None, "dp", "tensor"),
            P(None, "tensor", "dp"),
        ),
        check_vma=False,
    )
```

```python
import functools
import math
import types

import jax
import jax.numpy as jnp
import numpy as np
from jax import lax
from jax.experimental import pallas as pl
from jax.experimental.pallas import tpu as pltpu
from jax.sharding import PartitionSpec as P

HD = 128
LEN = 256
EPS = 1e-05
THETA = 500000.0
MESH = pl.DeviceIdType.MESH
SCALE = 1.0 / math.sqrt(HD)


def low(values):
    return values.astype(jnp.bfloat16)


def wide(values):
    return values.astype(jnp.float32)


def matmul(left_side, right_side):
    return jnp.dot(left_side, right_side, preferred_element_type=jnp.float32)


def contract_rows(left_side, right_side):
    return lax.dot_general(
        left_side, right_side, (((0,), (0,)), ((), ())), preferred_element_type=jnp.float32
    )


def contract_last(left_side, right_side):
    return lax.dot_general(
        left_side, right_side, (((1,), (1,)), ((), ())), preferred_element_type=jnp.float32
    )


def rope_tables(length, head_size):
    frequency = np.exp(-math.log(THETA) * 2.0 * np.arange(head_size // 2) / head_size)
    angles = np.arange(length)[:, None] * frequency.astype(np.float32)[None, :]
    cosine, sine = np.cos(angles), np.sin(angles)
    return (
        np.concatenate([cosine, cosine], axis=-1).astype(np.float32),
        np.concatenate([-sine, sine], axis=-1).astype(np.float32),
    )


def flip(index, mask):
    result = index
    bit = 1
    while bit <= mask:
        if mask & bit:
            result = result + bit - 2 * bit * lax.rem(lax.div(index, bit), 2)
        bit *= 2
    return result


def semaphore_count(sizes):
    batches, width = sizes
    return 24 * width + 22 * batches


class Fabric:
    def __init__(self, sizes, send, recv):
        self.batches, self.width = sizes
        self.chips = self.width // 2
        self.row = lax.axis_index("dp")
        self.col = lax.axis_index("tensor")
        self.send, self.recv, self.used = send, recv, 0
        self.pending = []
        self.guarded = []

    def copy(self, source, target, row, col):
        number = self.used
        self.used += 1
        assert number < semaphore_count((self.batches, self.width))
        made = pltpu.make_async_remote_copy(
            src_ref=source,
            dst_ref=target,
            send_sem=self.send.at[number],
            recv_sem=self.recv.at[number],
            device_id=(row, col),
            device_id_type=MESH,
        )
        made.start()
        self.pending.append(made)
        return made

    def drain(self, only=None):
        for made in self.pending if only is None else only:
            made.wait_send()
        gone = set() if only is None else {id(made) for made in only}
        self.pending = [made for made in self.pending if gone and id(made) not in gone]

    def drain_chains(self):
        for condition, made in self.guarded:
            pl.when(condition)(made.wait_send)
        self.guarded = []

    def mate(self):
        return flip(self.col, 1)

    def peer(self, step):
        return flip(self.col, 2 * step)

    def batch(self, step):
        return flip(self.row, step)

    def greet(self, along_tensor=True):
        barrier = pltpu.get_barrier_semaphore()
        peers = [(self.batch(step), self.col) for step in range(1, self.batches)]
        if along_tensor:
            peers += [(self.row, self.peer(step)) for step in range(1, self.chips)]
            peers.append((self.row, self.mate()))
        for peer in peers:
            pl.semaphore_signal(barrier, inc=1, device_id=peer, device_id_type=MESH)
        return lambda: pl.semaphore_wait(barrier, len(peers))

    def exchange(self, source, target):
        made = [
            self.copy(
                source.at[self.batch(step)], target.at[self.row], self.batch(step), self.col
            )
            for step in range(1, self.batches)
        ]
        target[self.row] = source[self.row]

        def finish():
            for copy in made:
                copy.wait_recv()

        return finish

    def reserve(self, count):
        first = self.used
        self.used += count
        assert self.used <= semaphore_count((self.batches, self.width))
        return first

    def hop(self, source, target, number, way):
        return pltpu.make_async_remote_copy(
            src_ref=source,
            dst_ref=target,
            send_sem=self.send.at[number],
            recv_sem=self.recv.at[number],
            device_id=(jnp.clip(self.row + way, 0, self.batches - 1), self.col),
            device_id_type=MESH,
        )

    def rank(self, way):
        return self.row if way > 0 else self.batches - 1 - self.row


class Gather:
    def __init__(self, fabric, source, slot, half):
        self.fabric, self.slot, self.half = fabric, slot, half
        self.made, self.beside = [], []
        there = slot(fabric.col)
        if fabric.chips == 4:
            self.first = [
                self.copy(half(source, 0), half(there, 0), fabric.peer(1)),
                self.copy(half(source, 1), half(there, 1), fabric.peer(2)),
            ]
            self.second = [
                self.copy(half(source, 1), half(there, 1), fabric.peer(1)),
                self.copy(half(source, 0), half(there, 0), fabric.peer(2)),
            ]
        else:
            self.direct = [
                self.copy(source, there, fabric.peer(step)) for step in range(1, fabric.chips)
            ]
        self.beside.append(self.copy(source, there, fabric.mate()))
        there[...] = source[...]

    def copy(self, source, target, col):
        made = self.fabric.copy(source, target, self.fabric.row, col)
        self.made.append(made)
        return made

    def beside_too(self, piece):
        self.beside.append(self.copy(piece, piece, self.fabric.mate()))

    def relay(self):
        fabric = self.fabric
        self.relayed = []
        if fabric.chips == 4:
            for number in range(2):
                self.first[number].wait_recv()
                piece = self.half(self.slot(fabric.peer(1 + number)), number)
                self.relayed.append(self.copy(piece, piece, fabric.peer(2 - number)))
                self.beside_too(piece)

    def forward(self):
        fabric = self.fabric
        if fabric.chips == 4:
            for number in range(2):
                self.second[number].wait_recv()
                self.beside_too(self.half(self.slot(fabric.peer(1 + number)), 1 - number))
            for number in range(2):
                self.relayed[number].wait_recv()
                self.beside_too(self.half(self.slot(fabric.peer(3)), number))
        else:
            for step in range(1, fabric.chips):
                self.direct[step - 1].wait_recv()
                self.beside_too(self.slot(fabric.peer(step)))

    def finish(self):
        for made in self.beside:
            made.wait_recv()

    def drain(self):
        self.fabric.drain(self.made)


class Reduce:
    def __init__(self, fabric, slot, beside, landed, relayed, half):
        self.fabric, self.slot, self.half = fabric, slot, half
        self.beside, self.landed, self.relayed = beside, landed, relayed
        self.paired = [
            fabric.copy(
                slot(flip(fabric.mate(), 2 * step)), beside.at[step], fabric.row, fabric.mate()
            )
            for step in range(fabric.chips)
        ]

    def add(self, step):
        self.paired[step].wait_recv()
        own = self.slot(self.fabric.peer(step))
        own[...] = low(wide(own[...]) + wide(self.beside[step]))

    def part(self, step, number):
        return self.half(self.slot(self.fabric.peer(step)), number)

    def send(self, step, number=None):
        fabric = self.fabric
        if number is None:
            source, target = self.slot(fabric.peer(step)), self.landed.at[step]
        else:
            source, target = self.part(step, number), self.half(self.landed.at[step], number)
        self.sent.append((step, number, fabric.copy(source, target, fabric.row, fabric.peer(step))))

    def spread(self):
        fabric = self.fabric
        self.sent = []
        if fabric.chips == 4:
            self.add(3)
            self.add(1)
            self.passed = [
                fabric.copy(
                    self.part(3, number),
                    self.relayed.at[number],
                    fabric.row,
                    fabric.peer(1 + number),
                )
                for number in range(2)
            ]
            self.add(2)
            self.send(1, 0)
        else:
            order = list(range(fabric.chips - 1, 0, -1))
            for place, step in enumerate(order):
                self.add(step)
                if place:
                    self.send(order[place - 1])
        self.paired[0].wait_recv()
        self.total = wide(self.slot(fabric.col)[...]) + wide(self.beside[0])
        if fabric.chips == 4:
            self.send(2, 1)
        elif order:
            self.send(order[-1])

    def relay(self):
        if self.fabric.chips == 4:
            for number in range(2):
                self.passed[number].wait_recv()
                part = self.part(2 - number, number)
                part[...] = low(wide(part[...]) + wide(self.relayed[number]))
                self.send(2 - number, number)

    def finish(self):
        result = self.total
        for step, number, made in self.sent:
            made.wait_recv()
        for step in range(1, self.fabric.chips):
            if self.fabric.chips != 4 or step < 3:
                result = result + wide(self.landed[step])
        return result


class GatherChain:
    def __init__(self, fabric, source, slot):
        self.fabric, self.source, self.slot = fabric, source, slot
        self.first = fabric.reserve(2 * (fabric.batches - 1))

    def number(self, way, step):
        return self.first + (0 if way > 0 else self.fabric.batches - 1) + step - 1

    def arrive(self, step):
        fabric = self.fabric
        for way in (1, -1):
            piece = jnp.clip(fabric.row - way * step, 0, fabric.batches - 1)
            place = self.slot(piece)
            made = fabric.hop(place, place, self.number(way, step), way)
            pl.when(fabric.rank(way) >= step)(made.wait_recv)

    def step(self, step):
        fabric = self.fabric
        if step > 1:
            self.arrive(step - 1)
        for way in (1, -1):
            piece = jnp.clip(fabric.row - way * (step - 1), 0, fabric.batches - 1)
            place = self.slot(piece)
            source = self.source if step == 1 else place
            made = fabric.hop(source, place, self.number(way, step), way)
            rank = fabric.rank(way)
            condition = (rank >= step - 1) & (rank < fabric.batches - 1)
            pl.when(condition)(made.start)
            fabric.guarded.append((condition, made))
        if step == 1:
            self.slot(fabric.row)[...] = self.source[...]

    def finish(self):
        self.arrive(self.fabric.batches - 1)


class ChainPair:
    def __init__(self, fabric, source, target):
        count = source.shape[0] // 2
        self.chains = [
            GatherChain(
                fabric,
                source.at[first : first + count],
                lambda piece, first=first: target.at[piece, first : first + count],
            )
            for first in (0, count)
        ]

    def step(self, step):
        for chain in self.chains:
            chain.step(step)

    def finish(self):
        for chain in self.chains:
            chain.finish()


class ScatterChain:
    def __init__(self, fabric, source, landed):
        self.fabric, self.source, self.landed = fabric, source, landed
        self.first = fabric.reserve(2 * (fabric.batches - 1))

    def hop(self, source, way, step):
        side = 0 if way > 0 else 1
        number = self.first + side * (self.fabric.batches - 1) + step - 1
        return self.fabric.hop(source, self.landed.at[side, step - 1], number, way)

    def step(self, step):
        fabric = self.fabric
        last = fabric.batches - 1
        for way in (1, -1):
            side = 0 if way > 0 else 1
            rank = fabric.rank(way)
            goal = jnp.clip(fabric.batches + rank - step, 0, last)
            goal = goal if way > 0 else last - goal
            own = self.hop(self.source.at[goal], way, step)
            pl.when(rank == 0)(own.start)
            fabric.guarded.append((rank == 0, own))
            if step > 1:
                buffer = self.source.at[goal]
                summed = self.hop(buffer, way, step)
                before = self.hop(buffer, way, step - 1)
                condition = (rank > 0) & (rank < step)

                @pl.when(condition)
                def _():
                    before.wait_recv()
                    buffer[...] = low(wide(buffer[...]) + wide(self.landed[side, step - 2]))
                    summed.start()

                fabric.guarded.append((condition, summed))

    def finish(self, total):
        fabric = self.fabric
        last = fabric.batches - 1
        total[...] = wide(self.source[fabric.row])
        for way in (1, -1):
            side = 0 if way > 0 else 1
            made = self.hop(self.source.at[fabric.row], way, last)

            @pl.when(fabric.rank(way) > 0)
            def _():
                made.wait_recv()
                total[...] += wide(self.landed[side, last - 1])


def inverse_of(stream):
    return lax.rsqrt(jnp.mean(stream * stream, axis=-1, keepdims=True) + EPS)


def set_shard(values, shard, pieces):
    rounded = low(values)
    shard[...] = rounded
    block = pieces.shape[-1]
    for number in range(pieces.shape[0]):
        pieces[number] = rounded[:, number * block : (number + 1) * block]


def joined(total, exchanged):
    block = exchanged.shape[-1]
    return jnp.concatenate(
        [
            total[:, number * block : (number + 1) * block] + wide(exchanged[number])
            for number in range(exchanged.shape[0])
        ],
        axis=-1,
    )


def turn(values, cosine, sine, direction):
    other = pltpu.roll(values, HD // 2, 1)
    if direction > 0:
        return values * cosine + other * sine
    return values * cosine - other * sine


def head(index):
    return slice(index * HD, (index + 1) * HD)


def allowed_keys(length):
    row_index = lax.broadcasted_iota(jnp.int32, (LEN, LEN), 0)
    column_index = lax.broadcasted_iota(jnp.int32, (LEN, LEN), 1)
    return (column_index <= row_index) & (column_index < length)


def softmax_weights(queries, keys, allowed):
    powers = jnp.where(allowed, jnp.exp(contract_last(queries, keys) * SCALE), 0.0)
    return powers / jnp.sum(powers, axis=-1, keepdims=True)


def centred(weights, values):
    return weights * (values - jnp.sum(weights * values, axis=-1, keepdims=True))


def each_head(total_rows, query_width, key_width):
    repeat = query_width // key_width
    for seq in range(total_rows // LEN):
        rows = slice(seq * LEN, (seq + 1) * LEN)
        for number in range(key_width // HD):
            yield seq, rows, number, range(number * repeat, (number + 1) * repeat)


def repeated(count, function):
    def once(index, carry):
        function(index)
        return carry

    lax.fori_loop(0, count, once, 0)


def columns(index, size):
    return pl.ds(pl.multiple_of(index * size, size), size)


def rows_of(block):
    return block.reshape(-1, block.shape[-1])


def project(source, weights, layer, acc, cut):
    acc[...] = jnp.zeros_like(acc)
    widths = [weight.shape[-1] for weight in weights]

    def once(index):
        at = columns(index, cut)
        part = rows_of(source[:, :, at])
        start = 0
        for weight, width in zip(weights, widths):
            acc[:, start : start + width] += matmul(part, weight[layer, at, :])
            start += width

    repeated(source.shape[-1] // cut, once)


def probe_terms(blocks, probes, layer, partial):
    def once(index):
        rows = rows_of(blocks[index])
        start = 0
        for probe in probes:
            width = probe.shape[-1]
            partial[index, :, start : start + width] = low(matmul(rows, probe[layer]))
            start += width

    repeated(blocks.shape[0], once)


def out_terms(mixed, weight, layer, terms, cut):
    def once(index):
        at = columns(index, cut)
        terms[:, :, at] = low(matmul(mixed[...], weight[layer, :, at])).reshape(
            terms.shape[0], terms.shape[1], cut
        )

    repeated(terms.shape[-1] // cut, once)


def out_probe_terms(blended_all, probe, layer, probed):
    def once(index):
        probed[index] = low(matmul(blended_all[index], probe[layer])).reshape(probed.shape[1:])

    repeated(probed.shape[0], once)


def primal_attention(lengths, acc, cosine, sine, queries, keys, values, blended):
    total_rows, query_width = queries.shape
    key_width = keys.shape[1]
    values[...] = low(acc[:, query_width + key_width :])
    for seq, rows, number, members in each_head(total_rows, query_width, key_width):
        allowed = allowed_keys(lengths[seq])
        key_at = head(query_width // HD + number)
        key_head = low(turn(acc[rows, key_at], cosine[...], sine[...], 1))
        keys[rows, head(number)] = key_head
        value_head = values[rows, head(number)]
        for member in members:
            query_head = low(turn(acc[rows, head(member)], cosine[...], sine[...], 1))
            queries[rows, head(member)] = query_head
            weights = low(softmax_weights(query_head, key_head, allowed))
            blended[rows, head(member)] = low(matmul(weights, value_head))


def tangent_attention(lengths, acc, cosine, sine, queries, keys, values, mixed):
    query_width, key_width = queries.shape[1], keys.shape[1]
    for seq, rows, number, members in each_head(queries.shape[0], query_width, key_width):
        allowed = allowed_keys(lengths[seq])
        key_head = keys[rows, head(number)]
        value_head = values[rows, head(number)]
        key_at = query_width // HD + number
        value_at = key_at + key_width // HD
        moved_key = low(turn(acc[rows, head(key_at)], cosine[...], sine[...], 1))
        moved_value = low(acc[rows, head(value_at)])
        for member in members:
            query_head = queries[rows, head(member)]
            moved_query = low(turn(acc[rows, head(member)], cosine[...], sine[...], 1))
            weights = softmax_weights(query_head, key_head, allowed)
            scores = SCALE * (
                contract_last(moved_query, key_head) + contract_last(query_head, moved_key)
            )
            moved_weights = low(centred(weights, scores))
            mixed[rows, head(member)] = low(
                matmul(moved_weights, value_head) + matmul(low(weights), moved_value)
            )


def mixed_grads(cotangent, weight, layer, acc, cut):
    query_width = weight.shape[1]
    acc[:, :query_width] = jnp.zeros((acc.shape[0], query_width), jnp.float32)

    def once(index):
        at = columns(index, cut)
        acc[:, :query_width] += contract_last(rows_of(cotangent[:, :, at]), weight[layer, :, at])

    repeated(cotangent.shape[-1] // cut, once)


def backward_attention(lengths, acc, cosine, sine, queries, keys, values, grads):
    query_width, key_width = queries.shape[1], keys.shape[1]
    for seq, rows, number, members in each_head(queries.shape[0], query_width, key_width):
        allowed = allowed_keys(lengths[seq])
        key_head = keys[rows, head(number)]
        value_head = values[rows, head(number)]
        key_at = query_width // HD + number
        value_at = key_at + key_width // HD
        key_total = jnp.zeros((LEN, HD), jnp.float32)
        value_total = jnp.zeros((LEN, HD), jnp.float32)
        for member in members:
            query_head = queries[rows, head(member)]
            mixed = low(acc[rows, head(member)])
            weights = softmax_weights(query_head, key_head, allowed)
            value_total = value_total + contract_rows(low(weights), mixed)
            scores = low(centred(weights, contract_last(mixed, value_head)) * SCALE)
            grads[rows, head(member)] = low(
                turn(matmul(scores, key_head), cosine[...], sine[...], -1)
            )
            key_total = key_total + contract_rows(scores, query_head)
        grads[rows, head(key_at)] = low(turn(key_total, cosine[...], sine[...], -1))
        grads[rows, head(value_at)] = low(value_total)


def grad_terms(grads, weights, layer, terms, cut):
    def once(index):
        at = columns(index, cut)
        total = 0.0
        start = 0
        for weight in weights:
            width = weight.shape[-1]
            total = total + contract_last(grads[:, start : start + width], weight[layer, at, :])
            start += width
        terms[:, :, at] = low(total).reshape(terms.shape[0], terms.shape[1], cut)

    repeated(terms.shape[-1] // cut, once)


class Loads:
    def __init__(self, pairs, layers, semaphores):
        self.made = {}
        number = 0
        for layer in range(layers):
            for name, source, target in pairs:
                made = pltpu.make_async_copy(
                    source.at[layer], target.at[layer], semaphores.at[number]
                )
                made.start()
                self.made[name, layer] = made
                number += 1

    def need(self, layer, *names):
        for name in names:
            self.made.pop((name, layer)).wait()


PROJECTIONS = ("query_weight", "key_weight", "value_weight")
PROBES = ("query_probe", "key_probe", "value_probe")


def flow_kernel(sizes, cut, names, *refs):
    m = types.SimpleNamespace(**dict(zip(names, refs)))
    fabric = Fabric(sizes, m.send, m.recv)
    ready = fabric.greet()
    loaded = PROJECTIONS + ("out_weight",) + PROBES + ("out_probe",)
    loads = Loads(
        [(name, getattr(m, name), getattr(m, name + "_held")) for name in loaded],
        m.query_weight.shape[0],
        m.load_sem,
    )
    weights = [getattr(m, name + "_held") for name in PROJECTIONS]
    probes = [getattr(m, name + "_held") for name in PROBES]
    tables = (m.cosine, m.sine)
    kept = [(m.queries.at[layer], m.keys.at[layer], m.values.at[layer]) for layer in range(2)]
    blended = [m.blended.at[layer] for layer in range(2)]
    blended_all = [m.blended_all.at[layer] for layer in range(2)]
    partial = [m.partial.at[layer] for layer in range(2)]
    grads = [m.grads.at[layer] for layer in range(2)]
    grads_held = [m.grads_held.at[layer] for layer in range(2)]
    blocks = [m.blocks.at[layer] for layer in range(2)]
    backs = [ScatterChain(fabric, partial[layer], m.returned.at[layer]) for layer in range(2)]
    fetches = [
        GatherChain(fabric, blended[layer], lambda piece, layer=layer: blended_all[layer].at[piece])
        for layer in range(2)
    ]
    grad_fetches = [ChainPair(fabric, grads[layer], grads_held[layer]) for layer in range(2)]
    share, model = m.tokens.shape
    sequences = m.whole.shape[0] * share // LEN
    lengths = [m.lengths[fabric.row * sequences + number] for number in range(sequences)]
    middle = list(range(2, fabric.batches - 1))
    final = fabric.batches - 1
    stores = []

    def whole(col):
        return m.whole.at[col]

    def slot(col):
        return m.terms.at[col]

    def slot_p(col):
        return m.probed.at[:, col]

    def onto_blocks(layer):
        return lambda col: blocks[layer].at[:, col]

    def half(ref, number):
        return ref.at[:, number * (model // 2) : (number + 1) * (model // 2)]

    def half_p(ref, number):
        count = fabric.batches // 2
        return ref.at[number * count : (number + 1) * count]

    def store(source, target, number):
        made = pltpu.make_async_copy(source, target, m.store_sem.at[number])
        made.start()
        return made

    def gather_shard():
        return Gather(fabric, m.shard, whole, half)

    def gather_blocks(number, layer):
        return Gather(fabric, m.exchanged.at[number], onto_blocks(layer), half_p)

    def exchange(number, place):
        return fabric.exchange(m.pieces.at[place], m.exchanged.at[number])

    def reduce_terms():
        return Reduce(fabric, slot, m.beside, m.landed, m.relayed, half)

    def reduce_probed():
        return Reduce(fabric, slot_p, m.beside_p, m.landed_p, m.relayed_p, half_p)

    def steps(chain, numbers):
        for number in numbers:
            chain.step(number)

    stream = wide(m.tokens[...])
    set_shard(stream * inverse_of(stream) * m.gains[0:1, :], m.shard, m.pieces.at[0])
    ready()
    arrived = exchange(0, 0)
    gathered = gather_shard()
    gathered.relay()
    arrived()
    gathered_blocks = gather_blocks(0, 0)
    gathered.forward()
    gathered.finish()
    loads.need(0, *PROJECTIONS)
    project(m.whole, weights, 0, m.acc, cut)
    gathered_blocks.relay()
    primal_attention(lengths, m.acc, *tables, *kept[0], blended[0])
    fetches[0].step(1)
    loads.need(0, "out_weight")
    out_terms(blended[0], m.out_weight_held, 0, m.terms, cut)
    gathered.drain()
    summing = reduce_terms()
    gathered_blocks.forward()
    summing.spread()
    gathered_blocks.finish()
    stores.append(store(blocks[0], m.blocks0, 0))
    loads.need(0, *PROBES)
    probe_terms(blocks[0], probes, 0, partial[0])
    backs[0].step(1)
    summing.relay()
    total = summing.finish()

    rounded = low(wide(m.tokens[...]) + total)
    m.stream[...] = rounded
    stream = wide(rounded)
    set_shard(stream * inverse_of(stream) * m.gains[1:2, :], m.shard, m.pieces.at[1])
    arrived = exchange(1, 1)
    gathered = gather_shard()
    gathered.relay()
    steps(backs[0], middle)
    steps(fetches[0], middle)
    arrived()
    gathered_blocks = gather_blocks(1, 1)
    gathered.forward()
    gathered.finish()
    loads.need(1, *PROJECTIONS)
    project(m.whole, weights, 1, m.acc, cut)
    gathered_blocks.relay()
    backs[0].step(final)
    primal_attention(lengths, m.acc, *tables, *kept[1], blended[1])
    fetches[0].step(final)
    gathered_blocks.forward()
    gathered_blocks.finish()
    stores.append(store(blocks[1], m.blocks1, 1))
    loads.need(1, *PROBES)
    probe_terms(blocks[1], probes, 1, partial[1])
    backs[0].finish(m.acc)
    backs[1].step(1)
    fetches[1].step(1)
    tangent_attention(lengths, m.acc, *tables, *kept[0], m.mixed)
    fetches[0].finish()
    stores.append(store(blended_all[0], m.blended_all0, 2))
    fabric.drain()
    loads.need(0, "out_probe")
    out_probe_terms(blended_all[0], m.out_probe_held, 0, m.probed)
    summing_p = reduce_probed()
    out_terms(m.mixed, m.out_weight_held, 0, m.terms, cut)
    summing = reduce_terms()

    summing_p.spread()
    summing_p.relay()
    summing.spread()
    steps(backs[1], middle)
    summing.relay()
    m.pieces[0] = low(summing_p.finish())
    arrived = exchange(2, 0)
    steps(fetches[1], middle)
    backs[1].step(final)
    total = summing.finish()
    arrived()
    change = joined(total, m.exchanged.at[2])
    m.tangent[...] = change
    stream = wide(m.stream[...])
    inverse = inverse_of(stream)
    shift = jnp.mean(stream * change, axis=-1, keepdims=True)
    m.shard[...] = low(
        m.gains[1:2, :] * (change * inverse - stream * inverse * inverse * inverse * shift)
    )
    gathered = gather_shard()
    gathered.relay()
    fetches[1].step(final)
    gathered.forward()
    gathered.finish()
    fabric.drain()
    project(m.whole, weights, 1, m.acc, cut)
    backs[1].finish(m.moved)
    m.acc[...] += m.moved[...]
    tangent_attention(lengths, m.acc, *tables, *kept[1], m.mixed)
    fetches[1].finish()
    stores.append(store(blended_all[1], m.blended_all1, 3))
    loads.need(1, "out_probe", "out_weight")
    out_probe_terms(blended_all[1], m.out_probe_held, 1, m.probed)
    summing_p = reduce_probed()
    out_terms(m.mixed, m.out_weight_held, 1, m.terms, cut)
    summing = reduce_terms()

    summing_p.spread()
    summing_p.relay()
    summing.spread()
    summing.relay()
    fabric.drain_chains()
    m.pieces[1] = low(summing_p.finish())
    arrived = exchange(3, 1)
    total = summing.finish()
    arrived()
    first_row = fabric.col * share
    sequence = lax.div(first_row, LEN)
    position = first_row - sequence * LEN + lax.broadcasted_iota(jnp.int32, (share, 1), 0)
    valid = position < m.lengths[fabric.row * sequences + sequence]
    cotangent = jnp.where(valid, 1.0, 0.0) * (
        m.tangent[...] + joined(total, m.exchanged.at[3])
    )
    m.tangent[...] = cotangent
    set_shard(cotangent, m.shard, m.pieces.at[0])
    gathered = gather_shard()
    arrived = exchange(4, 0)
    gathered.relay()
    gathered.forward()
    gathered.finish()
    fabric.drain()
    for made in stores:
        made.wait()
    mixed_grads(m.whole, m.out_weight_held, 1, m.acc, cut)
    backward_attention(lengths, m.acc, *tables, *kept[1], grads[1])
    grad_fetches[1].step(1)
    grad_terms(grads[1], weights, 1, m.terms, cut)
    summing = reduce_terms()

    summing.spread()
    summing.relay()
    steps(grad_fetches[1], middle)
    total = summing.finish()
    stream = wide(m.stream[...])
    inverse = inverse_of(stream)
    scaled = total * m.gains[1:2, :]
    shift = jnp.mean(stream * scaled, axis=-1, keepdims=True)
    cotangent = m.tangent[...] + inverse * (scaled - stream * inverse * inverse * shift)
    set_shard(cotangent, m.shard, m.pieces.at[1])
    gathered = gather_shard()
    last_arrived = exchange(5, 1)
    gathered.relay()
    grad_fetches[1].step(final)
    gathered.forward()
    arrived()
    gathered_blocks = gather_blocks(4, 0)
    gathered.finish()
    mixed_grads(m.whole, m.out_weight_held, 0, m.acc, cut)
    gathered_blocks.relay()
    backward_attention(lengths, m.acc, *tables, *kept[0], grads[0])
    grad_fetches[0].step(1)
    last_arrived()
    gathered_last = gather_blocks(5, 1)
    gathered_blocks.forward()
    gathered_blocks.finish()
    last_stores = [store(blocks[0], m.cotangents1, 0)]
    gathered_last.relay()
    grad_fetches[1].finish()
    last_stores.append(store(grads_held[1], m.grads_all1, 1))
    steps(grad_fetches[0], middle)
    gathered_last.forward()
    gathered_last.finish()
    last_stores.append(store(blocks[1], m.cotangents0, 2))
    grad_fetches[0].step(final)
    grad_fetches[0].finish()
    last_stores.append(store(grads_held[0], m.grads_all0, 3))
    for made in last_stores:
        made.wait()
    fabric.drain()
    fabric.drain_chains()


def product_kernel(layers, *refs):
    inputs, (query_out, key_out, value_out, out_out) = refs[:-4], refs[-4:]
    layer = pl.program_id(0)
    query_width, key_width = query_out.shape[-1], key_out.shape[-1]
    for number in range(layers):
        blocks, grads, blended, cotangent = inputs[4 * number : 4 * number + 4]

        @pl.when(layer == number)
        def _():
            product = contract_rows(blocks[...], grads[...])
            query_out[0] = product[:, :query_width]
            key_out[0] = product[:, query_width : query_width + key_width]
            value_out[0] = product[:, query_width + key_width :]
            out_out[0] = contract_rows(blended[...], cotangent[...])


CUTS = 2
FLOW_CUTS = 2


def body(
    tokens,
    lengths,
    norm_gains,
    query_weight,
    key_weight,
    value_weight,
    out_weight,
    query_probe,
    key_probe,
    value_probe,
    out_probe,
):
    width = lax.axis_size("tensor")
    batches = lax.axis_size("dp")
    sizes = (batches, width)
    tensor_index = lax.axis_index("tensor")
    share, model = tokens.shape
    group = share * width
    assert LEN % share == 0
    layers = query_weight.shape[0]
    assert layers == 2
    half_width = key_weight.shape[2]
    query_width = query_weight.shape[2]
    paired = half_width < HD
    key_width = 2 * half_width if paired else half_width
    sent_width = query_width + 2 * half_width
    block = query_probe.shape[1]
    cosine, sine = rope_tables(LEN, HD)
    lower_half = tensor_index % 2 == 0

    def swapped(value):
        pairs = [(source, source ^ 1) for source in range(width)]
        return lax.ppermute(value, "tensor", pairs)

    def join_halves(own_part):
        other_part = swapped(own_part)
        return jnp.where(
            lower_half,
            jnp.concatenate([own_part, other_part], axis=-1),
            jnp.concatenate([other_part, own_part], axis=-1),
        )

    def split_halves(values):
        first, second = values[:, :half_width], values[:, half_width:]
        own_part = jnp.where(lower_half, first, second)
        other_part = jnp.where(lower_half, second, first)
        return low(wide(own_part) + wide(swapped(other_part)))

    parts = [key_weight, value_weight, key_probe, value_probe]
    if paired:
        parts = [join_halves(part) for part in parts]
    key_full, value_full, key_probe_full, value_probe_full = parts

    def to_send(grads):
        if not paired:
            return grads
        return jnp.concatenate(
            [
                grads[:, :query_width],
                split_halves(grads[:, query_width : query_width + key_width]),
                split_halves(grads[:, query_width + key_width :]),
            ],
            axis=-1,
        )

    bf, f32 = jnp.bfloat16, jnp.float32
    chips = width // 2
    wide_width = query_width + 2 * key_width
    rows_in_all = batches * group

    def flow():
        inputs = dict(
            lengths=lengths,
            tokens=tokens,
            gains=norm_gains,
            cosine=cosine,
            sine=sine,
            query_weight=query_weight,
            key_weight=key_full,
            value_weight=value_full,
            out_weight=out_weight,
            query_probe=query_probe,
            key_probe=key_probe_full,
            value_probe=value_probe_full,
            out_probe=out_probe,
        )
        blocks_shape = (batches, width, share, block)
        outputs = dict(
            blocks0=blocks_shape,
            blocks1=blocks_shape,
            blended_all0=(batches, group, query_width),
            blended_all1=(batches, group, query_width),
            cotangents0=blocks_shape,
            cotangents1=blocks_shape,
            grads_all0=(batches, group, wide_width),
            grads_all1=(batches, group, wide_width),
        )
        held = {
            name + "_held": pltpu.VMEM(value.shape, bf)
            for name, value in list(inputs.items())[5:]
        }
        scratch = dict(
            whole=pltpu.VMEM((width, share, model), bf),
            blocks=pltpu.VMEM((layers,) + blocks_shape, bf),
            terms=pltpu.VMEM((width, share, model), bf),
            probed=pltpu.VMEM(blocks_shape, bf),
            beside=pltpu.VMEM((chips, share, model), bf),
            landed=pltpu.VMEM((chips, share, model), bf),
            beside_p=pltpu.VMEM((chips, batches, share, block), bf),
            landed_p=pltpu.VMEM((chips, batches, share, block), bf),
            relayed=pltpu.VMEM((2, share, model // 2), bf),
            relayed_p=pltpu.VMEM((2, batches // 2, share, block), bf),
            partial=pltpu.VMEM((layers, batches, group, wide_width), bf),
            returned=pltpu.VMEM((layers, 2, batches - 1, group, wide_width), bf),
            queries=pltpu.VMEM((layers, group, query_width), bf),
            keys=pltpu.VMEM((layers, group, key_width), bf),
            values=pltpu.VMEM((layers, group, key_width), bf),
            blended=pltpu.VMEM((layers, group, query_width), bf),
            blended_all=pltpu.VMEM((layers, batches, group, query_width), bf),
            mixed=pltpu.VMEM((group, query_width), bf),
            grads=pltpu.VMEM((layers, group, wide_width), bf),
            grads_held=pltpu.VMEM((layers, batches, group, wide_width), bf),
            acc=pltpu.VMEM((group, wide_width), f32),
            moved=pltpu.VMEM((group, wide_width), f32),
            shard=pltpu.VMEM((share, model), bf),
            stream=pltpu.VMEM((share, model), bf),
            tangent=pltpu.VMEM((share, model), f32),
            pieces=pltpu.VMEM((2, batches, share, block), bf),
            exchanged=pltpu.VMEM((6, batches, share, block), bf),
            **held,
            send=pltpu.SemaphoreType.DMA((semaphore_count(sizes),)),
            recv=pltpu.SemaphoreType.DMA((semaphore_count(sizes),)),
            load_sem=pltpu.SemaphoreType.DMA((layers * len(held),)),
            store_sem=pltpu.SemaphoreType.DMA((4,)),
        )
        vmem = pl.BlockSpec(memory_space=pltpu.VMEM)
        anywhere = pl.BlockSpec(memory_space=pl.ANY)
        return pl.pallas_call(
            functools.partial(
                flow_kernel, sizes, model // FLOW_CUTS, [*inputs, *outputs, *scratch]
            ),
            out_shape=[jax.ShapeDtypeStruct(shape, bf) for shape in outputs.values()],
            in_specs=[pl.BlockSpec(memory_space=pltpu.SMEM)]
            + [vmem] * 4
            + [anywhere] * len(held),
            out_specs=[anywhere] * len(outputs),
            scratch_shapes=list(scratch.values()),
            compiler_params=pltpu.CompilerParams(
                collective_id=0, has_side_effects=True, vmem_limit_bytes=67043328
            ),
        )(*inputs.values())

    def cost(flops, moved_bytes):
        return pl.CostEstimate(flops=flops, bytes_accessed=moved_bytes, transcendentals=0)

    def products(per_layer):
        out_block = out_probe.shape[2]
        by_rows = query_width % (CUTS * HD) == 0
        blended_cut = query_width // CUTS if by_rows else query_width
        out_cut = out_block if by_rows else out_block // CUTS
        in_specs, args = [], []
        for number, (blocks, grads, blended, cotangents) in enumerate(per_layer):

            def place(i, j, number=number):
                return (0, jnp.clip((i - number) * CUTS + j, 0, CUTS - 1))

            def still(i, j):
                return (0, 0)

            in_specs += [
                pl.BlockSpec((rows_in_all, block // CUTS), place),
                pl.BlockSpec((rows_in_all, sent_width), still),
                pl.BlockSpec((rows_in_all, blended_cut), place if by_rows else still),
                pl.BlockSpec((rows_in_all, out_cut), still if by_rows else place),
            ]
            args += [
                blocks.reshape(rows_in_all, block),
                grads.reshape(rows_in_all, sent_width),
                blended.reshape(rows_in_all, query_width),
                cotangents.reshape(rows_in_all, out_block),
            ]
        shapes = [
            (block, query_width),
            (block, half_width),
            (block, half_width),
            (query_width, out_block),
        ]
        return pl.pallas_call(
            functools.partial(product_kernel, layers),
            grid=(layers, CUTS),
            in_specs=in_specs,
            out_specs=[
                pl.BlockSpec((1, rows // CUTS, columns), lambda i, j: (i, j, 0))
                for rows, columns in shapes[:3]
            ]
            + [
                pl.BlockSpec(
                    (1, blended_cut, out_cut),
                    lambda i, j: (i, j, 0) if by_rows else (i, 0, j),
                )
            ],
            out_shape=[
                jax.ShapeDtypeStruct((layers, rows, columns), f32) for rows, columns in shapes
            ],
            compiler_params=pltpu.CompilerParams(
                dimension_semantics=("arbitrary", "arbitrary")
            ),
            cost_estimate=cost(2 * rows_in_all * block * query_width * 4, 32 << 20),
        )(*args)

    results = flow()
    blocks0, blocks1, blended0, blended1, cotangents0, cotangents1, grads0, grads1 = results
    sent = [to_send(grads.reshape(rows_in_all, wide_width)) for grads in (grads0, grads1)]
    return tuple(
        products(
            [
                (blocks0, sent[0], blended0, cotangents0),
                (blocks1, sent[1], blended1, cotangents1),
            ]
        )
    )


def solution(mesh):
    placed = (
        P(("dp", "tensor"), None),
        P(),
        P(),
        P(None, None, "tensor"),
        P(None, None, "tensor"),
        P(None, None, "tensor"),
        P(None, "tensor", None),
        P(None, "dp", "tensor"),
        P(None, "dp", "tensor"),
        P(None, "dp", "tensor"),
        P(None, "tensor", "dp"),
    )
    return jax.shard_map(
        body,
        mesh=mesh,
        in_specs=placed,
        out_specs=(
            P(None, "dp", "tensor"),
            P(None, "dp", "tensor"),
            P(None, "dp", "tensor"),
            P(None, "tensor", "dp"),
        ),
        check_vma=False,
    )
```
